32 devices in a mesh: dp: 1 (over z), tp: 4 (over y), cp: 8 (over x, core).
Axes of the slice: x: 4, y: 4, z: 1, core: 2. Of those that a mesh axis runs over, the one named last changes fastest.
The devices are a block of a 4x4x8 slice.
Arguments:
- x_in: bfloat16 [1, 8192, 2048], P('dp', 'cp')
- w_q: bfloat16 [2048, 16, 128], P(None, 'tp')
- w_k: bfloat16 [2048, 16, 128], P(None, 'tp')
- w_v: bfloat16 [2048, 16, 128], P(None, 'tp')
- w_o: bfloat16 [16, 128, 2048], P('tp')
- q_norm_w: float32 [16, 128], P('tp')
- k_norm_w: float32 [16, 128], P('tp')
- post_norm_w: float32 [2048], replicated
- grad_y: bfloat16 [1, 8192, 2048], P('dp', 'cp')
Outputs:
- output 1: bfloat16 [1, 8192, 2048], P('dp', 'cp')
- output 2: bfloat16 [1, 8192, 2048], P('dp', 'cp')
- output 3: float32 [2048, 16, 128], P('dp', 'tp')
- output 4: float32 [2048, 16, 128], P('dp', 'tp')
- output 5: float32 [2048, 16, 128], P('dp', 'tp')
- output 6: float32 [16, 128, 2048], P(('dp', 'tp'))
- output 7: float32 [16, 128], P(('dp', 'tp'))
- output 8: float32 [16, 128], P(('dp', 'tp'))
- output 9: float32 [2048], P('dp')
All inputs are finite; a program needn't handle non-finite values.
Results may differ from the reference program's by a relative error of at most 0.01742.
Values are sent between devices in bfloat16 or wider.
A program may use at most 768 MiB of HBM per device.

```python
import jax
import jax.numpy as jnp
from jax import lax

BATCH_SIZE = 1
SEQ_LEN = 8192
D_MODEL = 2048
NUM_HEADS = 16
KV_HEADS = 16
HEAD_DIM = 128
QUERY_ROWS = 256
ROPE_THETA = 500000.0
NORM_EPS = 1e-6


def setup_inputs(seed: int = 0, part: int = 0) -> dict:
    base_key = jax.random.key(seed)
    act_keys = jax.random.split(jax.random.fold_in(base_key, part), 2)
    wt_keys = jax.random.split(jax.random.fold_in(base_key, 1000003), 9)
    act_shape = (BATCH_SIZE, SEQ_LEN, D_MODEL)
    x_in = jax.random.normal(act_keys[0], act_shape, jnp.float32).astype(jnp.bfloat16)
    grad_y = jax.random.normal(act_keys[1], act_shape, jnp.float32).astype(jnp.bfloat16)
    in_scale = D_MODEL ** -0.5
    out_scale = (NUM_HEADS * HEAD_DIM) ** -0.5
    w_q = (jax.random.normal(wt_keys[0], (D_MODEL, NUM_HEADS, HEAD_DIM), jnp.float32) * in_scale).astype(jnp.bfloat16)
    w_k = (jax.random.normal(wt_keys[1], (D_MODEL, KV_HEADS, HEAD_DIM), jnp.float32) * in_scale).astype(jnp.bfloat16)
    w_v = (jax.random.normal(wt_keys[2], (D_MODEL, KV_HEADS, HEAD_DIM), jnp.float32) * in_scale).astype(jnp.bfloat16)
    w_o = (jax.random.normal(wt_keys[3], (NUM_HEADS, HEAD_DIM, D_MODEL), jnp.float32) * out_scale).astype(jnp.bfloat16)
    q_head_gain = jax.random.uniform(wt_keys[4], (NUM_HEADS, 1), jnp.float32, 0.6, 1.4)
    q_norm_w = q_head_gain * (1.0 + 0.1 * jax.random.normal(wt_keys[5], (NUM_HEADS, HEAD_DIM), jnp.float32))
    k_head_gain = jax.random.uniform(wt_keys[6], (KV_HEADS, 1), jnp.float32, 0.6, 1.4)
    k_norm_w = k_head_gain * (1.0 + 0.1 * jax.random.normal(wt_keys[7], (KV_HEADS, HEAD_DIM), jnp.float32))
    post_norm_w = 1.0 + 0.3 * jax.random.normal(wt_keys[8], (D_MODEL,), jnp.float32)
    return {"x_in": x_in, "w_q": w_q, "w_k": w_k, "w_v": w_v, "w_o": w_o, "q_norm_w": q_norm_w, "k_norm_w": k_norm_w, "post_norm_w": post_norm_w, "grad_y": grad_y}


def rope_tables():
    half_dim = HEAD_DIM // 2
    inv_freq = ROPE_THETA ** (-2.0 * jnp.arange(half_dim, dtype=jnp.float32) / HEAD_DIM)
    angles = jnp.arange(SEQ_LEN, dtype=jnp.float32)[:, None] * inv_freq[None, :]
    return jnp.cos(angles), jnp.sin(angles)


def apply_rope(values, cos_tab, sin_tab):
    half_dim = values.shape[-1] // 2
    low_half = values[..., :half_dim]
    high_half = values[..., half_dim:]
    cos_rows = cos_tab[:, None, :]
    sin_rows = sin_tab[:, None, :]
    return jnp.concatenate([low_half * cos_rows - high_half * sin_rows, high_half * cos_rows + low_half * sin_rows], axis=-1)


def whole_norm(lin_out, weight):
    inv_rms = lax.rsqrt(jnp.mean(lin_out * lin_out, axis=(-2, -1), keepdims=True) + NORM_EPS)
    return lin_out * inv_rms * weight


def causal_attention(q_rot, k_rot, v_val):
    group_size = NUM_HEADS // KV_HEADS
    n_blocks = SEQ_LEN // QUERY_ROWS
    q_heads = jnp.moveaxis(q_rot.reshape(BATCH_SIZE, SEQ_LEN, KV_HEADS, group_size, HEAD_DIM), 2, 0)
    k_heads = jnp.moveaxis(k_rot, 2, 0)
    v_heads = jnp.moveaxis(v_val, 2, 0)
    key_pos = jnp.arange(SEQ_LEN)
    score_scale = HEAD_DIM ** -0.5

    def one_head(head_args):
        q_head, k_head, v_head = head_args
        q_blocks = jnp.moveaxis(q_head.reshape(BATCH_SIZE, n_blocks, QUERY_ROWS, group_size, HEAD_DIM), 1, 0)

        def one_block(block_args):
            q_block, block_idx = block_args
            scores = jnp.einsum("bqgd,bkd->bgqk", q_block, k_head) * score_scale
            query_pos = block_idx * QUERY_ROWS + jnp.arange(QUERY_ROWS)
            allowed = query_pos[:, None] >= key_pos[None, :]
            scores = jnp.where(allowed, scores, -jnp.inf)
            probs_blk = jax.nn.softmax(scores, axis=-1)
            return jnp.einsum("bgqk,bkd->bqgd", probs_blk, v_head)

        out_blocks = lax.map(jax.checkpoint(one_block), (q_blocks, jnp.arange(n_blocks)))
        return jnp.moveaxis(out_blocks, 0, 1).reshape(BATCH_SIZE, SEQ_LEN, group_size, HEAD_DIM)

    out_heads = lax.map(one_head, (q_heads, k_heads, v_heads))
    return jnp.moveaxis(out_heads, 0, 2).reshape(BATCH_SIZE, SEQ_LEN, NUM_HEADS, HEAD_DIM)


def forward(x_f, w_q, w_k, w_v, w_o, q_norm_w, k_norm_w, post_norm_w):
    cos_tab, sin_tab = rope_tables()
    q_lin = jnp.einsum("btd,dhe->bthe", x_f, w_q)
    k_lin = jnp.einsum("btd,dhe->bthe", x_f, w_k)
    v_lin = jnp.einsum("btd,dhe->bthe", x_f, w_v)
    q_rot = apply_rope(whole_norm(q_lin, q_norm_w), cos_tab, sin_tab).astype(jnp.bfloat16).astype(jnp.float32)
    k_rot = apply_rope(whole_norm(k_lin, k_norm_w), cos_tab, sin_tab).astype(jnp.bfloat16).astype(jnp.float32)
    v_val = v_lin.astype(jnp.bfloat16).astype(jnp.float32)
    attn_out = causal_attention(q_rot, k_rot, v_val).astype(jnp.bfloat16).astype(jnp.float32)
    proj = jnp.einsum("bthe,hed->btd", attn_out, w_o)
    post_hat = proj * lax.rsqrt(jnp.mean(proj * proj, axis=-1, keepdims=True) + NORM_EPS)
    return x_f + post_hat * post_norm_w


def reference(x_in, w_q, w_k, w_v, w_o, q_norm_w, k_norm_w, post_norm_w, grad_y):
    y_full, pullback = jax.vjp(forward, x_in.astype(jnp.float32), w_q.astype(jnp.float32), w_k.astype(jnp.float32), w_v.astype(jnp.float32), w_o.astype(jnp.float32), q_norm_w, k_norm_w, post_norm_w)
    all_grads = pullback(grad_y.astype(jnp.float32))
    return (y_full.astype(jnp.bfloat16), all_grads[0].astype(jnp.bfloat16), all_grads[1], all_grads[2], all_grads[3], all_grads[4], all_grads[5], all_grads[6], all_grads[7])
```

```python
import functools
import math

import jax
import jax.numpy as jnp
from jax import lax
from jax.experimental import pallas as pl
from jax.experimental.pallas import tpu as pltpu
from jax.sharding import PartitionSpec as P

ROPE_THETA = 500000.0
NORM_EPS = 1e-6
LOG2E = 1.4426950408889634
VMEM = pltpu.VMEM
MESH = pl.DeviceIdType.MESH
NT = (((1,), (1,)), ((), ()))


def rope_tables(start_pos, seq_rows, head_dim):
    half_dim = head_dim // 2
    inv_freq = ROPE_THETA ** (-2.0 * jnp.arange(half_dim, dtype=jnp.float32) / head_dim)
    positions = (start_pos + jnp.arange(seq_rows)).astype(jnp.float32)
    angles = positions[:, None] * inv_freq[None, :]
    return jnp.cos(angles), jnp.sin(angles)


def apply_rope(values, cos_tab, sin_tab):
    half_dim = values.shape[-1] // 2
    low_half = values[..., :half_dim]
    high_half = values[..., half_dim:]
    return jnp.concatenate([low_half * cos_tab - high_half * sin_tab, high_half * cos_tab + low_half * sin_tab], axis=-1)


def rope_back(grad_in, cos_tab, sin_tab):
    return apply_rope(grad_in, cos_tab, -sin_tab)


def vmem_call(kernel, out_shape, n_in, scratch, collective_id=None, limit=48 << 20, cost=None):
    params = dict(vmem_limit_bytes=limit)
    if collective_id is not None:
        params.update(collective_id=collective_id, has_side_effects=True)
    return pl.pallas_call(
        kernel,
        out_shape=out_shape,
        in_specs=[pl.BlockSpec(memory_space=VMEM)] * n_in,
        out_specs=[pl.BlockSpec(memory_space=VMEM)] * len(out_shape),
        scratch_shapes=scratch,
        compiler_params=pltpu.CompilerParams(**params),
        cost_estimate=cost,
    )


def remote(src, dst, send_sem, recv_sem, device_id):
    return pltpu.make_async_remote_copy(src_ref=src, dst_ref=dst, send_sem=send_sem, recv_sem=recv_sem, device_id=device_id, device_id_type=MESH)


def cp_barrier(me, cp_size):
    barrier = pltpu.get_barrier_semaphore()
    for step in range(1, cp_size):
        pl.semaphore_signal(barrier, inc=1, device_id={"cp": lax.rem(me + step, cp_size)}, device_id_type=MESH)
    pl.semaphore_wait(barrier, cp_size - 1)


def group_barrier(me_tp, me_cp, tp_size, cp_size):
    barrier = pltpu.get_barrier_semaphore()
    for st in range(tp_size):
        for sc in range(cp_size):
            if st or sc:
                pl.semaphore_signal(barrier, inc=1, device_id={"tp": lax.rem(me_tp + st, tp_size), "cp": lax.rem(me_cp + sc, cp_size)}, device_id_type=MESH)
    pl.semaphore_wait(barrier, tp_size * cp_size - 1)


def scatter_qkv(heads, cp_size, q_in, k_in, v_in, q_out, k_out, v_out, loc, qs, qr, ks, kr, vs, vr, fks, fkr, fvs, fvr):
    me = lax.axis_index("cp")
    core = lax.rem(me, 2)
    chip = me // 2
    cp_barrier(me, cp_size)
    sends = []
    for r in (1, heads - 1, 2):
        dst = lax.rem(chip + r, heads)
        sends.append(remote(k_in.at[dst], k_out.at[me], ks.at[r], kr.at[r], {"cp": dst * 2 + core}))
        sends.append(remote(v_in.at[dst], v_out.at[me], vs.at[r], vr.at[r], {"cp": dst * 2 + core}))
    for r in range(1, cp_size):
        dst = lax.rem(me + r, cp_size)
        sends.append(remote(q_in.at[dst], q_out.at[me], qs.at[r], qr.at[r], {"cp": dst}))
    for copy in sends:
        copy.start()
    local = [
        pltpu.make_async_copy(q_in.at[me], q_out.at[me], loc.at[0]),
        pltpu.make_async_copy(k_in.at[chip], k_out.at[me], loc.at[1]),
        pltpu.make_async_copy(v_in.at[chip], v_out.at[me], loc.at[2]),
    ]
    for copy in local:
        copy.start()
    partner = {"cp": me + 1 - 2 * core}
    forwards = []
    for r in (0, 1, heads - 1, 2):
        src = lax.rem(chip - r + heads, heads) * 2 + core
        if r == 0:
            local[1].wait()
            local[2].wait()
        else:
            remote(k_in.at[0], k_out.at[src], ks.at[r], kr.at[r], partner).wait_recv()
            remote(v_in.at[0], v_out.at[src], vs.at[r], vr.at[r], partner).wait_recv()
        for buf, ss, rs in ((k_out, fks, fkr), (v_out, fvs, fvr)):
            copy = remote(buf.at[src], buf.at[src], ss.at[r], rs.at[r], partner)
            copy.start()
            forwards.append(copy)
    local[0].wait()
    for copy in sends:
        copy.wait_send()
    for r in range(1, cp_size):
        remote(q_in.at[0], q_out.at[lax.rem(me - r + cp_size, cp_size)], qs.at[r], qr.at[r], partner).wait_recv()
    for copy in forwards:
        copy.wait()


def attend(sub, scale, q_ref, k_ref, v_ref, o_ref, lse_ref, vt_scr, m_scr, l_scr, acc_scr):
    blk = pl.program_id(0)
    core = lax.rem(lax.axis_index("cp"), 2)
    coef = scale * LOG2E
    block_len = k_ref.shape[1]
    vt_scr[blk] = v_ref[blk].T
    m_scr[...] = jnp.full_like(m_scr, -jnp.inf)
    l_scr[...] = jnp.zeros_like(l_scr)
    acc_scr[...] = jnp.zeros_like(acc_scr)

    def step(b, masked):
        k_blk = k_ref[b]
        vt_blk = vt_scr[b]
        for part in range(2):
            cols = slice(part * sub, (part + 1) * sub)
            s = lax.dot_general(k_blk, q_ref[0, cols, :], NT, preferred_element_type=jnp.float32)
            if masked:
                first = (core if part == 0 else 3 - core) * sub
                kv_pos = lax.broadcasted_iota(jnp.int32, (block_len, sub), 0)
                q_pos = first + lax.broadcasted_iota(jnp.int32, (block_len, sub), 1)
                s = jnp.where(kv_pos <= q_pos, s, -jnp.inf)
            m_old = m_scr[:, cols]
            m_new = jnp.maximum(m_old, jnp.max(s, axis=0, keepdims=True))
            p = jnp.exp2(s * coef - m_new * coef)
            alpha = jnp.exp2((m_old - m_new) * coef)
            l_scr[:, cols] = l_scr[:, cols] * alpha + jnp.sum(p, axis=0, keepdims=True)
            acc_scr[:, cols] = acc_scr[:, cols] * alpha + jnp.dot(vt_blk, p.astype(jnp.bfloat16), preferred_element_type=jnp.float32)
            m_scr[:, cols] = m_new

    def body(b, carry):
        step(b, False)
        return carry

    lax.fori_loop(0, blk, body, 0)
    step(blk, True)
    o_ref[0] = (acc_scr[...] / l_scr[...]).T.astype(o_ref.dtype)
    lse_ref[0] = m_scr[...] * coef + jnp.log2(l_scr[...])


def attend_back(sub, scale, q_ref, k_ref, v_ref, o_ref, do_ref, lse_ref, dq_ref, dk_ref, dv_ref, kt_scr, dqt_scr, dl_scr):
    blk = pl.program_id(0)
    core = lax.rem(lax.axis_index("cp"), 2)
    coef = scale * LOG2E
    rows = q_ref.shape[1]
    block_len = k_ref.shape[1]
    kt_scr[blk] = k_ref[blk].T
    prod = o_ref[0].astype(jnp.float32) * do_ref[0].astype(jnp.float32)
    dl_scr[...] = jnp.sum(prod.T, axis=0, keepdims=True)
    dqt_scr[...] = jnp.zeros_like(dqt_scr)

    def step(b, masked):
        q = q_ref[0]
        do = do_ref[0]
        lse = lse_ref[0]
        delta = dl_scr[...]
        for part in range(block_len // sub):
            kv = slice(part * sub, (part + 1) * sub)
            k_blk = k_ref[b, kv, :]
            s = lax.dot_general(k_blk, q, NT, preferred_element_type=jnp.float32)
            p = jnp.exp2(s * coef - lse)
            if masked:
                kv_pos = part * sub + lax.broadcasted_iota(jnp.int32, (sub, rows), 0)
                col = lax.broadcasted_iota(jnp.int32, (sub, rows), 1)
                q_pos = jnp.where(col < sub, core * sub + col, (2 - core) * sub + col)
                p = jnp.where(kv_pos <= q_pos, p, 0.0)
            dp = lax.dot_general(v_ref[b, kv, :], do, NT, preferred_element_type=jnp.float32)
            ds = (p * (dp - delta)).astype(jnp.bfloat16)
            new_v = jnp.dot(p.astype(jnp.bfloat16), do, preferred_element_type=jnp.float32)
            new_k = jnp.dot(ds, q, preferred_element_type=jnp.float32) * scale
            if masked:
                dv_ref[b, kv, :] = new_v
                dk_ref[b, kv, :] = new_k
            else:
                dv_ref[b, kv, :] += new_v
                dk_ref[b, kv, :] += new_k
            dqt_scr[...] += jnp.dot(kt_scr[b, :, kv], ds, preferred_element_type=jnp.float32)

    def body(b, carry):
        step(b, False)
        return carry

    step(blk, True)
    lax.fori_loop(0, blk, body, 0)
    dq_ref[0] = dqt_scr[...].T * scale


def heads_to_rows(heads, tp_size, cp_size, o_in, o_out, ss, rs, loc):
    me_tp = lax.axis_index("tp")
    me_cp = lax.axis_index("cp")
    core = lax.rem(me_cp, 2)
    head = me_tp * heads + me_cp // 2
    sub = o_out.shape[1]
    group_barrier(me_tp, me_cp, tp_size, cp_size)
    for s in range(2):
        dst_tp = core if s == 0 else 3 - core
        for r in range(cp_size):
            dst_cp = lax.rem(me_cp + r, cp_size)
            src = o_in.at[dst_cp, pl.ds(s * sub, sub), :]
            if r == 0:
                own = dst_tp == me_tp

                @pl.when(own)
                def _():
                    pltpu.make_async_copy(src, o_out.at[head], rs.at[head]).start()

                @pl.when(jnp.logical_not(own))
                def _():
                    remote(src, o_out.at[head], ss.at[s, 0], rs.at[head], {"tp": dst_tp, "cp": dst_cp}).start()
            else:
                remote(src, o_out.at[head], ss.at[s, r], rs.at[head], {"tp": dst_tp, "cp": dst_cp}).start()
    for h in range(heads * tp_size):
        pltpu.make_async_copy(o_out.at[h], o_out.at[h], rs.at[h]).wait()
    for s in range(2):
        dst_tp = core if s == 0 else 3 - core
        for r in range(cp_size):
            wait = remote(o_in.at[0, pl.ds(0, sub), :], o_out.at[head], ss.at[s, r], rs.at[head], {"cp": me_cp})
            if r == 0:
                @pl.when(dst_tp != me_tp)
                def _():
                    wait.wait_send()
            else:
                wait.wait_send()


def rows_to_heads(heads, tp_size, cp_size, g_in, g_out, ss, rs, loc):
    me_tp = lax.axis_index("tp")
    me_cp = lax.axis_index("cp")
    core = lax.rem(me_cp, 2)
    sub = g_in.shape[1]
    row_core = jnp.where(me_tp < 2, me_tp, 3 - me_tp)
    row_slot = me_tp // 2
    group_barrier(me_tp, me_cp, tp_size, cp_size)
    for rt in range(tp_size):
        dst_tp = lax.rem(me_tp + rt, tp_size)
        for r in range(heads):
            dst_chip = lax.rem(me_cp // 2 + r, heads)
            dst_cp = dst_chip * 2 + row_core
            src = g_in.at[dst_tp * heads + dst_chip]
            dst = g_out.at[me_cp, pl.ds(row_slot * sub, sub), :]
            if rt == 0 and r == 0:
                @pl.when(row_core == core)
                def _():
                    pltpu.make_async_copy(src, dst, rs.at[me_cp, row_slot]).start()

                @pl.when(row_core != core)
                def _():
                    remote(src, dst, ss.at[rt, r], rs.at[me_cp, row_slot], {"tp": dst_tp, "cp": dst_cp}).start()
            else:
                remote(src, dst, ss.at[rt, r], rs.at[me_cp, row_slot], {"tp": dst_tp, "cp": dst_cp}).start()
    for i in range(cp_size):
        for s in range(2):
            part = g_out.at[i, pl.ds(s * sub, sub), :]
            pltpu.make_async_copy(part, part, rs.at[i, s]).wait()
    for rt in range(tp_size):
        for r in range(heads):
            wait = remote(g_in.at[0], g_out.at[0, pl.ds(0, sub), :], ss.at[rt, r], rs.at[0, 0], {"cp": me_cp})
            if rt == 0 and r == 0:
                @pl.when(row_core != core)
                def _():
                    wait.wait_send()
            else:
                wait.wait_send()


def gather_grads(heads, cp_size, dq_in, dk_in, dv_in, dq_out, dk_out, dv_out, pk, pv, sk, sv, loc, qs, qr, pks, pkr, pvs, pvr, ks, kr, vs, vr):
    me = lax.axis_index("cp")
    core = lax.rem(me, 2)
    chip = me // 2
    cp_barrier(me, cp_size)
    partner = {"cp": me + 1 - 2 * core}
    pair = []
    for x in range(heads):
        for src, dst, ss, rs in ((dk_in, pk, pks, pkr), (dv_in, pv, pvs, pvr)):
            copy = remote(src.at[2 * x + 1 - core], dst.at[x], ss.at[x], rs.at[x], partner)
            copy.start()
            pair.append(copy)
    sends = []
    for r in range(1, cp_size):
        dst = lax.rem(me + r, cp_size)
        copy = remote(dq_in.at[dst], dq_out.at[chip, core], qs.at[r], qr.at[r], {"cp": dst})
        copy.start()
        sends.append(copy)
    own = pltpu.make_async_copy(dq_in.at[me], dq_out.at[chip, core], loc.at[0])
    own.start()
    for x in range(heads):
        pair[2 * x].wait()
        pair[2 * x + 1].wait()
        sk[x] = dk_in[2 * x + core] + pk[x]
        sv[x] = (dv_in[2 * x + core] + pv[x]).astype(sv.dtype)
    for r in (1, heads - 1, 2):
        dst = lax.rem(chip + r, heads)
        for src, out, ss, rs in ((sk, dk_out, ks, kr), (sv, dv_out, vs, vr)):
            copy = remote(src.at[dst], out.at[chip], ss.at[r], rs.at[r], {"cp": dst * 2 + core})
            copy.start()
            sends.append(copy)
    locals_ = [pltpu.make_async_copy(sk.at[chip], dk_out.at[chip], loc.at[1]), pltpu.make_async_copy(sv.at[chip], dv_out.at[chip], loc.at[2])]
    for copy in locals_:
        copy.start()
    own.wait()
    for copy in locals_:
        copy.wait()
    for copy in sends:
        copy.wait_send()
    for r in range(1, cp_size):
        src = lax.rem(me - r + cp_size, cp_size)
        remote(dq_in.at[0], dq_out.at[src // 2, lax.rem(src, 2)], qs.at[r], qr.at[r], partner).wait_recv()
    for r in (1, heads - 1, 2):
        src = lax.rem(chip - r + heads, heads)
        remote(sk.at[0], dk_out.at[src], ks.at[r], kr.at[r], partner).wait_recv()
        remote(sv.at[0], dv_out.at[src], vs.at[r], vr.at[r], partner).wait_recv()


def solution(mesh):
    tp_size = mesh.shape["tp"]
    cp_size = mesh.shape["cp"]
    act_spec = P("dp", "cp", None)
    col_spec = P(None, "tp", None)
    part_col = P("dp", "tp", None)
    in_specs = (act_spec, col_spec, col_spec, col_spec, P("tp", None, None), P("tp", None), P("tp", None), P(None), act_spec)
    out_specs = (act_spec, act_spec, part_col, part_col, part_col, P(("dp", "tp"), None, None), P(("dp", "tp"), None), P(("dp", "tp"), None), P("dp"))
    dma = pltpu.SemaphoreType.DMA

    def local_run(x_in, w_q, w_k, w_v, w_o, q_norm_w, k_norm_w, post_norm_w, grad_y):
        n_batch, block_len, d_model = x_in.shape
        heads, head_dim = w_q.shape[1:]
        assert n_batch == 1 and w_k.shape[1] == heads and cp_size == 2 * heads and tp_size == 4
        sub = block_len // tp_size
        rows = 2 * sub
        width = heads * head_dim * tp_size
        scale = head_dim ** -0.5
        f32 = jnp.float32
        b16 = jnp.bfloat16
        tp_index = lax.axis_index("tp")
        cp_index = lax.axis_index("cp")
        cos_tab, sin_tab = rope_tables(cp_index * block_len, block_len, head_dim)
        x_loc = x_in[0]
        dy_loc = grad_y[0]
        w_o_full = lax.all_gather(w_o, "tp", axis=0, tiled=True)

        q_lin = jnp.einsum("ld,dhe->hle", x_loc, w_q, preferred_element_type=f32)
        k_lin = jnp.einsum("ld,dhe->hle", x_loc, w_k, preferred_element_type=f32)
        v_lin = jnp.einsum("ld,dhe->hle", x_loc, w_v, preferred_element_type=f32)
        sq = lax.psum(jnp.stack([jnp.sum(q_lin * q_lin, axis=(0, 2)), jnp.sum(k_lin * k_lin, axis=(0, 2))]), "tp")
        inv = lax.rsqrt(sq / width + NORM_EPS)
        q_inv = inv[0][None, :, None]
        k_inv = inv[1][None, :, None]
        q_rot = apply_rope(q_lin * q_inv * q_norm_w[:, None, :], cos_tab, sin_tab).astype(b16)
        k_rot = apply_rope(k_lin * k_inv * k_norm_w[:, None, :], cos_tab, sin_tab).astype(b16)
        v_val = v_lin.astype(b16)

        q4 = q_rot.reshape(heads, 4, sub, head_dim)
        q_send = jnp.stack([q4[:, 0], q4[:, 3], q4[:, 1], q4[:, 2]], axis=1).reshape(cp_size, rows, head_dim)
        q_all, k_all, v_all = vmem_call(
            functools.partial(scatter_qkv, heads, cp_size),
            [jax.ShapeDtypeStruct((cp_size, rows, head_dim), b16)] + [jax.ShapeDtypeStruct((cp_size, block_len, head_dim), b16)] * 2,
            3,
            [dma((3,)), dma((cp_size,)), dma((cp_size,))] + [dma((heads,))] * 8,
            collective_id=0,
        )(q_send, k_rot, v_val)

        qspec = pl.BlockSpec((1, rows, head_dim), lambda i: (i, 0, 0))
        lspec = pl.BlockSpec((1, 1, rows), lambda i: (i, 0, 0))
        whole = pl.BlockSpec(memory_space=VMEM)
        pair_flops = cp_size * (cp_size + 1) // 2 * rows * block_len * head_dim * 2
        o_all, lse = pl.pallas_call(
            functools.partial(attend, sub, scale),
            grid=(cp_size,),
            in_specs=[qspec, whole, whole],
            out_specs=[qspec, lspec],
            out_shape=[jax.ShapeDtypeStruct((cp_size, rows, head_dim), b16), jax.ShapeDtypeStruct((cp_size, 1, rows), f32)],
            scratch_shapes=[VMEM((cp_size, head_dim, block_len), b16), VMEM((1, rows), f32), VMEM((1, rows), f32), VMEM((head_dim, rows), f32)],
            compiler_params=pltpu.CompilerParams(vmem_limit_bytes=48 << 20),
            cost_estimate=pl.CostEstimate(flops=2 * pair_flops, bytes_accessed=6 << 20, transcendentals=0),
        )(q_all, k_all, v_all)

        n_heads = heads * tp_size
        o_rows = vmem_call(
            functools.partial(heads_to_rows, heads, tp_size, cp_size),
            [jax.ShapeDtypeStruct((n_heads, sub, head_dim), b16)],
            1,
            [dma((2, cp_size)), dma((n_heads,)), dma((1,))],
            collective_id=1,
        )(o_all)[0]

        x_rows = lax.dynamic_slice_in_dim(x_loc, tp_index * sub, sub, 0)
        dy_rows = lax.dynamic_slice_in_dim(dy_loc, tp_index * sub, sub, 0).astype(f32)
        proj = jnp.einsum("hle,hed->ld", o_rows, w_o_full, preferred_element_type=f32)
        post_inv = lax.rsqrt(jnp.mean(proj * proj, axis=-1, keepdims=True) + NORM_EPS)
        post_hat = proj * post_inv
        y_rows = (x_rows + post_hat * post_norm_w).astype(b16)
        grad_post = jnp.sum(dy_rows * post_hat, axis=0)
        grad_hat = dy_rows * post_norm_w
        gp_rows = (post_inv * (grad_hat - post_hat * jnp.mean(grad_hat * post_hat, axis=-1, keepdims=True))).astype(b16)
        do_rows = jnp.einsum("ld,hed->hle", gp_rows, w_o_full, preferred_element_type=f32).astype(b16)

        do_all = vmem_call(
            functools.partial(rows_to_heads, heads, tp_size, cp_size),
            [jax.ShapeDtypeStruct((cp_size, rows, head_dim), b16)],
            1,
            [dma((tp_size, heads)), dma((cp_size, 2)), dma((1,))],
            collective_id=2,
        )(do_rows)[0]

        y_out = lax.all_gather(y_rows, "tp", axis=0, tiled=True)
        grad_proj = lax.all_gather(gp_rows, "tp", axis=0, tiled=True)
        o_gath = lax.all_gather(o_rows, "tp", axis=0)
        o_own = lax.dynamic_slice_in_dim(o_gath, tp_index * heads, heads, 1)

        dq_all, dk_all, dv_all = pl.pallas_call(
            functools.partial(attend_back, sub, scale),
            grid=(cp_size,),
            in_specs=[qspec, whole, whole, qspec, qspec, lspec],
            out_specs=[qspec, whole, whole],
            out_shape=[jax.ShapeDtypeStruct((cp_size, rows, head_dim), f32)] + [jax.ShapeDtypeStruct((cp_size, block_len, head_dim), f32)] * 2,
            scratch_shapes=[VMEM((cp_size, head_dim, block_len), b16), VMEM((head_dim, rows), f32), VMEM((1, rows), f32)],
            compiler_params=pltpu.CompilerParams(vmem_limit_bytes=48 << 20),
            cost_estimate=pl.CostEstimate(flops=5 * pair_flops, bytes_accessed=16 << 20, transcendentals=0),
        )(q_all, k_all, v_all, o_all, do_all, lse)

        grad_w_o = jnp.einsum("thle,tld->hed", o_own, grad_proj.reshape(tp_size, sub, d_model), preferred_element_type=f32)

        dq_home, dk_home, dv_home = vmem_call(
            functools.partial(gather_grads, heads, cp_size),
            [jax.ShapeDtypeStruct((heads, 2, rows, head_dim), f32), jax.ShapeDtypeStruct((heads, block_len, head_dim), f32), jax.ShapeDtypeStruct((heads, block_len, head_dim), b16)],
            3,
            [VMEM((heads, block_len, head_dim), f32)] * 3 + [VMEM((heads, block_len, head_dim), b16)]
            + [dma((3,)), dma((cp_size,)), dma((cp_size,))] + [dma((heads,))] * 8,
            collective_id=3,
        )(dq_all, dk_all, dv_all)
        dq5 = dq_home.reshape(heads, 4, sub, head_dim)
        dq_rot = jnp.stack([dq5[:, 0], dq5[:, 2], dq5[:, 3], dq5[:, 1]], axis=1).reshape(heads, block_len, head_dim)

        dq_s = rope_back(dq_rot, cos_tab, sin_tab)
        dk_s = rope_back(dk_home, cos_tab, sin_tab)
        q_hat = q_lin * q_inv
        k_hat = k_lin * k_inv
        grad_qn = jnp.sum(dq_s * q_hat, axis=1)
        grad_kn = jnp.sum(dk_s * k_hat, axis=1)
        dq_n = dq_s * q_norm_w[:, None, :]
        dk_n = dk_s * k_norm_w[:, None, :]
        dots = lax.psum(jnp.stack([jnp.sum(dq_n * q_hat, axis=(0, 2)), jnp.sum(dk_n * k_hat, axis=(0, 2))]), "tp") / width
        dq16 = (q_inv * (dq_n - q_hat * dots[0][None, :, None])).astype(b16)
        dk16 = (k_inv * (dk_n - k_hat * dots[1][None, :, None])).astype(b16)
        grad_w_q = jnp.einsum("ld,hle->dhe", x_loc, dq16, preferred_element_type=f32)
        grad_w_k = jnp.einsum("ld,hle->dhe", x_loc, dk16, preferred_element_type=f32)
        grad_w_v = jnp.einsum("ld,hle->dhe", x_loc, dv_home, preferred_element_type=f32)
        dx_part = (jnp.einsum("hle,dhe->ld", dq16, w_q, preferred_element_type=f32)
                   + jnp.einsum("hle,dhe->ld", dk16, w_k, preferred_element_type=f32)
                   + jnp.einsum("hle,dhe->ld", dv_home, w_v, preferred_element_type=f32))
        dx_rows = lax.psum_scatter(dx_part, "tp", scatter_dimension=0, tiled=True)
        grad_x = lax.all_gather((dy_rows + dx_rows).astype(b16), "tp", axis=0, tiled=True)
        grad_post = lax.psum(grad_post, ("tp", "cp"))
        weight_grads = lax.psum((grad_w_q, grad_w_k, grad_w_v, grad_w_o, grad_qn, grad_kn), "cp")
        return (y_out[None], grad_x[None]) + tuple(weight_grads) + (grad_post,)

    return jax.shard_map(local_run, mesh=mesh, in_specs=in_specs, out_specs=out_specs, check_vma=False)
```

```python
import functools
import math

import jax
import jax.numpy as jnp
from jax import lax
from jax.experimental import pallas as pl
from jax.experimental.pallas import tpu as pltpu
from jax.sharding import PartitionSpec as P

ROPE_THETA = 500000.0
NORM_EPS = 1e-6
LOG2E = 1.4426950408889634
VMEM = pltpu.VMEM
MESH = pl.DeviceIdType.MESH
NT = (((1,), (1,)), ((), ()))


def rope_tables(start_pos, seq_rows, head_dim):
    half_dim = head_dim // 2
    inv_freq = ROPE_THETA ** (-2.0 * jnp.arange(half_dim, dtype=jnp.float32) / head_dim)
    positions = (start_pos + jnp.arange(seq_rows)).astype(jnp.float32)
    angles = positions[:, None] * inv_freq[None, :]
    return jnp.cos(angles), jnp.sin(angles)


def apply_rope(values, cos_tab, sin_tab):
    half_dim = values.shape[-1] // 2
    low_half = values[..., :half_dim]
    high_half = values[..., half_dim:]
    return jnp.concatenate([low_half * cos_tab - high_half * sin_tab, high_half * cos_tab + low_half * sin_tab], axis=-1)


def rope_back(grad_in, cos_tab, sin_tab):
    return apply_rope(grad_in, cos_tab, -sin_tab)


def vmem_call(kernel, out_shape, n_in, scratch, collective_id=None, limit=48 << 20, cost=None):
    params = dict(vmem_limit_bytes=limit)
    if collective_id is not None:
        params.update(collective_id=collective_id, has_side_effects=True)
    return pl.pallas_call(
        kernel,
        out_shape=out_shape,
        in_specs=[pl.BlockSpec(memory_space=VMEM)] * n_in,
        out_specs=[pl.BlockSpec(memory_space=VMEM)] * len(out_shape),
        scratch_shapes=scratch,
        compiler_params=pltpu.CompilerParams(**params),
        cost_estimate=cost,
    )


def remote(src, dst, send_sem, recv_sem, device_id):
    return pltpu.make_async_remote_copy(src_ref=src, dst_ref=dst, send_sem=send_sem, recv_sem=recv_sem, device_id=device_id, device_id_type=MESH)


def cp_barrier(me, cp_size):
    barrier = pltpu.get_barrier_semaphore()
    for step in range(1, cp_size):
        pl.semaphore_signal(barrier, inc=1, device_id={"cp": lax.rem(me + step, cp_size)}, device_id_type=MESH)
    pl.semaphore_wait(barrier, cp_size - 1)


def group_barrier(me_tp, me_cp, tp_size, cp_size):
    barrier = pltpu.get_barrier_semaphore()
    for st in range(tp_size):
        for sc in range(cp_size):
            if st or sc:
                pl.semaphore_signal(barrier, inc=1, device_id={"tp": lax.rem(me_tp + st, tp_size), "cp": lax.rem(me_cp + sc, cp_size)}, device_id_type=MESH)
    pl.semaphore_wait(barrier, tp_size * cp_size - 1)


def scatter_qkv(heads, cp_size, q_in, k_in, v_in, q_out, k_out, v_out, loc, qs, qr, ks, kr, vs, vr, fks, fkr, fvs, fvr):
    me = lax.axis_index("cp")
    core = lax.rem(me, 2)
    chip = me // 2
    cp_barrier(me, cp_size)
    sends = []
    for r in (1, heads - 1, 2):
        dst = lax.rem(chip + r, heads)
        sends.append(remote(k_in.at[dst], k_out.at[me], ks.at[r], kr.at[r], {"cp": dst * 2 + core}))
        sends.append(remote(v_in.at[dst], v_out.at[me], vs.at[r], vr.at[r], {"cp": dst * 2 + core}))
    for r in range(1, cp_size):
        dst = lax.rem(me + r, cp_size)
        sends.append(remote(q_in.at[dst], q_out.at[me], qs.at[r], qr.at[r], {"cp": dst}))
    for copy in sends:
        copy.start()
    local = [
        pltpu.make_async_copy(q_in.at[me], q_out.at[me], loc.at[0]),
        pltpu.make_async_copy(k_in.at[chip], k_out.at[me], loc.at[1]),
        pltpu.make_async_copy(v_in.at[chip], v_out.at[me], loc.at[2]),
    ]
    for copy in local:
        copy.start()
    partner = {"cp": me + 1 - 2 * core}
    forwards = []
    for r in (0, 1, heads - 1, 2):
        src = lax.rem(chip - r + heads, heads) * 2 + core
        if r == 0:
            local[1].wait()
            local[2].wait()
        else:
            remote(k_in.at[0], k_out.at[src], ks.at[r], kr.at[r], partner).wait_recv()
            remote(v_in.at[0], v_out.at[src], vs.at[r], vr.at[r], partner).wait_recv()
        for buf, ss, rs in ((k_out, fks, fkr), (v_out, fvs, fvr)):
            copy = remote(buf.at[src], buf.at[src], ss.at[r], rs.at[r], partner)
            copy.start()
            forwards.append(copy)
    local[0].wait()
    for copy in sends:
        copy.wait_send()
    for r in range(1, cp_size):
        remote(q_in.at[0], q_out.at[lax.rem(me - r + cp_size, cp_size)], qs.at[r], qr.at[r], partner).wait_recv()
    for copy in forwards:
        copy.wait()


def attend(sub, scale, q_ref, k_ref, v_ref, o_ref, lse_ref, vt_scr, m_scr, l_scr, acc_scr, s_a, s_b, mx_a):
    blk = pl.program_id(0)
    core = lax.rem(lax.axis_index("cp"), 2)
    coef = scale * LOG2E
    half = k_ref.shape[1] // 2
    cols = q_ref.shape[1]
    chunk = half // 2
    vt_scr[blk] = v_ref[blk].T
    m_scr[...] = jnp.full_like(m_scr, -jnp.inf)
    l_scr[...] = jnp.zeros_like(l_scr)
    acc_scr[...] = jnp.zeros_like(acc_scr)

    def fold(op, values):
        return op(values.reshape(values.shape[0] // 8, 8, cols), axis=0)

    def scores(b, h, c):
        kv = slice(h * half + c * chunk, h * half + (c + 1) * chunk)
        return lax.dot_general(k_ref[b, kv, :], q_ref[0], NT, preferred_element_type=jnp.float32)

    def mask(s, h, c):
        kv_pos = h * half + c * chunk + lax.broadcasted_iota(jnp.int32, s.shape, 0)
        col = lax.broadcasted_iota(jnp.int32, s.shape, 1)
        q_pos = jnp.where(col < sub, core * sub + col, (2 - core) * sub + col)
        return jnp.where(kv_pos <= q_pos, s, -jnp.inf)

    def step(buf, mx, b, h, nxt):
        m_old = m_scr[...]
        m_new = jnp.maximum(m_old, mx)
        mc = m_new * coef
        alpha = jnp.exp2((m_old - m_new) * coef)
        lsum = jnp.zeros((8, cols), jnp.float32)
        new_mx = None
        for c in range(2):
            rows = slice(c * chunk, (c + 1) * chunk)
            if nxt is not None:
                nbuf, nb, nh, masked = nxt
                s = scores(nb, nh, c)
                if masked:
                    s = mask(s, nh, c)
                nbuf[rows, :] = s
                part = fold(jnp.max, s)
                new_mx = part if new_mx is None else jnp.maximum(new_mx, part)
            p = jnp.exp2(buf[rows, :] * coef - mc)
            lsum = lsum + fold(jnp.sum, p)
            pv = jnp.dot(vt_scr[b, :, h * half + c * chunk : h * half + (c + 1) * chunk], p.astype(jnp.bfloat16), preferred_element_type=jnp.float32)
            acc_scr[...] = acc_scr[...] * alpha + pv if c == 0 else acc_scr[...] + pv
        l_scr[...] = l_scr[...] * alpha + jnp.sum(lsum, axis=0, keepdims=True)
        m_scr[...] = m_new
        return None if nxt is None else jnp.max(new_mx, axis=0, keepdims=True)

    for c in range(2):
        s_a[c * chunk : (c + 1) * chunk, :] = scores(0, 0, c)
    mx_a[...] = jnp.max(s_a[...], axis=0, keepdims=True)

    def body(b, carry):
        mx_b = step(s_a, mx_a[...], b, 0, (s_b, b, 1, False))
        mx_a[...] = step(s_b, mx_b, b, 1, (s_a, b + 1, 0, False))
        return carry

    lax.fori_loop(0, blk, body, 0)
    for c in range(2):
        rows = slice(c * chunk, (c + 1) * chunk)
        s_a[rows, :] = mask(s_a[rows, :], 0, c)
    mx_b = step(s_a, jnp.max(s_a[...], axis=0, keepdims=True), blk, 0, (s_b, blk, 1, True))
    step(s_b, mx_b, blk, 1, None)
    o_ref[0] = (acc_scr[...] / l_scr[...]).T.astype(o_ref.dtype)
    lse_ref[0] = m_scr[...] * coef + jnp.log2(l_scr[...])


def attend_back(sub, scale, q_ref, k_ref, v_ref, o_ref, do_ref, lse_ref, dq_ref, dk_ref, dv_ref, kt_scr, dqt_scr, dl_scr):
    blk = pl.program_id(0)
    core = lax.rem(lax.axis_index("cp"), 2)
    coef = scale * LOG2E
    rows = q_ref.shape[1]
    block_len = k_ref.shape[1]
    kt_scr[blk] = k_ref[blk].T
    prod = o_ref[0].astype(jnp.float32) * do_ref[0].astype(jnp.float32)
    dl_scr[...] = jnp.sum(prod.T, axis=0, keepdims=True)
    dqt_scr[...] = jnp.zeros_like(dqt_scr)

    def step(b, masked):
        q = q_ref[0]
        do = do_ref[0]
        lse = lse_ref[0]
        delta = dl_scr[...]
        for part in range(block_len // sub):
            kv = slice(part * sub, (part + 1) * sub)
            k_blk = k_ref[b, kv, :]
            s = lax.dot_general(k_blk, q, NT, preferred_element_type=jnp.float32)
            p = jnp.exp2(s * coef - lse)
            if masked:
                kv_pos = part * sub + lax.broadcasted_iota(jnp.int32, (sub, rows), 0)
                col = lax.broadcasted_iota(jnp.int32, (sub, rows), 1)
                q_pos = jnp.where(col < sub, core * sub + col, (2 - core) * sub + col)
                p = jnp.where(kv_pos <= q_pos, p, 0.0)
            dp = lax.dot_general(v_ref[b, kv, :], do, NT, preferred_element_type=jnp.float32)
            ds = (p * (dp - delta)).astype(jnp.bfloat16)
            new_v = jnp.dot(p.astype(jnp.bfloat16), do, preferred_element_type=jnp.float32)
            new_k = jnp.dot(ds, q, preferred_element_type=jnp.float32) * scale
            if masked:
                dv_ref[b, kv, :] = new_v
                dk_ref[b, kv, :] = new_k
            else:
                dv_ref[b, kv, :] += new_v
                dk_ref[b, kv, :] += new_k
            dqt_scr[...] += jnp.dot(kt_scr[b, :, kv], ds, preferred_element_type=jnp.float32)

    def body(b, carry):
        step(b, False)
        return carry

    step(blk, True)
    lax.fori_loop(0, blk, body, 0)
    dq_ref[0] = dqt_scr[...].T * scale


def heads_to_rows(heads, tp_size, cp_size, o_in, o_out, ss, rs, loc):
    me_tp = lax.axis_index("tp")
    me_cp = lax.axis_index("cp")
    core = lax.rem(me_cp, 2)
    head = me_tp * heads + me_cp // 2
    sub = o_out.shape[1]
    group_barrier(me_tp, me_cp, tp_size, cp_size)
    for s in range(2):
        dst_tp = core if s == 0 else 3 - core
        for r in range(cp_size):
            dst_cp = lax.rem(me_cp + r, cp_size)
            src = o_in.at[dst_cp, pl.ds(s * sub, sub), :]
            if r == 0:
                own = dst_tp == me_tp

                @pl.when(own)
                def _():
                    pltpu.make_async_copy(src, o_out.at[head], rs.at[head]).start()

                @pl.when(jnp.logical_not(own))
                def _():
                    remote(src, o_out.at[head], ss.at[s, 0], rs.at[head], {"tp": dst_tp, "cp": dst_cp}).start()
            else:
                remote(src, o_out.at[head], ss.at[s, r], rs.at[head], {"tp": dst_tp, "cp": dst_cp}).start()
    for h in range(heads * tp_size):
        pltpu.make_async_copy(o_out.at[h], o_out.at[h], rs.at[h]).wait()
    for s in range(2):
        dst_tp = core if s == 0 else 3 - core
        for r in range(cp_size):
            wait = remote(o_in.at[0, pl.ds(0, sub), :], o_out.at[head], ss.at[s, r], rs.at[head], {"cp": me_cp})
            if r == 0:
                @pl.when(dst_tp != me_tp)
                def _():
                    wait.wait_send()
            else:
                wait.wait_send()


def rows_to_heads(heads, tp_size, cp_size, g_in, g_out, ss, rs, loc):
    me_tp = lax.axis_index("tp")
    me_cp = lax.axis_index("cp")
    core = lax.rem(me_cp, 2)
    sub = g_in.shape[1]
    row_core = jnp.where(me_tp < 2, me_tp, 3 - me_tp)
    row_slot = me_tp // 2
    group_barrier(me_tp, me_cp, tp_size, cp_size)
    for rt in range(tp_size):
        dst_tp = lax.rem(me_tp + rt, tp_size)
        for r in range(heads):
            dst_chip = lax.rem(me_cp // 2 + r, heads)
            dst_cp = dst_chip * 2 + row_core
            src = g_in.at[dst_tp * heads + dst_chip]
            dst = g_out.at[me_cp, pl.ds(row_slot * sub, sub), :]
            if rt == 0 and r == 0:
                @pl.when(row_core == core)
                def _():
                    pltpu.make_async_copy(src, dst, rs.at[me_cp, row_slot]).start()

                @pl.when(row_core != core)
                def _():
                    remote(src, dst, ss.at[rt, r], rs.at[me_cp, row_slot], {"tp": dst_tp, "cp": dst_cp}).start()
            else:
                remote(src, dst, ss.at[rt, r], rs.at[me_cp, row_slot], {"tp": dst_tp, "cp": dst_cp}).start()
    for i in range(cp_size):
        for s in range(2):
            part = g_out.at[i, pl.ds(s * sub, sub), :]
            pltpu.make_async_copy(part, part, rs.at[i, s]).wait()
    for rt in range(tp_size):
        for r in range(heads):
            wait = remote(g_in.at[0], g_out.at[0, pl.ds(0, sub), :], ss.at[rt, r], rs.at[0, 0], {"cp": me_cp})
            if rt == 0 and r == 0:
                @pl.when(row_core != core)
                def _():
                    wait.wait_send()
            else:
                wait.wait_send()


def gather_grads(heads, cp_size, dq_in, dk_in, dv_in, dq_out, dk_out, dv_out, pk, pv, sk, sv, loc, qs, qr, pks, pkr, pvs, pvr, ks, kr, vs, vr):
    me = lax.axis_index("cp")
    core = lax.rem(me, 2)
    chip = me // 2
    cp_barrier(me, cp_size)
    partner = {"cp": me + 1 - 2 * core}
    pair = []
    for x in range(heads):
        for src, dst, ss, rs in ((dk_in, pk, pks, pkr), (dv_in, pv, pvs, pvr)):
            copy = remote(src.at[2 * x + 1 - core], dst.at[x], ss.at[x], rs.at[x], partner)
            copy.start()
            pair.append(copy)
    sends = []
    for r in range(1, cp_size):
        dst = lax.rem(me + r, cp_size)
        copy = remote(dq_in.at[dst], dq_out.at[chip, core], qs.at[r], qr.at[r], {"cp": dst})
        copy.start()
        sends.append(copy)
    own = pltpu.make_async_copy(dq_in.at[me], dq_out.at[chip, core], loc.at[0])
    own.start()
    for x in range(heads):
        pair[2 * x].wait()
        pair[2 * x + 1].wait()
        sk[x] = dk_in[2 * x + core] + pk[x]
        sv[x] = (dv_in[2 * x + core] + pv[x]).astype(sv.dtype)
    for r in (1, heads - 1, 2):
        dst = lax.rem(chip + r, heads)
        for src, out, ss, rs in ((sk, dk_out, ks, kr), (sv, dv_out, vs, vr)):
            copy = remote(src.at[dst], out.at[chip], ss.at[r], rs.at[r], {"cp": dst * 2 + core})
            copy.start()
            sends.append(copy)
    locals_ = [pltpu.make_async_copy(sk.at[chip], dk_out.at[chip], loc.at[1]), pltpu.make_async_copy(sv.at[chip], dv_out.at[chip], loc.at[2])]
    for copy in locals_:
        copy.start()
    own.wait()
    for copy in locals_:
        copy.wait()
    for copy in sends:
        copy.wait_send()
    for r in range(1, cp_size):
        src = lax.rem(me - r + cp_size, cp_size)
        remote(dq_in.at[0], dq_out.at[src // 2, lax.rem(src, 2)], qs.at[r], qr.at[r], partner).wait_recv()
    for r in (1, heads - 1, 2):
        src = lax.rem(chip - r + heads, heads)
        remote(sk.at[0], dk_out.at[src], ks.at[r], kr.at[r], partner).wait_recv()
        remote(sv.at[0], dv_out.at[src], vs.at[r], vr.at[r], partner).wait_recv()


def sum_tp(tp_size, vec, out, got, ss, rs):
    me = lax.axis_index("tp")
    barrier = pltpu.get_barrier_semaphore()
    for r in range(1, tp_size):
        pl.semaphore_signal(barrier, inc=1, device_id={"tp": lax.rem(me + r, tp_size)}, device_id_type=MESH)
    pl.semaphore_wait(barrier, tp_size - 1)
    copies = []
    for r in range(1, tp_size):
        copy = remote(vec, got.at[r], ss.at[r], rs.at[r], {"tp": lax.rem(me + r, tp_size)})
        copy.start()
        copies.append(copy)
    for copy in copies:
        copy.wait()
    out[...] = (vec[...] + got[2]) + (got[1] + got[3])


def reduce_tail(tp_size, cp_size, n_heads, *refs):
    n_w = 4
    w_in, (dx_in, dy_in, small) = refs[:n_w], refs[n_w : n_w + 3]
    refs = refs[n_w + 3 :]
    w_out, (dx_out, small_out) = refs[:n_w], refs[n_w : n_w + 2]
    refs = refs[n_w + 2 :]
    acc, pair, far_a, far_b, fin_l, fin_r = (refs[i * n_w : (i + 1) * n_w] for i in range(6))
    refs = refs[6 * n_w :]
    dxa, dxb, dx_own, dx_fa, dx_fb, dx_fl, dx_fr, dx16, got_small, got_post, ss, rs, ps, pr, fs, fr, loc, sms, smr, gps, gpr = refs
    me_tp = lax.axis_index("tp")
    me_cp = lax.axis_index("cp")
    core = lax.rem(me_cp, 2)
    chip = me_cp // 2
    ring = cp_size // 2
    left, right, far = (lax.rem(chip + d, ring) for d in (ring - 1, 1, 2))
    t_left, t_right, t_far = (lax.rem(me_tp + d, tp_size) for d in (tp_size - 1, 1, 2))
    partner = {"cp": me_cp + 1 - 2 * core}
    to_l, to_r = {"cp": left * 2 + core}, {"cp": right * 2 + core}
    tp_l, tp_r = {"tp": t_left}, {"tp": t_right}
    dx_i = n_w

    barrier = pltpu.get_barrier_semaphore()
    for r in range(1, cp_size):
        pl.semaphore_signal(barrier, inc=1, device_id={"cp": lax.rem(me_cp + r, cp_size)}, device_id_type=MESH)
    for r in range(1, tp_size):
        pl.semaphore_signal(barrier, inc=1, device_id={"tp": lax.rem(me_tp + r, tp_size)}, device_id_type=MESH)
    pl.semaphore_wait(barrier, cp_size + tp_size - 2)

    sent = []

    def go(src, dst, s_sem, r_sem, device):
        copy = remote(src, dst, s_sem, r_sem, device)
        copy.start()
        sent.append(copy)

    def landed(dst, s_sem, r_sem):
        remote(dst, dst, s_sem, r_sem, partner).wait_recv()

    def piece(ref, t, x, c, part=None):
        size = w_in[t].shape[0] // cp_size
        first = (2 * x + c) * size
        if part is None:
            return ref.at[pl.ds(pl.multiple_of(first, size), size), :]
        return ref.at[pl.ds(pl.multiple_of(first + part * (size // 2), size // 2), size // 2), :]

    def rows_of(ref, y, part=None):
        size = dx_in.shape[0] // tp_size
        if part is None:
            return ref.at[pl.ds(pl.multiple_of(y * size, size), size), :]
        return ref.at[pl.ds(pl.multiple_of(y * size + part * (size // 2), size // 2), size // 2), :]

    def half_of(ref, part):
        size = ref.shape[0] // 2
        return ref.at[pl.ds(part * size, size), :]

    for r in range(1, cp_size):
        go(small, got_small.at[me_cp], sms.at[r], smr.at[r], {"cp": lax.rem(me_cp + r, cp_size)})
    go(rows_of(dx_in, t_far, 0), dx_fa, ss.at[dx_i, 0], rs.at[dx_i, 0], tp_l)
    go(rows_of(dx_in, t_far, 1), dx_fb, ss.at[dx_i, 1], rs.at[dx_i, 1], tp_r)
    go(rows_of(dx_in, t_left, 1), half_of(dx_fr, 1), ss.at[dx_i, 2], rs.at[dx_i, 2], tp_l)
    go(rows_of(dx_in, t_right, 0), half_of(dx_fl, 0), ss.at[dx_i, 3], rs.at[dx_i, 3], tp_r)
    order = (far, left, right, chip)
    loads = []
    for t in range(n_w):
        for i, x in enumerate(order):
            go(piece(w_in[t], t, x, 1 - core), pair[t].at[x], ps.at[t, i], pr.at[t, i], partner)
            copy = pltpu.make_async_copy(piece(w_in[t], t, x, core), acc[t].at[x], loc.at[t, i])
            copy.start()
            loads.append(copy)
    dx_loads = [
        pltpu.make_async_copy(rows_of(dx_in, t_left, 0), dxa, loc.at[n_w, 0]),
        pltpu.make_async_copy(rows_of(dx_in, t_right, 1), dxb, loc.at[n_w, 1]),
        pltpu.make_async_copy(rows_of(dx_in, me_tp), dx_own, loc.at[n_w, 2]),
    ]
    for copy in dx_loads:
        copy.start()

    for t in range(n_w):
        for i, x in enumerate(order):
            loads[t * 4 + i].wait()
            landed(pair[t].at[x], ps.at[t, i], pr.at[t, i])
            acc[t][x] += pair[t][x]
        go(half_of(acc[t].at[far], 0), far_a[t], ss.at[t, 0], rs.at[t, 0], to_l)
        go(half_of(acc[t].at[far], 1), far_b[t], ss.at[t, 1], rs.at[t, 1], to_r)
        go(half_of(acc[t].at[left], 1), half_of(fin_r[t], 1), ss.at[t, 2], rs.at[t, 2], to_l)
        go(half_of(acc[t].at[right], 0), half_of(fin_l[t], 0), ss.at[t, 3], rs.at[t, 3], to_r)

    got_small[me_cp] = small[...]
    for r in range(1, cp_size):
        landed(got_small.at[lax.rem(me_cp - r + cp_size, cp_size)], sms.at[r], smr.at[r])
    total = got_small[0]
    for i in range(1, cp_size):
        total = total + got_small[i]
    small_out[...] = total
    n_gain = small.shape[0] - got_post.shape[1]

    def second_half(t, acc_l, acc_r, fa, fb, fl, fr, dev_l, dev_r):
        half = fa.shape[0]
        landed(fa, ss.at[t, 0], rs.at[t, 0])
        acc_l[...] += fa[...]
        landed(fb, ss.at[t, 1], rs.at[t, 1])
        acc_r[...] += fb[...]
        go(acc_l, half_of(fr, 0), ss.at[t, 4], rs.at[t, 4], dev_l)
        go(acc_r, half_of(fl, 1), ss.at[t, 5], rs.at[t, 5], dev_r)

    def all_landed(t, fl, fr):
        landed(half_of(fr, 1), ss.at[t, 2], rs.at[t, 2])
        landed(half_of(fl, 0), ss.at[t, 3], rs.at[t, 3])
        landed(half_of(fr, 0), ss.at[t, 4], rs.at[t, 4])
        landed(half_of(fl, 1), ss.at[t, 5], rs.at[t, 5])

    for t in range(n_w):
        second_half(t, half_of(acc[t].at[left], 0), half_of(acc[t].at[right], 1), far_a[t], far_b[t], fin_l[t], fin_r[t], to_l, to_r)
    for copy in dx_loads:
        copy.wait()
    second_half(dx_i, dxa, dxb, dx_fa, dx_fb, dx_fl, dx_fr, tp_l, tp_r)
    post = small_out.at[pl.ds(n_gain, got_post.shape[1]), :]
    for r in range(1, tp_size):
        go(post, got_post.at[r], gps.at[r], gpr.at[r], {"tp": lax.rem(me_tp + r, tp_size)})

    outs = []
    for t in range(n_w):
        all_landed(t, fin_l[t], fin_r[t])
        acc[t][chip] = acc[t][chip] + (fin_l[t][...] + fin_r[t][...])
        src = acc[t].at[chip]
        dst = piece(w_out[t], t, chip, core)
        copy = pltpu.make_async_copy(src, dst, loc.at[t, 4])
        copy.start()
        outs.append(copy)
        go(src, dst, ss.at[t, 6], rs.at[t, 6], to_l)
        go(src, dst, ss.at[t, 7], rs.at[t, 7], to_r)
        go(src, dst, fs.at[t, 0], fr.at[t, 0], partner)
    all_landed(dx_i, dx_fl, dx_fr)
    dx16[...] = (dx_own[...] + (dx_fl[...] + dx_fr[...]) + dy_in[...].astype(jnp.float32)).astype(dx16.dtype)
    copy = pltpu.make_async_copy(dx16, rows_of(dx_out, me_tp), loc.at[n_w, 4])
    copy.start()
    outs.append(copy)
    go(dx16, rows_of(dx_out, me_tp), ss.at[dx_i, 6], rs.at[dx_i, 6], tp_l)
    go(dx16, rows_of(dx_out, me_tp), ss.at[dx_i, 7], rs.at[dx_i, 7], tp_r)

    for t in range(n_w):
        landed(piece(w_out[t], t, right, core), ss.at[t, 6], rs.at[t, 6])
        half = piece(w_out[t], t, right, core, 0)
        go(half, half, ss.at[t, 8], rs.at[t, 8], to_l)
        whole = piece(w_out[t], t, right, core)
        go(whole, whole, fs.at[t, 1], fr.at[t, 1], partner)
        landed(piece(w_out[t], t, left, core), ss.at[t, 7], rs.at[t, 7])
        half = piece(w_out[t], t, left, core, 1)
        go(half, half, ss.at[t, 9], rs.at[t, 9], to_r)
        whole = piece(w_out[t], t, left, core)
        go(whole, whole, fs.at[t, 2], fr.at[t, 2], partner)
    landed(rows_of(dx_out, t_right), ss.at[dx_i, 6], rs.at[dx_i, 6])
    half = rows_of(dx_out, t_right, 0)
    go(half, half, ss.at[dx_i, 8], rs.at[dx_i, 8], tp_l)
    landed(rows_of(dx_out, t_left), ss.at[dx_i, 7], rs.at[dx_i, 7])
    half = rows_of(dx_out, t_left, 1)
    go(half, half, ss.at[dx_i, 9], rs.at[dx_i, 9], tp_r)

    sums = small_out[n_gain:, :]
    for r in range(1, tp_size):
        landed(got_post.at[r], gps.at[r], gpr.at[r])
    sums = (sums + got_post[2]) + (got_post[1] + got_post[3])

    for t in range(n_w):
        for kind, part in ((8, 0), (9, 1)):
            half = piece(w_out[t], t, far, core, part)
            landed(half, ss.at[t, kind], rs.at[t, kind])
            go(half, half, fs.at[t, 3 + part], fr.at[t, 3 + part], partner)
    for kind, part in ((8, 0), (9, 1)):
        landed(rows_of(dx_out, t_far, part), ss.at[dx_i, kind], rs.at[dx_i, kind])
    for t in range(n_w):
        for i, x in enumerate((chip, right, left)):
            landed(piece(w_out[t], t, x, 1 - core), fs.at[t, i], fr.at[t, i])
        for part in range(2):
            landed(piece(w_out[t], t, far, 1 - core, part), fs.at[t, 3 + part], fr.at[t, 3 + part])
    for copy in outs:
        copy.wait()
    for copy in sent:
        copy.wait_send()
    small_out[n_gain:, :] = sums


def solution(mesh):
    tp_size = mesh.shape["tp"]
    cp_size = mesh.shape["cp"]
    act_spec = P("dp", "cp", None)
    col_spec = P(None, "tp", None)
    part_col = P("dp", "tp", None)
    in_specs = (act_spec, col_spec, col_spec, col_spec, P("tp", None, None), P("tp", None), P("tp", None), P(None), act_spec)
    out_specs = (act_spec, act_spec, part_col, part_col, part_col, P(("dp", "tp"), None, None), P(("dp", "tp"), None), P(("dp", "tp"), None), P("dp"))
    dma = pltpu.SemaphoreType.DMA

    def local_run(x_in, w_q, w_k, w_v, w_o, q_norm_w, k_norm_w, post_norm_w, grad_y):
        n_batch, block_len, d_model = x_in.shape
        heads, head_dim = w_q.shape[1:]
        assert n_batch == 1 and w_k.shape[1] == heads and cp_size == 2 * heads and tp_size == 4
        sub = block_len // tp_size
        rows = 2 * sub
        width = heads * head_dim * tp_size
        scale = head_dim ** -0.5
        f32 = jnp.float32
        b16 = jnp.bfloat16
        tp_index = lax.axis_index("tp")
        cp_index = lax.axis_index("cp")
        cos_tab, sin_tab = rope_tables(cp_index * block_len, block_len, head_dim)
        x_loc = x_in[0]
        dy_loc = grad_y[0]
        w_o_full = lax.all_gather(w_o, "tp", axis=0, tiled=True)

        q_lin = jnp.einsum("ld,dhe->hle", x_loc, w_q, preferred_element_type=f32)
        k_lin = jnp.einsum("ld,dhe->hle", x_loc, w_k, preferred_element_type=f32)
        v_lin = jnp.einsum("ld,dhe->hle", x_loc, w_v, preferred_element_type=f32)
        def tp_sum(q_part, k_part, cid):
            vec = jnp.stack([q_part, k_part]).reshape(-1, 128)
            out = vmem_call(
                functools.partial(sum_tp, tp_size),
                [jax.ShapeDtypeStruct(vec.shape, f32)],
                1,
                [VMEM((tp_size,) + vec.shape, f32), dma((tp_size,)), dma((tp_size,))],
                collective_id=cid,
            )(vec)[0]
            return out.reshape(2, -1)

        sq = tp_sum(jnp.sum(q_lin * q_lin, axis=(0, 2)), jnp.sum(k_lin * k_lin, axis=(0, 2)), 4)
        inv = lax.rsqrt(sq / width + NORM_EPS)
        q_inv = inv[0][None, :, None]
        k_inv = inv[1][None, :, None]
        q_rot = apply_rope(q_lin * q_inv * q_norm_w[:, None, :], cos_tab, sin_tab).astype(b16)
        k_rot = apply_rope(k_lin * k_inv * k_norm_w[:, None, :], cos_tab, sin_tab).astype(b16)
        v_val = v_lin.astype(b16)

        q4 = q_rot.reshape(heads, 4, sub, head_dim)
        q_send = jnp.stack([q4[:, 0], q4[:, 3], q4[:, 1], q4[:, 2]], axis=1).reshape(cp_size, rows, head_dim)
        q_all, k_all, v_all = vmem_call(
            functools.partial(scatter_qkv, heads, cp_size),
            [jax.ShapeDtypeStruct((cp_size, rows, head_dim), b16)] + [jax.ShapeDtypeStruct((cp_size, block_len, head_dim), b16)] * 2,
            3,
            [dma((3,)), dma((cp_size,)), dma((cp_size,))] + [dma((heads,))] * 8,
            collective_id=0,
        )(q_send, k_rot, v_val)

        qspec = pl.BlockSpec((1, rows, head_dim), lambda i: (i, 0, 0))
        lspec = pl.BlockSpec((1, 1, rows), lambda i: (i, 0, 0))
        whole = pl.BlockSpec(memory_space=VMEM)
        pair_flops = cp_size * (cp_size + 1) // 2 * rows * block_len * head_dim * 2
        o_all, lse = pl.pallas_call(
            functools.partial(attend, sub, scale),
            grid=(cp_size,),
            in_specs=[qspec, whole, whole],
            out_specs=[qspec, lspec],
            out_shape=[jax.ShapeDtypeStruct((cp_size, rows, head_dim), b16), jax.ShapeDtypeStruct((cp_size, 1, rows), f32)],
            scratch_shapes=[VMEM((cp_size, head_dim, block_len), b16), VMEM((1, rows), f32), VMEM((1, rows), f32), VMEM((head_dim, rows), f32)]
            + [VMEM((block_len // 2, rows), f32)] * 2 + [VMEM((1, rows), f32)],
            compiler_params=pltpu.CompilerParams(vmem_limit_bytes=48 << 20),
            cost_estimate=pl.CostEstimate(flops=2 * pair_flops, bytes_accessed=6 << 20, transcendentals=0),
        )(q_all, k_all, v_all)

        n_heads = heads * tp_size
        o_rows = vmem_call(
            functools.partial(heads_to_rows, heads, tp_size, cp_size),
            [jax.ShapeDtypeStruct((n_heads, sub, head_dim), b16)],
            1,
            [dma((2, cp_size)), dma((n_heads,)), dma((1,))],
            collective_id=1,
        )(o_all)[0]

        x_rows = lax.dynamic_slice_in_dim(x_loc, tp_index * sub, sub, 0)
        dy_rows = lax.dynamic_slice_in_dim(dy_loc, tp_index * sub, sub, 0).astype(f32)
        proj = jnp.einsum("hle,hed->ld", o_rows, w_o_full, preferred_element_type=f32)
        post_inv = lax.rsqrt(jnp.mean(proj * proj, axis=-1, keepdims=True) + NORM_EPS)
        post_hat = proj * post_inv
        y_rows = (x_rows + post_hat * post_norm_w).astype(b16)
        grad_post = jnp.sum(dy_rows * post_hat, axis=0)
        grad_hat = dy_rows * post_norm_w
        gp_rows = (post_inv * (grad_hat - post_hat * jnp.mean(grad_hat * post_hat, axis=-1, keepdims=True))).astype(b16)
        do_rows = jnp.einsum("ld,hed->hle", gp_rows, w_o_full, preferred_element_type=f32).astype(b16)

        do_all = vmem_call(
            functools.partial(rows_to_heads, heads, tp_size, cp_size),
            [jax.ShapeDtypeStruct((cp_size, rows, head_dim), b16)],
            1,
            [dma((tp_size, heads)), dma((cp_size, 2)), dma((1,))],
            collective_id=2,
        )(do_rows)[0]

        y_out = lax.all_gather(y_rows, "tp", axis=0, tiled=True)
        grad_proj = lax.all_gather(gp_rows, "tp", axis=0, tiled=True)
        o_gath = lax.all_gather(o_rows, "tp", axis=0)
        o_own = lax.dynamic_slice_in_dim(o_gath, tp_index * heads, heads, 1)

        dq_all, dk_all, dv_all = pl.pallas_call(
            functools.partial(attend_back, sub, scale),
            grid=(cp_size,),
            in_specs=[qspec, whole, whole, qspec, qspec, lspec],
            out_specs=[qspec, whole, whole],
            out_shape=[jax.ShapeDtypeStruct((cp_size, rows, head_dim), f32)] + [jax.ShapeDtypeStruct((cp_size, block_len, head_dim), f32)] * 2,
            scratch_shapes=[VMEM((cp_size, head_dim, block_len), b16), VMEM((head_dim, rows), f32), VMEM((1, rows), f32)],
            compiler_params=pltpu.CompilerParams(vmem_limit_bytes=48 << 20),
            cost_estimate=pl.CostEstimate(flops=5 * pair_flops, bytes_accessed=16 << 20, transcendentals=0),
        )(q_all, k_all, v_all, o_all, do_all, lse)

        grad_w_o = jnp.einsum("thle,tld->hed", o_own, grad_proj.reshape(tp_size, sub, d_model), preferred_element_type=f32)

        dq_home, dk_home, dv_home = vmem_call(
            functools.partial(gather_grads, heads, cp_size),
            [jax.ShapeDtypeStruct((heads, 2, rows, head_dim), f32), jax.ShapeDtypeStruct((heads, block_len, head_dim), f32), jax.ShapeDtypeStruct((heads, block_len, head_dim), b16)],
            3,
            [VMEM((heads, block_len, head_dim), f32)] * 3 + [VMEM((heads, block_len, head_dim), b16)]
            + [dma((3,)), dma((cp_size,)), dma((cp_size,))] + [dma((heads,))] * 8,
            collective_id=3,
        )(dq_all, dk_all, dv_all)
        dq5 = dq_home.reshape(heads, 4, sub, head_dim)
        dq_rot = jnp.stack([dq5[:, 0], dq5[:, 2], dq5[:, 3], dq5[:, 1]], axis=1).reshape(heads, block_len, head_dim)

        dq_s = rope_back(dq_rot, cos_tab, sin_tab)
        dk_s = rope_back(dk_home, cos_tab, sin_tab)
        q_hat = q_lin * q_inv
        k_hat = k_lin * k_inv
        grad_qn = jnp.sum(dq_s * q_hat, axis=1)
        grad_kn = jnp.sum(dk_s * k_hat, axis=1)
        dq_n = dq_s * q_norm_w[:, None, :]
        dk_n = dk_s * k_norm_w[:, None, :]
        dots = tp_sum(jnp.sum(dq_n * q_hat, axis=(0, 2)), jnp.sum(dk_n * k_hat, axis=(0, 2)), 5) / width
        dq16 = (q_inv * (dq_n - q_hat * dots[0][None, :, None])).astype(b16)
        dk16 = (k_inv * (dk_n - k_hat * dots[1][None, :, None])).astype(b16)
        grad_w_q = jnp.einsum("ld,hle->dhe", x_loc, dq16, preferred_element_type=f32)
        grad_w_k = jnp.einsum("ld,hle->dhe", x_loc, dk16, preferred_element_type=f32)
        grad_w_v = jnp.einsum("ld,hle->dhe", x_loc, dv_home, preferred_element_type=f32)
        dx_part = (jnp.einsum("hle,dhe->ld", dq16, w_q, preferred_element_type=f32)
                   + jnp.einsum("hle,dhe->ld", dk16, w_k, preferred_element_type=f32)
                   + jnp.einsum("hle,dhe->ld", dv_home, w_v, preferred_element_type=f32))
        w_parts = [grad_w_o.reshape(-1, d_model)] + [g.reshape(d_model, -1) for g in (grad_w_v, grad_w_q, grad_w_k)]
        small = jnp.concatenate([grad_qn, grad_kn, grad_post.reshape(-1, head_dim)], axis=0)
        any_spec = pl.BlockSpec(memory_space=pl.ANY)
        vmem_spec = pl.BlockSpec(memory_space=VMEM)

        def bufs(lead, div):
            return [VMEM(lead + (w.shape[0] // div, w.shape[1]), f32) for w in w_parts]

        ring = cp_size // 2
        rows_dx, half_dx = VMEM((sub, d_model), f32), VMEM((sub // 2, d_model), f32)
        res = pl.pallas_call(
            functools.partial(reduce_tail, tp_size, cp_size, heads),
            out_shape=[jax.ShapeDtypeStruct(w.shape, f32) for w in w_parts] + [jax.ShapeDtypeStruct((block_len, d_model), b16), jax.ShapeDtypeStruct(small.shape, f32)],
            in_specs=[any_spec] * 5 + [vmem_spec] * 2,
            out_specs=[any_spec] * 5 + [vmem_spec],
            scratch_shapes=bufs((ring,), cp_size) * 2 + bufs((), 2 * cp_size) * 2 + bufs((), cp_size) * 2
            + [half_dx, half_dx, rows_dx, half_dx, half_dx, rows_dx, rows_dx, VMEM((sub, d_model), b16)]
            + [VMEM((cp_size,) + small.shape, f32), VMEM((tp_size, d_model // head_dim, head_dim), f32)]
            + [dma((5, 10))] * 2 + [dma((4, 4))] * 2 + [dma((4, 5))] * 2 + [dma((5, 5))] + [dma((cp_size,))] * 2 + [dma((tp_size,))] * 2,
            compiler_params=pltpu.CompilerParams(vmem_limit_bytes=56 << 20, collective_id=6, has_side_effects=True),
        )(*w_parts, dx_part, dy_rows.astype(b16), small)
        grad_w_o, grad_w_v, grad_w_q, grad_w_k = (g.reshape(t.shape) for g, t in zip(res[:4], (grad_w_o, grad_w_v, grad_w_q, grad_w_k)))
        grad_x, small_sum = res[4:]
        grad_qn, grad_kn = small_sum[:heads], small_sum[heads : 2 * heads]
        return (y_out[None], grad_x[None], grad_w_q, grad_w_k, grad_w_v, grad_w_o, grad_qn, grad_kn, small_sum[2 * heads :].reshape(-1))

    return jax.shard_map(local_run, mesh=mesh, in_specs=in_specs, out_specs=out_specs, check_vma=False)
```

```python
import functools
import math

import jax
import jax.numpy as jnp
from jax import lax
from jax.experimental import pallas as pl
from jax.experimental.pallas import tpu as pltpu
from jax.sharding import PartitionSpec as P

ROPE_THETA = 500000.0
NORM_EPS = 1e-6
LOG2E = 1.4426950408889634
LIMIT = 56 << 20
LANES = 128
VMEM = pltpu.VMEM
MESH = pl.DeviceIdType.MESH
NT = (((1,), (1,)), ((), ()))


def rope_tables(start_pos, seq_rows, head_dim):
    half_dim = head_dim // 2
    lane = jnp.arange(head_dim)
    inv_freq = ROPE_THETA ** (-2.0 * (lane % half_dim).astype(jnp.float32) / head_dim)
    positions = (start_pos + jnp.arange(seq_rows)).astype(jnp.float32)
    angles = positions[:, None] * inv_freq[None, :]
    return jnp.cos(angles), jnp.where(lane < half_dim, -1.0, 1.0) * jnp.sin(angles)


def vmem_call(kernel, out_shape, n_in, scratch, collective_id=None, limit=LIMIT, cost=None):
    params = dict(vmem_limit_bytes=limit)
    if collective_id is not None:
        params.update(collective_id=collective_id, has_side_effects=True)
    return pl.pallas_call(
        kernel,
        out_shape=out_shape,
        in_specs=[pl.BlockSpec(memory_space=VMEM)] * n_in,
        out_specs=[pl.BlockSpec(memory_space=VMEM)] * len(out_shape),
        scratch_shapes=scratch,
        compiler_params=pltpu.CompilerParams(**params),
        cost_estimate=cost,
    )


def remote(src, dst, send_sem, recv_sem, device_id):
    return pltpu.make_async_remote_copy(src_ref=src, dst_ref=dst, send_sem=send_sem, recv_sem=recv_sem, device_id=device_id, device_id_type=MESH)


def cross_barrier(me_tp, me_cp, tp_size, cp_size):
    barrier = pltpu.get_barrier_semaphore()
    for axis, me, size in (("cp", me_cp, cp_size), ("tp", me_tp, tp_size)):
        for step in range(1, size):
            pl.semaphore_signal(barrier, inc=1, device_id={axis: lax.rem(me + step, size)}, device_id_type=MESH)
    pl.semaphore_wait(barrier, cp_size + tp_size - 2)


def cols(ref, head, rows=None):
    lanes = pl.ds(pl.multiple_of(head * LANES, LANES), LANES)
    return ref.at[:, lanes] if rows is None else ref.at[rows, lanes]


def sub_rows(core, slot, sub):
    first = core if slot == 0 else 3 - core
    return pl.ds(pl.multiple_of(first * sub, sub), sub)


def share_over_tp(tp_size, me, vec, got, ss, rs):
    copies = []
    for r in range(1, tp_size):
        copy = remote(vec, got.at[r], ss.at[r], rs.at[r], {"tp": lax.rem(me + r, tp_size)})
        copy.start()
        copies.append(copy)

    def finish():
        for copy in copies:
            copy.wait()
        return (vec[...] + got[2]) + (got[1] + got[3])

    return finish


def rolled(t, c, s):
    return t * c + pltpu.roll(t, LANES // 2, 1) * s


def group_barrier(me_tp, me_cp, tp_size, cp_size):
    barrier = pltpu.get_barrier_semaphore()
    for st in range(tp_size):
        for sc in range(cp_size):
            if st or sc:
                pl.semaphore_signal(barrier, inc=1, device_id={"tp": lax.rem(me_tp + st, tp_size), "cp": lax.rem(me_cp + sc, cp_size)}, device_id_type=MESH)
    pl.semaphore_wait(barrier, tp_size * cp_size - 1)


def scatter_qkv(heads, tp_size, cp_size, width, q_lin, k_lin, v_in, vec, q_gain, k_gain, cos_t, sin_t, q_out, k_out, v_out, inv_out, q16, k16, got, loc, qs, qr, ks, kr, vs, vr, fks, fkr, fvs, fvr, ts, tr):
    me_tp = lax.axis_index("tp")
    me = lax.axis_index("cp")
    core = lax.rem(me, 2)
    chip = me // 2
    sub = q_out.shape[1] // 2
    cross_barrier(me_tp, me, tp_size, cp_size)
    finish = share_over_tp(tp_size, me_tp, vec, got, ts, tr)
    far_chips = (1, heads - 1, 2)
    sends = []

    def spread(src, out, ss, rs):
        for r in far_chips:
            dst = lax.rem(chip + r, heads)
            copy = remote(cols(src, dst), out.at[me], ss.at[r], rs.at[r], {"cp": dst * 2 + core})
            copy.start()
            sends.append(copy)

    spread(v_in, v_out, vs, vr)
    inv_out[...] = lax.rsqrt(finish() / width + NORM_EPS)
    n_chunk = inv_out.shape[0] // 2
    inv_cols = inv_out[...].T

    def rotate(lin, gain, out16, first):
        for r in range(n_chunk):
            rows = slice(r * LANES, (r + 1) * LANES)
            scale = inv_cols[:, first + r : first + r + 1]
            for h in range(heads):
                lanes = slice(h * LANES, (h + 1) * LANES)
                out16[rows, lanes] = rolled(lin[rows, lanes] * scale * gain[:, lanes], cos_t[rows, :], sin_t[rows, :]).astype(out16.dtype)

    rotate(k_lin, k_gain, k16, n_chunk)
    spread(k16, k_out, ks, kr)
    rotate(q_lin, q_gain, q16, 0)
    own = [pltpu.make_async_copy(cols(k16, chip), k_out.at[me], loc.at[0]), pltpu.make_async_copy(cols(v_in, chip), v_out.at[me], loc.at[1])]
    for r in range(cp_size):
        dst = lax.rem(me + r, cp_size)
        for s in range(2):
            src = cols(q16, dst // 2, sub_rows(lax.rem(dst, 2), s, sub))
            place = q_out.at[me, s * sub : (s + 1) * sub, :]
            if r == 0:
                own.append(pltpu.make_async_copy(src, place, loc.at[2 + s]))
            else:
                copy = remote(src, place, qs.at[r, s], qr.at[r, s], {"cp": dst})
                copy.start()
                sends.append(copy)
    for copy in own:
        copy.start()
    partner = {"cp": me + 1 - 2 * core}
    forwards = []
    for r in (0,) + far_chips:
        src = lax.rem(chip - r + heads, heads) * 2 + core
        for i, (buf, ss, rs, fs, fr) in enumerate(((v_out, vs, vr, fvs, fvr), (k_out, ks, kr, fks, fkr))):
            if r == 0:
                own[1 - i].wait()
            else:
                remote(buf.at[src], buf.at[src], ss.at[r], rs.at[r], partner).wait_recv()
            copy = remote(buf.at[src], buf.at[src], fs.at[r], fr.at[r], partner)
            copy.start()
            forwards.append(copy)
    for copy in own[2:]:
        copy.wait()
    for copy in sends:
        copy.wait_send()
    for r in range(1, cp_size):
        for s in range(2):
            place = q_out.at[lax.rem(me - r + cp_size, cp_size), s * sub : (s + 1) * sub, :]
            remote(place, place, qs.at[r, s], qr.at[r, s], partner).wait_recv()
    for copy in forwards:
        copy.wait()


def attend(sub, scale, q_ref, k_ref, v_ref, o_ref, lse_ref, vt_scr, m_scr, l_scr, acc_scr, s_a, s_b, mx_a):
    blk = pl.program_id(0)
    core = lax.rem(lax.axis_index("cp"), 2)
    coef = scale * LOG2E
    half = k_ref.shape[1] // 2
    cols = q_ref.shape[1]
    chunk = half // 2
    vt_scr[blk] = v_ref[blk].T
    m_scr[...] = jnp.full_like(m_scr, -jnp.inf)
    l_scr[...] = jnp.zeros_like(l_scr)
    acc_scr[...] = jnp.zeros_like(acc_scr)

    def fold(op, values):
        return op(values.reshape(values.shape[0] // 8, 8, cols), axis=0)

    def scores(b, h, c):
        kv = slice(h * half + c * chunk, h * half + (c + 1) * chunk)
        return lax.dot_general(k_ref[b, kv, :], q_ref[0], NT, preferred_element_type=jnp.float32)

    def mask(s, h, c):
        kv_pos = h * half + c * chunk + lax.broadcasted_iota(jnp.int32, s.shape, 0)
        col = lax.broadcasted_iota(jnp.int32, s.shape, 1)
        q_pos = jnp.where(col < sub, core * sub + col, (2 - core) * sub + col)
        return jnp.where(kv_pos <= q_pos, s, -jnp.inf)

    def step(buf, mx, b, h, nxt):
        m_old = m_scr[...]
        m_new = jnp.maximum(m_old, mx)
        mc = m_new * coef
        alpha = jnp.exp2((m_old - m_new) * coef)
        lsum = jnp.zeros((8, cols), jnp.float32)
        new_mx = None
        for c in range(2):
            rows = slice(c * chunk, (c + 1) * chunk)
            if nxt is not None:
                nbuf, nb, nh, masked = nxt
                s = scores(nb, nh, c)
                if masked:
                    s = mask(s, nh, c)
                nbuf[rows, :] = s
                part = fold(jnp.max, s)
                new_mx = part if new_mx is None else jnp.maximum(new_mx, part)
            p = jnp.exp2(buf[rows, :] * coef - mc)
            lsum = lsum + fold(jnp.sum, p)
            pv = jnp.dot(vt_scr[b, :, h * half + c * chunk : h * half + (c + 1) * chunk], p.astype(jnp.bfloat16), preferred_element_type=jnp.float32)
            acc_scr[...] = acc_scr[...] * alpha + pv if c == 0 else acc_scr[...] + pv
        l_scr[...] = l_scr[...] * alpha + jnp.sum(lsum, axis=0, keepdims=True)
        m_scr[...] = m_new
        return None if nxt is None else jnp.max(new_mx, axis=0, keepdims=True)

    for c in range(2):
        s_a[c * chunk : (c + 1) * chunk, :] = scores(0, 0, c)
    mx_a[...] = jnp.max(s_a[...], axis=0, keepdims=True)

    def body(b, carry):
        mx_b = step(s_a, mx_a[...], b, 0, (s_b, b, 1, False))
        mx_a[...] = step(s_b, mx_b, b, 1, (s_a, b + 1, 0, False))
        return carry

    lax.fori_loop(0, blk, body, 0)
    for c in range(2):
        rows = slice(c * chunk, (c + 1) * chunk)
        s_a[rows, :] = mask(s_a[rows, :], 0, c)
    mx_b = step(s_a, jnp.max(s_a[...], axis=0, keepdims=True), blk, 0, (s_b, blk, 1, True))
    step(s_b, mx_b, blk, 1, None)
    o_ref[0] = (acc_scr[...] / l_scr[...]).T.astype(o_ref.dtype)
    lse_ref[0] = m_scr[...] * coef + jnp.log2(l_scr[...])


def attend_back(sub, scale, q_ref, k_ref, v_ref, o_ref, do_ref, lse_ref, dq_ref, dk_ref, dv_ref, kt_scr, dqt_scr, dl_scr):
    blk = pl.program_id(0)
    core = lax.rem(lax.axis_index("cp"), 2)
    coef = scale * LOG2E
    rows = q_ref.shape[1]
    block_len = k_ref.shape[1]
    kt_scr[blk] = k_ref[blk].T
    prod = o_ref[0].astype(jnp.float32) * do_ref[0].astype(jnp.float32)
    dl_scr[...] = jnp.sum(prod.T, axis=0, keepdims=True)
    dqt_scr[...] = jnp.zeros_like(dqt_scr)

    def step(b, masked):
        q = q_ref[0]
        do = do_ref[0]
        lse = lse_ref[0]
        delta = dl_scr[...]
        for part in range(block_len // sub):
            kv = slice(part * sub, (part + 1) * sub)
            k_blk = k_ref[b, kv, :]
            s = lax.dot_general(k_blk, q, NT, preferred_element_type=jnp.float32)
            p = jnp.exp2(s * coef - lse)
            if masked:
                kv_pos = part * sub + lax.broadcasted_iota(jnp.int32, (sub, rows), 0)
                col = lax.broadcasted_iota(jnp.int32, (sub, rows), 1)
                q_pos = jnp.where(col < sub, core * sub + col, (2 - core) * sub + col)
                p = jnp.where(kv_pos <= q_pos, p, 0.0)
            dp = lax.dot_general(v_ref[b, kv, :], do, NT, preferred_element_type=jnp.float32)
            ds = (p * (dp - delta)).astype(jnp.bfloat16)
            new_v = jnp.dot(p.astype(jnp.bfloat16), do, preferred_element_type=jnp.float32)
            new_k = jnp.dot(ds, q, preferred_element_type=jnp.float32) * scale
            if masked:
                dv_ref[b, kv, :] = new_v
                dk_ref[b, kv, :] = new_k
            else:
                dv_ref[b, kv, :] += new_v
                dk_ref[b, kv, :] += new_k
            dqt_scr[...] += jnp.dot(kt_scr[b, :, kv], ds, preferred_element_type=jnp.float32)

    def body(b, carry):
        step(b, False)
        return carry

    step(blk, True)
    lax.fori_loop(0, blk, body, 0)
    dq_ref[0] = dqt_scr[...].T * scale


def heads_to_rows(heads, tp_size, cp_size, o_in, o_out, ss, rs):
    me_tp = lax.axis_index("tp")
    me_cp = lax.axis_index("cp")
    core = lax.rem(me_cp, 2)
    head = me_tp * heads + me_cp // 2
    sub = o_out.shape[0]
    place = cols(o_out, head)
    group_barrier(me_tp, me_cp, tp_size, cp_size)
    for finish in range(2):
        if finish:
            for h in range(heads * tp_size):
                part = o_out.at[:, h * LANES : (h + 1) * LANES]
                pltpu.make_async_copy(part, part, rs.at[h]).wait()
        for s in range(2):
            dst_tp = core if s == 0 else 3 - core
            for r in range(cp_size):
                dst_cp = lax.rem(me_cp + r, cp_size)
                src = o_in.at[dst_cp, s * sub : (s + 1) * sub, :]
                copy = remote(src, place, ss.at[s, r], rs.at[head], {"tp": dst_tp, "cp": dst_cp})
                act = copy.wait_send if finish else copy.start
                if r:
                    act()
                    continue
                pl.when(dst_tp != me_tp)(act)
                if not finish:
                    pl.when(dst_tp == me_tp)(pltpu.make_async_copy(src, place, rs.at[head]).start)


def rows_to_heads(heads, tp_size, cp_size, g_in, g_out, ss, rs):
    me_tp = lax.axis_index("tp")
    me_cp = lax.axis_index("cp")
    core = lax.rem(me_cp, 2)
    sub = g_in.shape[0]
    row_core = jnp.where(me_tp < 2, me_tp, 3 - me_tp)
    slot = me_tp // 2
    place = g_out.at[me_cp, pl.ds(pl.multiple_of(slot * sub, sub), sub), :]
    group_barrier(me_tp, me_cp, tp_size, cp_size)
    for finish in range(2):
        if finish:
            for i in range(cp_size):
                for s in range(2):
                    part = g_out.at[i, s * sub : (s + 1) * sub, :]
                    pltpu.make_async_copy(part, part, rs.at[i, s]).wait()
        for rt in range(tp_size):
            dst_tp = lax.rem(me_tp + rt, tp_size)
            for r in range(heads):
                chip = lax.rem(me_cp // 2 + r, heads)
                src = cols(g_in, dst_tp * heads + chip)
                copy = remote(src, place, ss.at[rt, r], rs.at[me_cp, slot], {"tp": dst_tp, "cp": chip * 2 + row_core})
                act = copy.wait_send if finish else copy.start
                if rt or r:
                    act()
                    continue
                pl.when(row_core != core)(act)
                if not finish:
                    pl.when(row_core == core)(pltpu.make_async_copy(src, place, rs.at[me_cp, slot]).start)


def gather_grads(heads, tp_size, cp_size, width, dq_in, dk_in, dv_in, q_lin, k_lin, inv, q_gain, k_gain, cos_t, sin_t, dq_out, dk_out, dv_out, gain_out, dq, dk, pk, pv, sk, sv, part, got, loc, qs, qr, pks, pkr, pvs, pvr, ks, kr, vs, vr, ts, tr):
    me_tp = lax.axis_index("tp")
    me = lax.axis_index("cp")
    core = lax.rem(me, 2)
    chip = me // 2
    sub = dq_in.shape[1] // 2
    cross_barrier(me_tp, me, tp_size, cp_size)
    partner = {"cp": me + 1 - 2 * core}
    order = (1, heads - 1, 2, 0)
    pair, sends, own = [], [], []
    for i, r in enumerate(order):
        x = lax.rem(chip + r, heads)
        for src, dst, ss, rs in ((dk_in, pk, pks, pkr), (dv_in, pv, pvs, pvr)):
            copy = remote(src.at[2 * x + 1 - core], dst.at[x], ss.at[i], rs.at[i], partner)
            copy.start()
            pair.append(copy)
    for r in range(cp_size):
        dst = lax.rem(me + r, cp_size)
        for s in range(2):
            src = dq_in.at[dst, s * sub : (s + 1) * sub, :]
            place = cols(dq, chip, sub_rows(core, s, sub))
            if r == 0:
                own.append(pltpu.make_async_copy(src, place, loc.at[s]))
                own[s].start()
            else:
                copy = remote(src, place, qs.at[r, s], qr.at[r, s], {"cp": dst})
                copy.start()
                sends.append(copy)
    for i, r in enumerate(order):
        x = lax.rem(chip + r, heads)
        pair[2 * i].wait()
        pair[2 * i + 1].wait()
        sk[x] = dk_in[2 * x + core] + pk[x]
        sv[x] = (dv_in[2 * x + core] + pv[x]).astype(sv.dtype)
        for j, (src, out, ss, rs) in enumerate(((sk, dk, ks, kr), (sv, dv_out, vs, vr))):
            if r == 0:
                copy = pltpu.make_async_copy(src.at[x], cols(out, chip), loc.at[2 + j])
                own.append(copy)
            else:
                copy = remote(src.at[x], cols(out, chip), ss.at[r], rs.at[r], {"cp": x * 2 + core})
                sends.append(copy)
            copy.start()
    for copy in own:
        copy.wait()
    for r in range(1, cp_size):
        src = lax.rem(me - r + cp_size, cp_size)
        for s in range(2):
            place = cols(dq, src // 2, sub_rows(lax.rem(src, 2), s, sub))
            remote(place, place, qs.at[r, s], qr.at[r, s], partner).wait_recv()
    inv_cols = inv[...].T
    n_chunk = inv.shape[0] // 2
    dots = []

    def first_pass(i, grad, lin, gain):
        gains = [jnp.zeros((1, LANES), jnp.float32)] * heads
        for r in range(n_chunk):
            rows = slice(r * LANES, (r + 1) * LANES)
            scale = inv_cols[:, i * n_chunk + r : i * n_chunk + r + 1]
            total = jnp.zeros((LANES, LANES), jnp.float32)
            for h in range(heads):
                lanes = slice(h * LANES, (h + 1) * LANES)
                hat = lin[rows, lanes] * scale
                back = rolled(grad[rows, lanes], cos_t[rows, :], -sin_t[rows, :])
                both = back * hat
                gains[h] = gains[h] + jnp.sum(both, axis=0, keepdims=True)
                total = total + both * gain[:, lanes]
                grad[rows, lanes] = back * gain[:, lanes]
            dots.append(jnp.sum(total, axis=1, keepdims=True))
        for h in range(heads):
            gain_out[i * heads + h : i * heads + h + 1, :] = gains[h]

    first_pass(0, dq, q_lin, q_gain)
    for r in order[:-1]:
        place = cols(dk, lax.rem(chip - r + heads, heads))
        remote(place, place, ks.at[r], kr.at[r], partner).wait_recv()
    first_pass(1, dk, k_lin, k_gain)
    part[...] = jnp.concatenate(dots, axis=1).T
    total_dots = share_over_tp(tp_size, me_tp, part, got, ts, tr)() / width
    dot_cols = total_dots.T
    for i, (grad, lin, out) in enumerate(((dq, q_lin, dq_out), (dk, k_lin, dk_out))):
        for r in range(n_chunk):
            rows = slice(r * LANES, (r + 1) * LANES)
            c = i * n_chunk + r
            scale = inv_cols[:, c : c + 1]
            out[rows, :] = (scale * (grad[rows, :] - lin[rows, :] * scale * dot_cols[:, c : c + 1])).astype(out.dtype)
    for copy in sends:
        copy.wait_send()
    for r in order[:-1]:
        place = cols(dv_out, lax.rem(chip - r + heads, heads))
        remote(place, place, vs.at[r], vr.at[r], partner).wait_recv()


def reduce_tail(tp_size, cp_size, n_heads, *refs):
    n_w = 4
    w_in, (dx_in, dy_in, small) = refs[:n_w], refs[n_w : n_w + 3]
    refs = refs[n_w + 3 :]
    w_out, (dx_out, small_out) = refs[:n_w], refs[n_w : n_w + 2]
    refs = refs[n_w + 2 :]
    acc, pair, far_a, far_b, fin_l, fin_r = (refs[i * n_w : (i + 1) * n_w] for i in range(6))
    refs = refs[6 * n_w :]
    dxa, dxb, dx_own, dx_fa, dx_fb, dx_fl, dx_fr, dx16, got_small, got_post, ss, rs, ps, pr, fs, fr, loc, sms, smr, gps, gpr = refs
    me_tp = lax.axis_index("tp")
    me_cp = lax.axis_index("cp")
    core = lax.rem(me_cp, 2)
    chip = me_cp // 2
    ring = cp_size // 2
    left, right, far = (lax.rem(chip + d, ring) for d in (ring - 1, 1, 2))
    t_left, t_right, t_far = (lax.rem(me_tp + d, tp_size) for d in (tp_size - 1, 1, 2))
    partner = {"cp": me_cp + 1 - 2 * core}
    to_l, to_r = {"cp": left * 2 + core}, {"cp": right * 2 + core}
    tp_l, tp_r = {"tp": t_left}, {"tp": t_right}
    dx_i = n_w

    def ring_sems(t, kind):
        return ss.at[t, kind], rs.at[t, kind]

    def pair_sems(t, kind):
        return fs.at[t, kind], fr.at[t, kind]

    cross_barrier(me_tp, me_cp, tp_size, cp_size)
    sent = []

    def go(src, dst, s_sem, r_sem, device):
        copy = remote(src, dst, s_sem, r_sem, device)
        copy.start()
        sent.append(copy)

    def landed(dst, s_sem, r_sem):
        remote(dst, dst, s_sem, r_sem, partner).wait_recv()

    def piece(ref, t, x, c, part=None):
        size = w_in[t].shape[0] // cp_size
        first = (2 * x + c) * size
        if part is None:
            return ref.at[pl.ds(pl.multiple_of(first, size), size), :]
        return ref.at[pl.ds(pl.multiple_of(first + part * (size // 2), size // 2), size // 2), :]

    def rows_of(ref, y, part=None):
        size = dx_in.shape[0] // tp_size
        if part is None:
            return ref.at[pl.ds(pl.multiple_of(y * size, size), size), :]
        return ref.at[pl.ds(pl.multiple_of(y * size + part * (size // 2), size // 2), size // 2), :]

    def half_of(ref, part):
        size = ref.shape[0] // 2
        return ref.at[pl.ds(part * size, size), :]

    for r in range(1, cp_size):
        go(small, got_small.at[me_cp], sms.at[r], smr.at[r], {"cp": lax.rem(me_cp + r, cp_size)})
    go(rows_of(dx_in, t_far, 0), dx_fa, *ring_sems(dx_i, 0), tp_l)
    go(rows_of(dx_in, t_far, 1), dx_fb, *ring_sems(dx_i, 1), tp_r)
    go(rows_of(dx_in, t_left, 1), half_of(dx_fr, 1), *ring_sems(dx_i, 2), tp_l)
    go(rows_of(dx_in, t_right, 0), half_of(dx_fl, 0), *ring_sems(dx_i, 3), tp_r)
    order = (far, left, right, chip)
    loads = []
    for t in range(n_w):
        for i, x in enumerate(order):
            go(piece(w_in[t], t, x, 1 - core), pair[t].at[x], ps.at[t, i], pr.at[t, i], partner)
            copy = pltpu.make_async_copy(piece(w_in[t], t, x, core), acc[t].at[x], loc.at[t, i])
            copy.start()
            loads.append(copy)
    dx_loads = [
        pltpu.make_async_copy(rows_of(dx_in, t_left, 0), dxa, loc.at[n_w, 0]),
        pltpu.make_async_copy(rows_of(dx_in, t_right, 1), dxb, loc.at[n_w, 1]),
        pltpu.make_async_copy(rows_of(dx_in, me_tp), dx_own, loc.at[n_w, 2]),
    ]
    for copy in dx_loads:
        copy.start()

    for t in range(n_w):
        for i, x in enumerate(order):
            loads[t * 4 + i].wait()
            landed(pair[t].at[x], ps.at[t, i], pr.at[t, i])
            acc[t][x] += pair[t][x]
        go(half_of(acc[t].at[far], 0), far_a[t], *ring_sems(t, 0), to_l)
        go(half_of(acc[t].at[far], 1), far_b[t], *ring_sems(t, 1), to_r)
        go(half_of(acc[t].at[left], 1), half_of(fin_r[t], 1), *ring_sems(t, 2), to_l)
        go(half_of(acc[t].at[right], 0), half_of(fin_l[t], 0), *ring_sems(t, 3), to_r)

    got_small[me_cp] = small[...]
    for r in range(1, cp_size):
        landed(got_small.at[lax.rem(me_cp - r + cp_size, cp_size)], sms.at[r], smr.at[r])
    total = got_small[0]
    for i in range(1, cp_size):
        total = total + got_small[i]
    small_out[...] = total
    n_gain = small.shape[0] - got_post.shape[1]

    def second_half(t, acc_l, acc_r, fa, fb, fl, fr, dev_l, dev_r):
        half = fa.shape[0]
        landed(fa, *ring_sems(t, 0))
        acc_l[...] += fa[...]
        landed(fb, *ring_sems(t, 1))
        acc_r[...] += fb[...]
        go(acc_l, half_of(fr, 0), *ring_sems(t, 4), dev_l)
        go(acc_r, half_of(fl, 1), *ring_sems(t, 5), dev_r)

    def all_landed(t, fl, fr):
        landed(half_of(fr, 1), *ring_sems(t, 2))
        landed(half_of(fl, 0), *ring_sems(t, 3))
        landed(half_of(fr, 0), *ring_sems(t, 4))
        landed(half_of(fl, 1), *ring_sems(t, 5))

    for t in range(n_w):
        second_half(t, half_of(acc[t].at[left], 0), half_of(acc[t].at[right], 1), far_a[t], far_b[t], fin_l[t], fin_r[t], to_l, to_r)
    for copy in dx_loads:
        copy.wait()
    second_half(dx_i, dxa, dxb, dx_fa, dx_fb, dx_fl, dx_fr, tp_l, tp_r)
    post = small_out.at[pl.ds(n_gain, got_post.shape[1]), :]
    for r in range(1, tp_size):
        go(post, got_post.at[r], gps.at[r], gpr.at[r], {"tp": lax.rem(me_tp + r, tp_size)})

    outs = []
    for t in range(n_w):
        all_landed(t, fin_l[t], fin_r[t])
        acc[t][chip] = acc[t][chip] + (fin_l[t][...] + fin_r[t][...])
        src = acc[t].at[chip]
        dst = piece(w_out[t], t, chip, core)
        copy = pltpu.make_async_copy(src, dst, loc.at[t, 4])
        copy.start()
        outs.append(copy)
        go(src, dst, *ring_sems(t, 6), to_l)
        go(src, dst, *ring_sems(t, 7), to_r)
        go(src, dst, *pair_sems(t, 0), partner)
    all_landed(dx_i, dx_fl, dx_fr)
    dx16[...] = (dx_own[...] + (dx_fl[...] + dx_fr[...]) + dy_in[...].astype(jnp.float32)).astype(dx16.dtype)
    copy = pltpu.make_async_copy(dx16, rows_of(dx_out, me_tp), loc.at[n_w, 4])
    copy.start()
    outs.append(copy)
    go(dx16, rows_of(dx_out, me_tp), *ring_sems(dx_i, 6), tp_l)
    go(dx16, rows_of(dx_out, me_tp), *ring_sems(dx_i, 7), tp_r)

    for t in range(n_w):
        landed(piece(w_out[t], t, right, core), *ring_sems(t, 6))
        half = piece(w_out[t], t, right, core, 0)
        go(half, half, *ring_sems(t, 8), to_l)
        whole = piece(w_out[t], t, right, core)
        go(whole, whole, *pair_sems(t, 1), partner)
        landed(piece(w_out[t], t, left, core), *ring_sems(t, 7))
        half = piece(w_out[t], t, left, core, 1)
        go(half, half, *ring_sems(t, 9), to_r)
        whole = piece(w_out[t], t, left, core)
        go(whole, whole, *pair_sems(t, 2), partner)
    landed(rows_of(dx_out, t_right), *ring_sems(dx_i, 6))
    half = rows_of(dx_out, t_right, 0)
    go(half, half, *ring_sems(dx_i, 8), tp_l)
    landed(rows_of(dx_out, t_left), *ring_sems(dx_i, 7))
    half = rows_of(dx_out, t_left, 1)
    go(half, half, *ring_sems(dx_i, 9), tp_r)

    sums = small_out[n_gain:, :]
    for r in range(1, tp_size):
        landed(got_post.at[r], gps.at[r], gpr.at[r])
    sums = (sums + got_post[2]) + (got_post[1] + got_post[3])

    for t in range(n_w):
        for kind, part in ((8, 0), (9, 1)):
            half = piece(w_out[t], t, far, core, part)
            landed(half, *ring_sems(t, kind))
            go(half, half, *pair_sems(t, 3 + part), partner)
    for kind, part in ((8, 0), (9, 1)):
        landed(rows_of(dx_out, t_far, part), *ring_sems(dx_i, kind))
    for t in range(n_w):
        for i, x in enumerate((chip, right, left)):
            landed(piece(w_out[t], t, x, 1 - core), *pair_sems(t, i))
        for part in range(2):
            landed(piece(w_out[t], t, far, 1 - core, part), *pair_sems(t, 3 + part))
    for copy in outs:
        copy.wait()
    for copy in sent:
        copy.wait_send()
    small_out[n_gain:, :] = sums


def solution(mesh):
    tp_size = mesh.shape["tp"]
    cp_size = mesh.shape["cp"]
    act_spec = P("dp", "cp", None)
    col_spec = P(None, "tp", None)
    part_col = P("dp", "tp", None)
    in_specs = (act_spec, col_spec, col_spec, col_spec, P("tp", None, None), P("tp", None), P("tp", None), P(None), act_spec)
    out_specs = (act_spec, act_spec, part_col, part_col, part_col, P(("dp", "tp"), None, None), P(("dp", "tp"), None), P(("dp", "tp"), None), P("dp"))
    dma = pltpu.SemaphoreType.DMA

    def local_run(x_in, w_q, w_k, w_v, w_o, q_norm_w, k_norm_w, post_norm_w, grad_y):
        n_batch, block_len, d_model = x_in.shape
        heads, head_dim = w_q.shape[1:]
        assert n_batch == 1 and w_k.shape[1] == heads and cp_size == 2 * heads and tp_size == 4
        sub = block_len // tp_size
        rows = 2 * sub
        width = heads * head_dim * tp_size
        scale = head_dim ** -0.5
        f32 = jnp.float32
        b16 = jnp.bfloat16
        tp_index = lax.axis_index("tp")
        cp_index = lax.axis_index("cp")
        cos_tab, sin_tab = rope_tables(cp_index * block_len, block_len, head_dim)
        x_loc = x_in[0]
        dy_loc = grad_y[0]
        w_o_full = lax.all_gather(w_o.reshape(-1, d_model), "tp", axis=0, tiled=True)
        w_q2, w_k2, w_v2 = (w.reshape(d_model, -1) for w in (w_q, w_k, w_v))
        gains = [g.reshape(1, -1) for g in (q_norm_w, k_norm_w)]
        loc_width = heads * head_dim

        q_lin = jnp.dot(x_loc, w_q2, preferred_element_type=f32)
        k_lin = jnp.dot(x_loc, w_k2, preferred_element_type=f32)
        v_val = jnp.dot(x_loc, w_v2, preferred_element_type=f32).astype(b16)
        vec = jnp.stack([jnp.sum(t * t, axis=1) for t in (q_lin, k_lin)]).reshape(-1, LANES)
        vec_shape = jax.ShapeDtypeStruct(vec.shape, f32)
        kv_shape = jax.ShapeDtypeStruct((cp_size, block_len, head_dim), b16)
        lin16 = VMEM((block_len, loc_width), b16)
        tp_scratch = VMEM((tp_size,) + vec.shape, f32)
        q_all, k_all, v_all, inv = vmem_call(
            functools.partial(scatter_qkv, heads, tp_size, cp_size, width),
            [jax.ShapeDtypeStruct((cp_size, rows, head_dim), b16), kv_shape, kv_shape, vec_shape],
            8,
            [lin16, lin16, tp_scratch, dma((4,))] + [dma((cp_size, 2))] * 2 + [dma((heads,))] * 8 + [dma((tp_size,))] * 2,
            collective_id=0,
        )(q_lin, k_lin, v_val, vec, *gains, cos_tab, sin_tab)

        qspec = pl.BlockSpec((1, rows, head_dim), lambda i: (i, 0, 0))
        lspec = pl.BlockSpec((1, 1, rows), lambda i: (i, 0, 0))
        whole = pl.BlockSpec(memory_space=VMEM)
        pair_flops = cp_size * (cp_size + 1) // 2 * rows * block_len * head_dim * 2
        o_all, lse = pl.pallas_call(
            functools.partial(attend, sub, scale),
            grid=(cp_size,),
            in_specs=[qspec, whole, whole],
            out_specs=[qspec, lspec],
            out_shape=[jax.ShapeDtypeStruct((cp_size, rows, head_dim), b16), jax.ShapeDtypeStruct((cp_size, 1, rows), f32)],
            scratch_shapes=[VMEM((cp_size, head_dim, block_len), b16), VMEM((1, rows), f32), VMEM((1, rows), f32), VMEM((head_dim, rows), f32)]
            + [VMEM((block_len // 2, rows), f32)] * 2 + [VMEM((1, rows), f32)],
            compiler_params=pltpu.CompilerParams(vmem_limit_bytes=LIMIT),
            cost_estimate=pl.CostEstimate(flops=2 * pair_flops, bytes_accessed=6 << 20, transcendentals=0),
        )(q_all, k_all, v_all)

        n_heads = heads * tp_size
        o_rows = vmem_call(
            functools.partial(heads_to_rows, heads, tp_size, cp_size),
            [jax.ShapeDtypeStruct((sub, width), b16)],
            1,
            [dma((2, cp_size)), dma((n_heads,))],
            collective_id=1,
        )(o_all)[0]

        x_rows = lax.dynamic_slice_in_dim(x_loc, tp_index * sub, sub, 0)
        dy_rows = lax.dynamic_slice_in_dim(dy_loc, tp_index * sub, sub, 0)
        dy_f = dy_rows.astype(f32)
        proj = jnp.dot(o_rows, w_o_full, preferred_element_type=f32)
        post_inv = lax.rsqrt(jnp.mean(proj * proj, axis=-1, keepdims=True) + NORM_EPS)
        post_hat = proj * post_inv
        y_rows = (x_rows + post_hat * post_norm_w).astype(b16)
        grad_post = jnp.sum(dy_f * post_hat, axis=0)
        grad_hat = dy_f * post_norm_w
        gp_rows = (post_inv * (grad_hat - post_hat * jnp.mean(grad_hat * post_hat, axis=-1, keepdims=True))).astype(b16)
        do_rows = lax.dot_general(gp_rows, w_o_full, NT, preferred_element_type=f32).astype(b16)

        do_all = vmem_call(
            functools.partial(rows_to_heads, heads, tp_size, cp_size),
            [jax.ShapeDtypeStruct((cp_size, rows, head_dim), b16)],
            1,
            [dma((tp_size, heads)), dma((cp_size, 2))],
            collective_id=2,
        )(do_rows)[0]

        grad_proj = lax.all_gather(gp_rows, "tp", axis=0, tiled=True)
        o_gath = lax.all_gather(o_rows, "tp", axis=0, tiled=True)
        y_out = lax.all_gather(y_rows, "tp", axis=0, tiled=True)

        dq_all, dk_all, dv_all = pl.pallas_call(
            functools.partial(attend_back, sub, scale),
            grid=(cp_size,),
            in_specs=[qspec, whole, whole, qspec, qspec, lspec],
            out_specs=[qspec, whole, whole],
            out_shape=[jax.ShapeDtypeStruct((cp_size, rows, head_dim), f32)] + [jax.ShapeDtypeStruct((cp_size, block_len, head_dim), f32)] * 2,
            scratch_shapes=[VMEM((cp_size, head_dim, block_len), b16), VMEM((head_dim, rows), f32), VMEM((1, rows), f32)],
            compiler_params=pltpu.CompilerParams(vmem_limit_bytes=LIMIT),
            cost_estimate=pl.CostEstimate(flops=5 * pair_flops, bytes_accessed=16 << 20, transcendentals=0),
        )(q_all, k_all, v_all, o_all, do_all, lse)

        dq_all, grad_proj, o_gath = lax.optimization_barrier((dq_all, grad_proj, o_gath))
        lin_f, lin_h = VMEM((block_len, loc_width), f32), jax.ShapeDtypeStruct((block_len, loc_width), b16)
        head_f = VMEM((heads, block_len, head_dim), f32)
        dq16, dk16, dv16, gain_grads = vmem_call(
            functools.partial(gather_grads, heads, tp_size, cp_size, width),
            [lin_h, lin_h, lin_h, jax.ShapeDtypeStruct((2 * heads, head_dim), f32)],
            10,
            [lin_f, lin_f, head_f, head_f, head_f, VMEM((heads, block_len, head_dim), b16), VMEM(vec.shape, f32), tp_scratch, dma((4,))]
            + [dma((cp_size, 2))] * 2 + [dma((heads,))] * 8 + [dma((tp_size,))] * 2,
            collective_id=3,
        )(dq_all, dk_all, dv_all, q_lin, k_lin, inv, *gains, cos_tab, sin_tab)
        o_own = lax.dynamic_slice_in_dim(o_gath, tp_index * loc_width, loc_width, 1)

        def wgrad(left, right):
            return lax.dot_general(left, right, (((0,), (0,)), ((), ())), preferred_element_type=f32)

        grad_w_o, grad_w_v, grad_w_q, grad_w_k = wgrad(o_own, grad_proj), wgrad(x_loc, dv16), wgrad(x_loc, dq16), wgrad(x_loc, dk16)
        dx_part = sum(lax.dot_general(g, w, NT, preferred_element_type=f32) for g, w in ((dq16, w_q2), (dk16, w_k2), (dv16, w_v2)))
        w_parts = [grad_w_o, grad_w_v, grad_w_q, grad_w_k]
        small = jnp.concatenate([gain_grads, grad_post.reshape(-1, head_dim)], axis=0)
        any_spec = pl.BlockSpec(memory_space=pl.ANY)
        vmem_spec = pl.BlockSpec(memory_space=VMEM)

        def bufs(lead, div):
            return [VMEM(lead + (w.shape[0] // div, w.shape[1]), f32) for w in w_parts]

        ring = cp_size // 2
        rows_dx, half_dx = VMEM((sub, d_model), f32), VMEM((sub // 2, d_model), f32)
        res = pl.pallas_call(
            functools.partial(reduce_tail, tp_size, cp_size, heads),
            out_shape=[jax.ShapeDtypeStruct(w.shape, f32) for w in w_parts] + [jax.ShapeDtypeStruct((block_len, d_model), b16), jax.ShapeDtypeStruct(small.shape, f32)],
            in_specs=[any_spec] * 5 + [vmem_spec] * 2,
            out_specs=[any_spec] * 5 + [vmem_spec],
            scratch_shapes=bufs((ring,), cp_size) * 2 + bufs((), 2 * cp_size) * 2 + bufs((), cp_size) * 2
            + [half_dx, half_dx, rows_dx, half_dx, half_dx, rows_dx, rows_dx, VMEM((sub, d_model), b16)]
            + [VMEM((cp_size,) + small.shape, f32), VMEM((tp_size, d_model // head_dim, head_dim), f32)]
            + [dma((5, 10))] * 2 + [dma((4, 4))] * 2 + [dma((4, 5))] * 2 + [dma((5, 5))] + [dma((cp_size,))] * 2 + [dma((tp_size,))] * 2,
            compiler_params=pltpu.CompilerParams(vmem_limit_bytes=LIMIT, collective_id=6, has_side_effects=True),
        )(*w_parts, dx_part, dy_rows, small)
        grad_w_v, grad_w_q, grad_w_k = (g.reshape(w_q.shape) for g in res[1:4])
        grad_x, small_sum = res[4:]
        return (y_out[None], grad_x[None], grad_w_q, grad_w_k, grad_w_v, res[0].reshape(w_o.shape), small_sum[:heads], small_sum[heads : 2 * heads], small_sum[2 * heads :].reshape(-1))

    return jax.shard_map(local_run, mesh=mesh, in_specs=in_specs, out_specs=out_specs, check_vma=False)
```

```python
import functools
import math

import jax
import jax.numpy as jnp
from jax import lax
from jax.experimental import pallas as pl
from jax.experimental.pallas import tpu as pltpu
from jax.sharding import PartitionSpec as P

ROPE_THETA = 500000.0
NORM_EPS = 1e-6
LOG2E = 1.4426950408889634
LIMIT = 56 << 20
LANES = 128
FAR_A, FAR_B, NEAR_L, NEAR_R, SUM_L, SUM_R, OUT_L, OUT_R, RELAY_L, RELAY_R = range(10)
PARTS = tuple(zip((RELAY_L, RELAY_R), range(2)))
VMEM = pltpu.VMEM
MESH = pl.DeviceIdType.MESH
NT = (((1,), (1,)), ((), ()))


def rope_tables(start_pos, seq_rows, head_dim):
    half_dim = head_dim // 2
    lane = jnp.arange(head_dim)
    inv_freq = ROPE_THETA ** (-2.0 * (lane % half_dim).astype(jnp.float32) / head_dim)
    positions = (start_pos + jnp.arange(seq_rows)).astype(jnp.float32)
    angles = positions[:, None] * inv_freq[None, :]
    return jnp.cos(angles), jnp.where(lane < half_dim, -1.0, 1.0) * jnp.sin(angles)


def vmem_call(kernel, out_shape, n_in, scratch, collective_id, n_any=0):
    n_out = len(out_shape) - n_any
    return pl.pallas_call(
        kernel,
        out_shape=out_shape,
        in_specs=[pl.BlockSpec(memory_space=VMEM)] * n_in,
        out_specs=[pl.BlockSpec(memory_space=VMEM)] * n_out + [pl.BlockSpec(memory_space=pl.ANY)] * n_any,
        scratch_shapes=scratch,
        compiler_params=pltpu.CompilerParams(vmem_limit_bytes=LIMIT, collective_id=collective_id, has_side_effects=True),
    )


def block_of(ref, index, size):
    return ref.at[pl.ds(pl.multiple_of(index * size, size), size), :]


def remote(src, dst, send_sem, recv_sem, device_id):
    return pltpu.make_async_remote_copy(src_ref=src, dst_ref=dst, send_sem=send_sem, recv_sem=recv_sem, device_id=device_id, device_id_type=MESH)


def cross_barrier(me_tp, me_cp, tp_size, cp_size):
    barrier = pltpu.get_barrier_semaphore()
    for axis, me, size in (("cp", me_cp, cp_size), ("tp", me_tp, tp_size)):
        for step in range(1, size):
            pl.semaphore_signal(barrier, inc=1, device_id={axis: lax.rem(me + step, size)}, device_id_type=MESH)
    pl.semaphore_wait(barrier, cp_size + tp_size - 2)


def cols(ref, head, rows=None):
    lanes = pl.ds(pl.multiple_of(head * LANES, LANES), LANES)
    return ref.at[:, lanes] if rows is None else ref.at[rows, lanes]


def sub_rows(core, slot, sub):
    first = core if slot == 0 else 3 - core
    return pl.ds(pl.multiple_of(first * sub, sub), sub)


def share_over_tp(tp_size, me, vec, got, ss, rs):
    copies = []
    for r in range(1, tp_size):
        copy = remote(vec, got.at[r], ss.at[r], rs.at[r], {"tp": lax.rem(me + r, tp_size)})
        copy.start()
        copies.append(copy)

    def finish():
        for copy in copies:
            copy.wait()
        return (vec[...] + got[2]) + (got[1] + got[3])

    return finish


def rolled(t, c, s):
    return t * c + pltpu.roll(t, LANES // 2, 1) * s


def group_barrier(me_tp, me_cp, tp_size, cp_size):
    barrier = pltpu.get_barrier_semaphore()
    for st in range(tp_size):
        for sc in range(cp_size):
            if st or sc:
                pl.semaphore_signal(barrier, inc=1, device_id={"tp": lax.rem(me_tp + st, tp_size), "cp": lax.rem(me_cp + sc, cp_size)}, device_id_type=MESH)
    pl.semaphore_wait(barrier, tp_size * cp_size - 1)


def scatter_qkv(heads, tp_size, cp_size, width, q_lin, k_lin, v_in, vec, q_gain, k_gain, cos_t, sin_t, wo_in, q_out, k_out, v_out, inv_out, wo_out, q16, k16, got, loc, qs, qr, ks, kr, vs, vr, fks, fkr, fvs, fvr, ts, tr, ws, wr, wfs, wfr):
    me_tp = lax.axis_index("tp")
    me = lax.axis_index("cp")
    core = lax.rem(me, 2)
    chip = me // 2
    sub = q_out.shape[1] // 2
    cross_barrier(me_tp, me, tp_size, cp_size)
    finish = share_over_tp(tp_size, me_tp, vec, got, ts, tr)
    far_chips = (1, heads - 1, 2)
    sends = []

    def spread(src, out, ss, rs):
        for r in far_chips:
            dst = lax.rem(chip + r, heads)
            copy = remote(cols(src, dst), out.at[me], ss.at[r], rs.at[r], {"cp": dst * 2 + core})
            copy.start()
            sends.append(copy)

    spread(v_in, v_out, vs, vr)
    shard = wo_in.shape[0]
    keep = pltpu.make_async_copy(wo_in, block_of(wo_out, me_tp, shard), loc.at[4])
    keep.start()
    for r in range(1, tp_size):
        copy = remote(block_of(wo_in, core, shard // 2), block_of(wo_out, me_tp * 2 + core, shard // 2), ws.at[r], wr.at[r], {"tp": lax.rem(me_tp + r, tp_size)})
        copy.start()
        sends.append(copy)
    inv_out[...] = lax.rsqrt(finish() / width + NORM_EPS)
    n_chunk = inv_out.shape[0] // 2
    inv_cols = inv_out[...].T

    def rotate(lin, gain, out16, first):
        for r in range(n_chunk):
            rows = slice(r * LANES, (r + 1) * LANES)
            scale = inv_cols[:, first + r : first + r + 1]
            for h in range(heads):
                lanes = slice(h * LANES, (h + 1) * LANES)
                out16[rows, lanes] = rolled(lin[rows, lanes] * scale * gain[:, lanes], cos_t[rows, :], sin_t[rows, :]).astype(out16.dtype)

    rotate(k_lin, k_gain, k16, n_chunk)
    spread(k16, k_out, ks, kr)
    rotate(q_lin, q_gain, q16, 0)
    own = [pltpu.make_async_copy(cols(k16, chip), k_out.at[me], loc.at[0]), pltpu.make_async_copy(cols(v_in, chip), v_out.at[me], loc.at[1])]
    for r in range(cp_size):
        dst = lax.rem(me + r, cp_size)
        for s in range(2):
            src = cols(q16, dst // 2, sub_rows(lax.rem(dst, 2), s, sub))
            place = q_out.at[me, s * sub : (s + 1) * sub, :]
            if r == 0:
                own.append(pltpu.make_async_copy(src, place, loc.at[2 + s]))
            else:
                copy = remote(src, place, qs.at[r, s], qr.at[r, s], {"cp": dst})
                copy.start()
                sends.append(copy)
    for copy in own:
        copy.start()
    partner = {"cp": me + 1 - 2 * core}
    forwards = []
    for r in (0,) + far_chips:
        src = lax.rem(chip - r + heads, heads) * 2 + core
        for i, (buf, ss, rs, fs, fr) in enumerate(((v_out, vs, vr, fvs, fvr), (k_out, ks, kr, fks, fkr))):
            if r == 0:
                own[1 - i].wait()
            else:
                remote(buf.at[src], buf.at[src], ss.at[r], rs.at[r], partner).wait_recv()
            copy = remote(buf.at[src], buf.at[src], fs.at[r], fr.at[r], partner)
            copy.start()
            forwards.append(copy)
    for copy in own[2:] + [keep]:
        copy.wait()
    for r in range(1, tp_size):
        part = block_of(wo_out, lax.rem(me_tp - r + tp_size, tp_size) * 2 + core, shard // 2)
        remote(part, part, ws.at[r], wr.at[r], partner).wait_recv()
        copy = remote(part, part, wfs.at[r], wfr.at[r], partner)
        copy.start()
        forwards.append(copy)
    for copy in sends:
        copy.wait_send()
    for r in range(1, cp_size):
        for s in range(2):
            place = q_out.at[lax.rem(me - r + cp_size, cp_size), s * sub : (s + 1) * sub, :]
            remote(place, place, qs.at[r, s], qr.at[r, s], partner).wait_recv()
    for copy in forwards:
        copy.wait()


def attend(sub, scale, q_ref, k_ref, v_ref, o_ref, lse_ref, vt_scr, m_scr, l_scr, acc_scr, s_a, s_b, mx_a):
    blk = pl.program_id(0)
    core = lax.rem(lax.axis_index("cp"), 2)
    coef = scale * LOG2E
    half = k_ref.shape[1] // 2
    cols = q_ref.shape[1]
    chunk = half // 2
    vt_scr[blk] = v_ref[blk].T
    m_scr[...] = jnp.full_like(m_scr, -jnp.inf)
    l_scr[...] = jnp.zeros_like(l_scr)
    acc_scr[...] = jnp.zeros_like(acc_scr)

    def fold(op, values):
        return op(values.reshape(values.shape[0] // 8, 8, cols), axis=0)

    def scores(b, h, c):
        kv = slice(h * half + c * chunk, h * half + (c + 1) * chunk)
        return lax.dot_general(k_ref[b, kv, :], q_ref[0], NT, preferred_element_type=jnp.float32)

    def mask(s, h, c):
        kv_pos = h * half + c * chunk + lax.broadcasted_iota(jnp.int32, s.shape, 0)
        col = lax.broadcasted_iota(jnp.int32, s.shape, 1)
        q_pos = jnp.where(col < sub, core * sub + col, (2 - core) * sub + col)
        return jnp.where(kv_pos <= q_pos, s, -jnp.inf)

    def step(buf, mx, b, h, nxt):
        m_old = m_scr[...]
        m_new = jnp.maximum(m_old, mx)
        mc = m_new * coef
        alpha = jnp.exp2((m_old - m_new) * coef)
        lsum = jnp.zeros((8, cols), jnp.float32)
        new_mx = None
        for c in range(2):
            rows = slice(c * chunk, (c + 1) * chunk)
            if nxt is not None:
                nbuf, nb, nh, masked = nxt
                s = scores(nb, nh, c)
                if masked:
                    s = mask(s, nh, c)
                nbuf[rows, :] = s
                part = fold(jnp.max, s)
                new_mx = part if new_mx is None else jnp.maximum(new_mx, part)
            p = jnp.exp2(buf[rows, :] * coef - mc)
            lsum = lsum + fold(jnp.sum, p)
            pv = jnp.dot(vt_scr[b, :, h * half + c * chunk : h * half + (c + 1) * chunk], p.astype(jnp.bfloat16), preferred_element_type=jnp.float32)
            acc_scr[...] = acc_scr[...] * alpha + pv if c == 0 else acc_scr[...] + pv
        l_scr[...] = l_scr[...] * alpha + jnp.sum(lsum, axis=0, keepdims=True)
        m_scr[...] = m_new
        return None if nxt is None else jnp.max(new_mx, axis=0, keepdims=True)

    for c in range(2):
        s_a[c * chunk : (c + 1) * chunk, :] = scores(0, 0, c)
    mx_a[...] = jnp.max(s_a[...], axis=0, keepdims=True)

    def body(b, carry):
        mx_b = step(s_a, mx_a[...], b, 0, (s_b, b, 1, False))
        mx_a[...] = step(s_b, mx_b, b, 1, (s_a, b + 1, 0, False))
        return carry

    lax.fori_loop(0, blk, body, 0)
    for c in range(2):
        rows = slice(c * chunk, (c + 1) * chunk)
        s_a[rows, :] = mask(s_a[rows, :], 0, c)
    mx_b = step(s_a, jnp.max(s_a[...], axis=0, keepdims=True), blk, 0, (s_b, blk, 1, True))
    step(s_b, mx_b, blk, 1, None)
    o_ref[0] = (acc_scr[...] / l_scr[...]).T.astype(o_ref.dtype)
    lse_ref[0] = m_scr[...] * coef + jnp.log2(l_scr[...])


def heads_to_rows(heads, tp_size, cp_size, o_in, o_out, ss, rs):
    me_tp = lax.axis_index("tp")
    me_cp = lax.axis_index("cp")
    core = lax.rem(me_cp, 2)
    head = me_tp * heads + me_cp // 2
    sub = o_out.shape[0]
    place = cols(o_out, head)
    group_barrier(me_tp, me_cp, tp_size, cp_size)
    for finish in range(2):
        if finish:
            for h in range(heads * tp_size):
                part = o_out.at[:, h * LANES : (h + 1) * LANES]
                pltpu.make_async_copy(part, part, rs.at[h]).wait()
        for s in range(2):
            dst_tp = core if s == 0 else 3 - core
            for r in range(cp_size):
                dst_cp = lax.rem(me_cp + r, cp_size)
                src = o_in.at[dst_cp, s * sub : (s + 1) * sub, :]
                copy = remote(src, place, ss.at[s, r], rs.at[head], {"tp": dst_tp, "cp": dst_cp})
                act = copy.wait_send if finish else copy.start
                if r:
                    act()
                    continue
                pl.when(dst_tp != me_tp)(act)
                if not finish:
                    pl.when(dst_tp == me_tp)(pltpu.make_async_copy(src, place, rs.at[head]).start)


def rows_to_heads(heads, tp_size, cp_size, g_in, g_out, ss, rs):
    me_tp = lax.axis_index("tp")
    me_cp = lax.axis_index("cp")
    core = lax.rem(me_cp, 2)
    sub = g_in.shape[0]
    row_core = jnp.where(me_tp < 2, me_tp, 3 - me_tp)
    slot = me_tp // 2
    place = g_out.at[me_cp, pl.ds(pl.multiple_of(slot * sub, sub), sub), :]
    group_barrier(me_tp, me_cp, tp_size, cp_size)
    for finish in range(2):
        if finish:
            for i in range(cp_size):
                for s in range(2):
                    part = g_out.at[i, s * sub : (s + 1) * sub, :]
                    pltpu.make_async_copy(part, part, rs.at[i, s]).wait()
        for rt in range(tp_size):
            dst_tp = lax.rem(me_tp + rt, tp_size)
            for r in range(heads):
                chip = lax.rem(me_cp // 2 + r, heads)
                src = cols(g_in, dst_tp * heads + chip)
                copy = remote(src, place, ss.at[rt, r], rs.at[me_cp, slot], {"tp": dst_tp, "cp": chip * 2 + row_core})
                act = copy.wait_send if finish else copy.start
                if rt or r:
                    act()
                    continue
                pl.when(row_core != core)(act)
                if not finish:
                    pl.when(row_core == core)(pltpu.make_async_copy(src, place, rs.at[me_cp, slot]).start)


def attend_back(heads, tp_size, cp_size, width, scale, q_ref, k_ref, v_ref, o_ref, do_ref, lse_ref, q_lin, k_lin, inv, q_gain, k_gain, cos_t, sin_t, gp_in, or_in,
                dq_out, dk_out, dv_out, gain_out, gp_out, oo_out,
                kt_scr, dqt_scr, dl_scr, dqs, acc_k, acc_v, dq, dk, pk, pv, sk, sv, part, got, loc, qs, qr, pks, pkr, pvs, pvr, ks, kr, vs, vr, ts, tr, gs, gr, os, orr):
    me_tp = lax.axis_index("tp")
    me = lax.axis_index("cp")
    core = lax.rem(me, 2)
    chip = me // 2
    rows = q_ref.shape[1]
    sub = rows // 2
    block_len = k_ref.shape[1]
    coef = scale * LOG2E
    f32 = jnp.float32
    partner = {"cp": me + 1 - 2 * core}
    cross_barrier(me_tp, me, tp_size, cp_size)
    sends = []
    loc_width = heads * LANES
    own = [
        pltpu.make_async_copy(gp_in, block_of(gp_out, me_tp, sub), loc.at[4]),
        pltpu.make_async_copy(or_in.at[:, pl.ds(pl.multiple_of(me_tp * loc_width, loc_width), loc_width)], block_of(oo_out, me_tp, sub), loc.at[5]),
    ]
    for r in range(1, tp_size):
        dst = lax.rem(me_tp + r, tp_size)
        sends.append(remote(gp_in, block_of(gp_out, me_tp, sub), gs.at[r], gr.at[r], {"tp": dst}))
        sends.append(remote(or_in.at[:, pl.ds(pl.multiple_of(dst * loc_width, loc_width), loc_width)], block_of(oo_out, me_tp, sub), os.at[r], orr.at[r], {"tp": dst}))
    for copy in own + sends:
        copy.start()

    def prepare(i, carry):
        kt_scr[i] = k_ref[i].T
        prod = o_ref[i].astype(f32) * do_ref[i].astype(f32)
        dl_scr[i] = jnp.sum(prod.T, axis=0, keepdims=True)
        dqt_scr[i] = jnp.zeros((LANES, rows), f32)
        return carry

    lax.fori_loop(0, cp_size, prepare, 0)

    def tile(i, b, s, e, masked):
        q = q_ref[i]
        do = do_ref[i]
        lse = lse_ref[i]
        delta = dl_scr[i]
        for j in range(block_len // sub):
            kv = slice(j * sub, (j + 1) * sub)
            scores = lax.dot_general(k_ref[b, kv, :], q, NT, preferred_element_type=f32)
            p = jnp.exp2(scores * coef - lse)
            if masked:
                kv_pos = j * sub + lax.broadcasted_iota(jnp.int32, (sub, rows), 0)
                col = lax.broadcasted_iota(jnp.int32, (sub, rows), 1)
                q_pos = jnp.where(col < sub, core * sub + col, (2 - core) * sub + col)
                p = jnp.where(kv_pos <= q_pos, p, 0.0)
            dp = lax.dot_general(v_ref[b, kv, :], do, NT, preferred_element_type=f32)
            ds = (p * (dp - delta)).astype(jnp.bfloat16)
            for acc, left, right in ((acc_v, p.astype(jnp.bfloat16), do), (acc_k, ds, q)):
                new = jnp.dot(left, right, preferred_element_type=f32)
                acc[s, e, kv, :] = new if masked else acc[s, e, kv, :] + new
            dqt_scr[i] += jnp.dot(kt_scr[b, :, kv], ds, preferred_element_type=f32)

    def pair_copies(s):
        return [remote(acc.at[s, 1 - core], dst.at[s], ss.at[s], rs.at[s], partner) for acc, dst, ss, rs in ((acc_k, pk, pks, pkr), (acc_v, pv, pvs, pvr))]

    def home_copies(s):
        dst = {"cp": lax.rem(chip + 1 + s, heads) * 2 + core}
        return [remote(src.at[s], cols(out, chip), ss.at[s], rs.at[s], dst) for src, out, ss, rs in ((sk, dk, ks, kr), (sv, dv_out, vs, vr))]

    def add_pair(s):
        for copy in pair_copies(s):
            copy.wait()
        sk[s] = (acc_k[s, core] + pk[s]) * scale
        sv[s] = (acc_v[s, core] + pv[s]).astype(sv.dtype)

    def key_pair(s, carry):
        def key_block(e, inner):
            b = lax.rem(chip + 1 + s, heads) * 2 + e
            tile(b, b, s, e, True)

            def full(i, last):
                tile(i, b, s, e, False)
                return last

            return lax.fori_loop(b + 1, cp_size, full, inner)

        lax.fori_loop(0, 2, key_block, 0)
        for copy in pair_copies(s):
            copy.start()

        @pl.when(s > 0)
        def _():
            add_pair(s - 1)
            for copy in home_copies(s - 1):
                copy.start()

        return carry

    lax.fori_loop(0, heads, key_pair, 0)
    for r in range(cp_size):
        dst = lax.rem(me + r, cp_size)
        dqs[dst] = dqt_scr[dst].T * scale
        for s in range(2):
            src = dqs.at[dst, s * sub : (s + 1) * sub, :]
            place = cols(dq, chip, sub_rows(core, s, sub))
            if r == 0:
                copy = pltpu.make_async_copy(src, place, loc.at[s])
                own.append(copy)
            else:
                copy = remote(src, place, qs.at[r, s], qr.at[r, s], {"cp": dst})
                sends.append(copy)
            copy.start()
    last = heads - 1
    add_pair(last)
    for j, (src, out) in enumerate(((sk, dk), (sv, dv_out))):
        copy = pltpu.make_async_copy(src.at[last], cols(out, chip), loc.at[2 + j])
        copy.start()
        own.append(copy)
    for copy in own:
        copy.wait()
    inv_cols = inv[...].T
    n_chunk = inv.shape[0] // 2
    dots = []

    def first_pass(i, grad, lin, gain):
        gains = [jnp.zeros((1, LANES), f32)] * heads
        for r in range(n_chunk):
            part_rows = slice(r * LANES, (r + 1) * LANES)
            c = i * n_chunk + r
            norm = inv_cols[:, c : c + 1]
            total = jnp.zeros((LANES, LANES), f32)
            for h in range(heads):
                lanes = slice(h * LANES, (h + 1) * LANES)
                hat = lin[part_rows, lanes] * norm
                back = rolled(grad[part_rows, lanes], cos_t[part_rows, :], -sin_t[part_rows, :])
                both = back * hat
                gains[h] = gains[h] + jnp.sum(both, axis=0, keepdims=True)
                total = total + both * gain[:, lanes]
                grad[part_rows, lanes] = back * gain[:, lanes]
            dots.append(jnp.sum(total, axis=1, keepdims=True))
        for h in range(heads):
            gain_out[i * heads + h : i * heads + h + 1, :] = gains[h]

    for s in range(last):
        place = cols(dk, lax.rem(chip - 1 - s + heads, heads))
        remote(place, place, ks.at[s], kr.at[s], partner).wait_recv()
    first_pass(1, dk, k_lin, k_gain)
    for r in range(1, cp_size):
        src = lax.rem(me - r + cp_size, cp_size)
        for s in range(2):
            place = cols(dq, src // 2, sub_rows(lax.rem(src, 2), s, sub))
            remote(place, place, qs.at[r, s], qr.at[r, s], partner).wait_recv()
    first_pass(0, dq, q_lin, q_gain)
    part[...] = jnp.concatenate(dots[n_chunk:] + dots[:n_chunk], axis=1).T
    dot_cols = (share_over_tp(tp_size, me_tp, part, got, ts, tr)() / width).T
    for i, (grad, lin, out) in enumerate(((dq, q_lin, dq_out), (dk, k_lin, dk_out))):
        for r in range(n_chunk):
            part_rows = slice(r * LANES, (r + 1) * LANES)
            c = i * n_chunk + r
            norm = inv_cols[:, c : c + 1]
            out[part_rows, :] = (norm * (grad[part_rows, :] - lin[part_rows, :] * norm * dot_cols[:, c : c + 1])).astype(out.dtype)
    for s in range(last):
        sends.extend(home_copies(s))
        place = cols(dv_out, lax.rem(chip - 1 - s + heads, heads))
        remote(place, place, vs.at[s], vr.at[s], partner).wait_recv()
    for r in range(1, tp_size):
        for out, ss, rs in ((gp_out, gs, gr), (oo_out, os, orr)):
            place = block_of(out, lax.rem(me_tp - r + tp_size, tp_size), sub)
            remote(place, place, ss.at[r], rs.at[r], partner).wait_recv()
    for copy in sends:
        copy.wait_send()


def reduce_tail(tp_size, cp_size, *refs):
    n_w = 4
    w_in, (dx_in, dy_in, small, y_in) = refs[:n_w], refs[n_w : 2 * n_w]
    refs = refs[2 * n_w :]
    w_out, (dx_out, y_out, small_out) = refs[:n_w], refs[n_w : n_w + 3]
    refs = refs[n_w + 3 :]
    acc, pair, far_a, far_b, fin_l, fin_r = (refs[i * n_w : (i + 1) * n_w] for i in range(6))
    refs = refs[6 * n_w :]
    dxa, dxb, dx_own, dx_fa, dx_fb, dx_fl, dx_fr, dx16, got_small, got_post, ss, rs, ps, pr, fs, fr, loc, sms, smr, gps, gpr = refs
    me_tp = lax.axis_index("tp")
    me_cp = lax.axis_index("cp")
    core = lax.rem(me_cp, 2)
    chip = me_cp // 2
    ring = cp_size // 2
    left, right, far = (lax.rem(chip + d, ring) for d in (ring - 1, 1, 2))
    t_left, t_right, t_far = (lax.rem(me_tp + d, tp_size) for d in (tp_size - 1, 1, 2))
    partner = {"cp": me_cp + 1 - 2 * core}
    to_l, to_r = {"cp": left * 2 + core}, {"cp": right * 2 + core}
    tp_l, tp_r = {"tp": t_left}, {"tp": t_right}
    dx_i, y_i = n_w, n_w + 1
    outs = []

    def ring_sems(t, kind):
        return ss.at[t, kind], rs.at[t, kind]

    def pair_sems(t, kind):
        return fs.at[t, kind], fr.at[t, kind]

    cross_barrier(me_tp, me_cp, tp_size, cp_size)
    sent = []

    def go(src, dst, s_sem, r_sem, device):
        copy = remote(src, dst, s_sem, r_sem, device)
        copy.start()
        sent.append(copy)

    def landed(dst, s_sem, r_sem):
        remote(dst, dst, s_sem, r_sem, partner).wait_recv()

    def piece(ref, t, x, c, part=None):
        size = w_in[t].shape[0] // cp_size
        first = (2 * x + c) * size
        if part is None:
            return ref.at[pl.ds(pl.multiple_of(first, size), size), :]
        return ref.at[pl.ds(pl.multiple_of(first + part * (size // 2), size // 2), size // 2), :]

    def rows_of(ref, y, part=None):
        size = dx_in.shape[0] // tp_size
        if part is None:
            return ref.at[pl.ds(pl.multiple_of(y * size, size), size), :]
        return ref.at[pl.ds(pl.multiple_of(y * size + part * (size // 2), size // 2), size // 2), :]

    def half_of(ref, part):
        size = ref.shape[0] // 2
        return ref.at[pl.ds(part * size, size), :]

    for r in range(1, cp_size):
        go(small, got_small.at[me_cp], sms.at[r], smr.at[r], {"cp": lax.rem(me_cp + r, cp_size)})
    go(rows_of(dx_in, t_far, 0), dx_fa, *ring_sems(dx_i, FAR_A), tp_l)
    go(rows_of(dx_in, t_far, 1), dx_fb, *ring_sems(dx_i, FAR_B), tp_r)
    go(rows_of(dx_in, t_left, 1), half_of(dx_fr, 1), *ring_sems(dx_i, NEAR_L), tp_l)
    go(rows_of(dx_in, t_right, 0), half_of(dx_fl, 0), *ring_sems(dx_i, NEAR_R), tp_r)
    def give(src, stream, out, dev_l, dev_r):
        copy = pltpu.make_async_copy(src, out, loc.at[stream, n_w])
        copy.start()
        outs.append(copy)
        go(src, out, *ring_sems(stream, OUT_L), dev_l)
        go(src, out, *ring_sems(stream, OUT_R), dev_r)

    give(y_in, y_i, rows_of(y_out, me_tp), tp_l, tp_r)
    order = (far, left, right, chip)
    loads = []
    for t in range(n_w):
        for i, x in enumerate(order):
            go(piece(w_in[t], t, x, 1 - core), pair[t].at[x], ps.at[t, i], pr.at[t, i], partner)
            copy = pltpu.make_async_copy(piece(w_in[t], t, x, core), acc[t].at[x], loc.at[t, i])
            copy.start()
            loads.append(copy)
    dx_loads = [
        pltpu.make_async_copy(rows_of(dx_in, t_left, 0), dxa, loc.at[n_w, 0]),
        pltpu.make_async_copy(rows_of(dx_in, t_right, 1), dxb, loc.at[n_w, 1]),
        pltpu.make_async_copy(rows_of(dx_in, me_tp), dx_own, loc.at[n_w, 2]),
    ]
    for copy in dx_loads:
        copy.start()

    for t in range(n_w):
        for i, x in enumerate(order):
            loads[t * 4 + i].wait()
            landed(pair[t].at[x], ps.at[t, i], pr.at[t, i])
            acc[t][x] += pair[t][x]
        go(half_of(acc[t].at[far], 0), far_a[t], *ring_sems(t, FAR_A), to_l)
        go(half_of(acc[t].at[far], 1), far_b[t], *ring_sems(t, FAR_B), to_r)
        go(half_of(acc[t].at[left], 1), half_of(fin_r[t], 1), *ring_sems(t, NEAR_L), to_l)
        go(half_of(acc[t].at[right], 0), half_of(fin_l[t], 0), *ring_sems(t, NEAR_R), to_r)

    got_small[me_cp] = small[...]
    for r in range(1, cp_size):
        landed(got_small.at[lax.rem(me_cp - r + cp_size, cp_size)], sms.at[r], smr.at[r])
    total = got_small[0]
    for i in range(1, cp_size):
        total = total + got_small[i]
    small_out[...] = total
    n_gain = small.shape[0] - got_post.shape[1]

    def second_half(t, acc_l, acc_r, fa, fb, fl, fr, dev_l, dev_r):
        half = fa.shape[0]
        landed(fa, *ring_sems(t, FAR_A))
        acc_l[...] += fa[...]
        landed(fb, *ring_sems(t, FAR_B))
        acc_r[...] += fb[...]
        go(acc_l, half_of(fr, 0), *ring_sems(t, SUM_L), dev_l)
        go(acc_r, half_of(fl, 1), *ring_sems(t, SUM_R), dev_r)

    def all_landed(t, fl, fr):
        landed(half_of(fr, 1), *ring_sems(t, NEAR_L))
        landed(half_of(fl, 0), *ring_sems(t, NEAR_R))
        landed(half_of(fr, 0), *ring_sems(t, SUM_L))
        landed(half_of(fl, 1), *ring_sems(t, SUM_R))

    for t in range(n_w):
        second_half(t, half_of(acc[t].at[left], 0), half_of(acc[t].at[right], 1), far_a[t], far_b[t], fin_l[t], fin_r[t], to_l, to_r)
    for copy in dx_loads:
        copy.wait()
    second_half(dx_i, dxa, dxb, dx_fa, dx_fb, dx_fl, dx_fr, tp_l, tp_r)
    post = small_out.at[pl.ds(n_gain, got_post.shape[1]), :]
    for r in range(1, tp_size):
        go(post, got_post.at[r], gps.at[r], gpr.at[r], {"tp": lax.rem(me_tp + r, tp_size)})

    for t in range(n_w):
        all_landed(t, fin_l[t], fin_r[t])
        acc[t][chip] = acc[t][chip] + (fin_l[t][...] + fin_r[t][...])
        src = acc[t].at[chip]
        dst = piece(w_out[t], t, chip, core)
        give(src, t, dst, to_l, to_r)
        go(src, dst, *pair_sems(t, 0), partner)
    all_landed(dx_i, dx_fl, dx_fr)
    dx16[...] = (dx_own[...] + (dx_fl[...] + dx_fr[...]) + dy_in[...].astype(jnp.float32)).astype(dx16.dtype)
    give(dx16, dx_i, rows_of(dx_out, me_tp), tp_l, tp_r)

    def relay(stream, part_of, x_l, x_r, dev_l, dev_r, pass_on):
        for arrived, x, kind, part, dev in ((OUT_L, x_r, RELAY_L, 0, dev_l), (OUT_R, x_l, RELAY_R, 1, dev_r)):
            whole = part_of(x)
            landed(whole, *ring_sems(stream, arrived))
            half = part_of(x, part)
            go(half, half, *ring_sems(stream, kind), dev)
            if pass_on:
                go(whole, whole, *pair_sems(stream, 1 + part), partner)

    for t in range(n_w):
        relay(t, functools.partial(lambda ref, t, x, part=None: piece(ref, t, x, core, part), w_out[t], t), left, right, to_l, to_r, True)
    for stream, out in ((y_i, y_out), (dx_i, dx_out)):
        relay(stream, functools.partial(rows_of, out), t_left, t_right, tp_l, tp_r, False)

    sums = small_out[n_gain:, :]
    for r in range(1, tp_size):
        landed(got_post.at[r], gps.at[r], gpr.at[r])
    sums = (sums + got_post[2]) + (got_post[1] + got_post[3])

    for t in range(n_w):
        for kind, part in PARTS:
            half = piece(w_out[t], t, far, core, part)
            landed(half, *ring_sems(t, kind))
            go(half, half, *pair_sems(t, 3 + part), partner)
    for stream, out in ((y_i, y_out), (dx_i, dx_out)):
        for kind, part in PARTS:
            landed(rows_of(out, t_far, part), *ring_sems(stream, kind))
    for t in range(n_w):
        for i, x in enumerate((chip, right, left)):
            landed(piece(w_out[t], t, x, 1 - core), *pair_sems(t, i))
        for part in range(2):
            landed(piece(w_out[t], t, far, 1 - core, part), *pair_sems(t, 3 + part))
    for copy in outs:
        copy.wait()
    for copy in sent:
        copy.wait_send()
    small_out[n_gain:, :] = sums


def solution(mesh):
    tp_size = mesh.shape["tp"]
    cp_size = mesh.shape["cp"]
    act_spec = P("dp", "cp", None)
    col_spec = P(None, "tp", None)
    part_col = P("dp", "tp", None)
    in_specs = (act_spec, col_spec, col_spec, col_spec, P("tp", None, None), P("tp", None), P("tp", None), P(None), act_spec)
    out_specs = (act_spec, act_spec, part_col, part_col, part_col, P(("dp", "tp"), None, None), P(("dp", "tp"), None), P(("dp", "tp"), None), P("dp"))
    dma = pltpu.SemaphoreType.DMA

    def local_run(x_in, w_q, w_k, w_v, w_o, q_norm_w, k_norm_w, post_norm_w, grad_y):
        n_batch, block_len, d_model = x_in.shape
        heads, head_dim = w_q.shape[1:]
        assert n_batch == 1 and w_k.shape[1] == heads and cp_size == 2 * heads and tp_size == 4
        sub = block_len // tp_size
        rows = 2 * sub
        width = heads * head_dim * tp_size
        scale = head_dim ** -0.5
        f32 = jnp.float32
        b16 = jnp.bfloat16
        tp_index = lax.axis_index("tp")
        cp_index = lax.axis_index("cp")
        cos_tab, sin_tab = rope_tables(cp_index * block_len, block_len, head_dim)
        x_loc = x_in[0]
        dy_loc = grad_y[0]
        w_q2, w_k2, w_v2 = (w.reshape(d_model, -1) for w in (w_q, w_k, w_v))
        gains = [g.reshape(1, -1) for g in (q_norm_w, k_norm_w)]
        loc_width = heads * head_dim

        q_lin = jnp.dot(x_loc, w_q2, preferred_element_type=f32)
        k_lin = jnp.dot(x_loc, w_k2, preferred_element_type=f32)
        v_val = jnp.dot(x_loc, w_v2, preferred_element_type=f32).astype(b16)
        vec = jnp.stack([jnp.sum(t * t, axis=1) for t in (q_lin, k_lin)]).reshape(-1, LANES)
        vec_shape = jax.ShapeDtypeStruct(vec.shape, f32)
        kv_shape = jax.ShapeDtypeStruct((cp_size, block_len, head_dim), b16)
        lin16 = VMEM((block_len, loc_width), b16)
        tp_scratch = VMEM((tp_size,) + vec.shape, f32)
        q_all, k_all, v_all, inv, w_o_full = vmem_call(
            functools.partial(scatter_qkv, heads, tp_size, cp_size, width),
            [jax.ShapeDtypeStruct((cp_size, rows, head_dim), b16), kv_shape, kv_shape, vec_shape, jax.ShapeDtypeStruct((width, d_model), b16)],
            9,
            [lin16, lin16, tp_scratch, dma((5,))] + [dma((cp_size, 2))] * 2 + [dma((heads,))] * 8 + [dma((tp_size,))] * 6,
            0,
            1,
        )(q_lin, k_lin, v_val, vec, *gains, cos_tab, sin_tab, w_o.reshape(-1, d_model))

        qspec = pl.BlockSpec((1, rows, head_dim), lambda i: (i, 0, 0))
        lspec = pl.BlockSpec((1, 1, rows), lambda i: (i, 0, 0))
        whole = pl.BlockSpec(memory_space=VMEM)
        pair_flops = cp_size * (cp_size + 1) // 2 * rows * block_len * head_dim * 2
        o_all, lse = pl.pallas_call(
            functools.partial(attend, sub, scale),
            grid=(cp_size,),
            in_specs=[qspec, whole, whole],
            out_specs=[qspec, lspec],
            out_shape=[jax.ShapeDtypeStruct((cp_size, rows, head_dim), b16), jax.ShapeDtypeStruct((cp_size, 1, rows), f32)],
            scratch_shapes=[VMEM((cp_size, head_dim, block_len), b16), VMEM((1, rows), f32), VMEM((1, rows), f32), VMEM((head_dim, rows), f32)]
            + [VMEM((block_len // 2, rows), f32)] * 2 + [VMEM((1, rows), f32)],
            compiler_params=pltpu.CompilerParams(vmem_limit_bytes=LIMIT),
            cost_estimate=pl.CostEstimate(flops=2 * pair_flops, bytes_accessed=6 << 20, transcendentals=0),
        )(q_all, k_all, v_all)

        n_heads = heads * tp_size
        o_rows = vmem_call(
            functools.partial(heads_to_rows, heads, tp_size, cp_size),
            [jax.ShapeDtypeStruct((sub, width), b16)],
            1,
            [dma((2, cp_size)), dma((n_heads,))],
            1,
        )(o_all)[0]

        x_rows = lax.dynamic_slice_in_dim(x_loc, tp_index * sub, sub, 0)
        dy_rows = lax.dynamic_slice_in_dim(dy_loc, tp_index * sub, sub, 0)
        dy_f = dy_rows.astype(f32)
        proj = jnp.dot(o_rows, w_o_full, preferred_element_type=f32)
        post_inv = lax.rsqrt(jnp.mean(proj * proj, axis=-1, keepdims=True) + NORM_EPS)
        post_hat = proj * post_inv
        y_rows = (x_rows + post_hat * post_norm_w).astype(b16)
        grad_post = jnp.sum(dy_f * post_hat, axis=0)
        grad_hat = dy_f * post_norm_w
        gp_rows = (post_inv * (grad_hat - post_hat * jnp.mean(grad_hat * post_hat, axis=-1, keepdims=True))).astype(b16)
        do_rows = lax.dot_general(gp_rows, w_o_full, NT, preferred_element_type=f32).astype(b16)

        do_all = vmem_call(
            functools.partial(rows_to_heads, heads, tp_size, cp_size),
            [jax.ShapeDtypeStruct((cp_size, rows, head_dim), b16)],
            1,
            [dma((tp_size, heads)), dma((cp_size, 2))],
            2,
        )(do_rows)[0]

        lin_h, f_lin = jax.ShapeDtypeStruct((block_len, loc_width), b16), VMEM((block_len, loc_width), f32)
        head_f = VMEM((heads, block_len, head_dim), f32)
        pair_f = VMEM((heads, 2, block_len, head_dim), f32)
        dq16, dk16, dv16, gain_grads, grad_proj, o_own = vmem_call(
            functools.partial(attend_back, heads, tp_size, cp_size, width, scale),
            [lin_h, lin_h, lin_h, jax.ShapeDtypeStruct((2 * heads, head_dim), f32), jax.ShapeDtypeStruct((block_len, d_model), b16), lin_h],
            15,
            [VMEM((cp_size, head_dim, block_len), b16), VMEM((cp_size, head_dim, rows), f32), VMEM((cp_size, 1, rows), f32), VMEM((cp_size, rows, head_dim), f32)]
            + [pair_f, pair_f, f_lin, f_lin, head_f, head_f, head_f, VMEM((heads, block_len, head_dim), b16), VMEM(vec.shape, f32), tp_scratch, dma((6,))]
            + [dma((cp_size, 2))] * 2 + [dma((heads,))] * 8 + [dma((tp_size,))] * 6,
            3,
            2,
        )(q_all, k_all, v_all, o_all, do_all, lse, q_lin, k_lin, inv, *gains, cos_tab, sin_tab, gp_rows, o_rows)

        def wgrad(left, right):
            return lax.dot_general(left, right, (((0,), (0,)), ((), ())), preferred_element_type=f32)

        grad_w_o, grad_w_v, grad_w_q, grad_w_k = wgrad(o_own, grad_proj), wgrad(x_loc, dv16), wgrad(x_loc, dq16), wgrad(x_loc, dk16)
        dx_part = sum(lax.dot_general(g, w, NT, preferred_element_type=f32) for g, w in ((dq16, w_q2), (dk16, w_k2), (dv16, w_v2)))
        w_parts = [grad_w_o, grad_w_v, grad_w_q, grad_w_k]
        small = jnp.concatenate([gain_grads, grad_post.reshape(-1, head_dim)], axis=0)
        any_spec = pl.BlockSpec(memory_space=pl.ANY)
        vmem_spec = pl.BlockSpec(memory_space=VMEM)

        def bufs(lead, div):
            return [VMEM(lead + (w.shape[0] // div, w.shape[1]), f32) for w in w_parts]

        ring = cp_size // 2
        rows_dx, half_dx = VMEM((sub, d_model), f32), VMEM((sub // 2, d_model), f32)
        res = pl.pallas_call(
            functools.partial(reduce_tail, tp_size, cp_size),
            out_shape=[jax.ShapeDtypeStruct(w.shape, f32) for w in w_parts] + [jax.ShapeDtypeStruct((block_len, d_model), b16)] * 2 + [jax.ShapeDtypeStruct(small.shape, f32)],
            in_specs=[any_spec] * 5 + [vmem_spec] * 3,
            out_specs=[any_spec] * 6 + [vmem_spec],
            scratch_shapes=bufs((ring,), cp_size) * 2 + bufs((), 2 * cp_size) * 2 + bufs((), cp_size) * 2
            + [half_dx, half_dx, rows_dx, half_dx, half_dx, rows_dx, rows_dx, VMEM((sub, d_model), b16)]
            + [VMEM((cp_size,) + small.shape, f32), VMEM((tp_size, d_model // head_dim, head_dim), f32)]
            + [dma((6, 10))] * 2 + [dma((4, 4))] * 2 + [dma((4, 5))] * 2 + [dma((6, 5))] + [dma((cp_size,))] * 2 + [dma((tp_size,))] * 2,
            compiler_params=pltpu.CompilerParams(vmem_limit_bytes=LIMIT, collective_id=6, has_side_effects=True),
        )(*w_parts, dx_part, dy_rows, small, y_rows)
        grad_w_v, grad_w_q, grad_w_k = (g.reshape(w_q.shape) for g in res[1:4])
        grad_x, y_out, small_sum = res[4:]
        return (y_out[None], grad_x[None], grad_w_q, grad_w_k, grad_w_v, res[0].reshape(w_o.shape), small_sum[:heads], small_sum[heads : 2 * heads], small_sum[2 * heads :].reshape(-1))

    return jax.shard_map(local_run, mesh=mesh, in_specs=in_specs, out_specs=out_specs, check_vma=False)
```

```python
import functools
import math

import jax
import jax.numpy as jnp
from jax import lax
from jax.experimental import pallas as pl
from jax.experimental.pallas import tpu as pltpu
from jax.sharding import PartitionSpec as P

ROPE_THETA = 500000.0
NORM_EPS = 1e-6
LOG2E = 1.4426950408889634
LIMIT = 56 << 20
LANES = 128
FAR_A, FAR_B, NEAR_L, NEAR_R, SUM_L, SUM_R, OUT_L, OUT_R, RELAY_L, RELAY_R = range(10)
PARTS = tuple(zip((RELAY_L, RELAY_R), range(2)))
VMEM = pltpu.VMEM
MESH = pl.DeviceIdType.MESH
NT = (((1,), (1,)), ((), ()))


def rope_tables(start_pos, seq_rows, head_dim):
    half_dim = head_dim // 2
    lane = jnp.arange(head_dim)
    inv_freq = ROPE_THETA ** (-2.0 * (lane % half_dim).astype(jnp.float32) / head_dim)
    positions = (start_pos + jnp.arange(seq_rows)).astype(jnp.float32)
    angles = positions[:, None] * inv_freq[None, :]
    return jnp.cos(angles), jnp.where(lane < half_dim, -1.0, 1.0) * jnp.sin(angles)


def vmem_call(kernel, out_shape, n_in, scratch, collective_id, n_any=0, n_any_in=0):
    n_out = len(out_shape) - n_any
    return pl.pallas_call(
        kernel,
        out_shape=out_shape,
        in_specs=[pl.BlockSpec(memory_space=VMEM)] * (n_in - n_any_in) + [pl.BlockSpec(memory_space=pl.ANY)] * n_any_in,
        out_specs=[pl.BlockSpec(memory_space=VMEM)] * n_out + [pl.BlockSpec(memory_space=pl.ANY)] * n_any,
        scratch_shapes=scratch,
        compiler_params=pltpu.CompilerParams(vmem_limit_bytes=LIMIT, collective_id=collective_id, has_side_effects=True),
    )


def block_of(ref, index, size):
    return ref.at[pl.ds(pl.multiple_of(index * size, size), size), :]


def remote(src, dst, send_sem, recv_sem, device_id):
    return pltpu.make_async_remote_copy(src_ref=src, dst_ref=dst, send_sem=send_sem, recv_sem=recv_sem, device_id=device_id, device_id_type=MESH)


def cross_barrier(me_tp, me_cp, tp_size, cp_size):
    barrier = pltpu.get_barrier_semaphore()
    for axis, me, size in (("cp", me_cp, cp_size), ("tp", me_tp, tp_size)):
        for step in range(1, size):
            pl.semaphore_signal(barrier, inc=1, device_id={axis: lax.rem(me + step, size)}, device_id_type=MESH)
    pl.semaphore_wait(barrier, cp_size + tp_size - 2)


def cols(ref, head, rows=None):
    lanes = pl.ds(pl.multiple_of(head * LANES, LANES), LANES)
    return ref.at[:, lanes] if rows is None else ref.at[rows, lanes]


def sub_rows(core, slot, sub):
    first = core if slot == 0 else 3 - core
    return pl.ds(pl.multiple_of(first * sub, sub), sub)


def share_over_tp(tp_size, me, vec, got, ss, rs):
    copies = []
    for r in range(1, tp_size):
        copy = remote(vec, got.at[r], ss.at[r], rs.at[r], {"tp": lax.rem(me + r, tp_size)})
        copy.start()
        copies.append(copy)

    def finish():
        for copy in copies:
            copy.wait()
        return (vec[...] + got[2]) + (got[1] + got[3])

    return finish


def rolled(t, c, s):
    return t * c + pltpu.roll(t, LANES // 2, 1) * s


def group_barrier(me_tp, me_cp, tp_size, cp_size):
    barrier = pltpu.get_barrier_semaphore()
    for st in range(tp_size):
        for sc in range(cp_size):
            if st or sc:
                pl.semaphore_signal(barrier, inc=1, device_id={"tp": lax.rem(me_tp + st, tp_size), "cp": lax.rem(me_cp + sc, cp_size)}, device_id_type=MESH)
    pl.semaphore_wait(barrier, tp_size * cp_size - 1)


def scatter_qkv(heads, tp_size, cp_size, width, q_lin, k_lin, vec, q_gain, k_gain, cos_t, sin_t, wo_in, v_in, q_out, k_out, v_out, inv_out, wo_out, q16, k16, got, loc, qs, qr, ks, kr, vs, vr, fks, fkr, fvs, fvr, ts, tr, ws, wr, wfs, wfr):
    me_tp = lax.axis_index("tp")
    me = lax.axis_index("cp")
    core = lax.rem(me, 2)
    chip = me // 2
    sub = q_out.shape[1] // 2
    cross_barrier(me_tp, me, tp_size, cp_size)
    finish = share_over_tp(tp_size, me_tp, vec, got, ts, tr)
    far_chips = (1, heads - 1, 2)
    sends = []

    def spread(src, out, ss, rs):
        for r in far_chips:
            dst = lax.rem(chip + r, heads)
            copy = remote(cols(src, dst), out.at[me], ss.at[r], rs.at[r], {"cp": dst * 2 + core})
            copy.start()
            sends.append(copy)

    spread(v_in, v_out, vs, vr)
    shard = wo_in.shape[0]
    keep = pltpu.make_async_copy(wo_in, block_of(wo_out, me_tp, shard), loc.at[4])
    keep.start()
    t_left, t_right, t_far = (lax.rem(me_tp + d, tp_size) for d in (tp_size - 1, 1, 2))
    ways = tuple(enumerate(((t_right, t_left), (t_left, t_right))))
    for k, (_, dst) in ways:
        copy = remote(block_of(wo_in, core, shard // 2), block_of(wo_out, me_tp * 2 + core, shard // 2), ws.at[k], wr.at[k], {"tp": dst})
        copy.start()
        sends.append(copy)
    inv_out[...] = lax.rsqrt(finish() / width + NORM_EPS)
    n_chunk = inv_out.shape[0] // 2
    inv_cols = inv_out[...].T

    def rotate(lin, gain, out16, first):
        for r in range(n_chunk):
            rows = slice(r * LANES, (r + 1) * LANES)
            scale = inv_cols[:, first + r : first + r + 1]
            for h in range(heads):
                lanes = slice(h * LANES, (h + 1) * LANES)
                out16[rows, lanes] = rolled(lin[rows, lanes] * scale * gain[:, lanes], cos_t[rows, :], sin_t[rows, :]).astype(out16.dtype)

    rotate(k_lin, k_gain, k16, n_chunk)
    spread(k16, k_out, ks, kr)
    rotate(q_lin, q_gain, q16, 0)
    own = [pltpu.make_async_copy(cols(k16, chip), k_out.at[me], loc.at[0]), pltpu.make_async_copy(cols(v_in, chip), v_out.at[me], loc.at[1])]
    for r in range(cp_size):
        dst = lax.rem(me + r, cp_size)
        for s in range(2):
            src = cols(q16, dst // 2, sub_rows(lax.rem(dst, 2), s, sub))
            place = q_out.at[me, s * sub : (s + 1) * sub, :]
            if r == 0:
                own.append(pltpu.make_async_copy(src, place, loc.at[2 + s]))
            else:
                copy = remote(src, place, qs.at[r, s], qr.at[r, s], {"cp": dst})
                copy.start()
                sends.append(copy)
    for copy in own:
        copy.start()
    partner = {"cp": me + 1 - 2 * core}
    forwards = []

    def pass_on(part, ss, rs):
        copy = remote(part, part, ss, rs, partner)
        copy.start()
        forwards.append(copy)

    def forward(local, buf, ss, rs, fs, fr):
        for r in (0,) + far_chips:
            src = lax.rem(chip - r + heads, heads) * 2 + core
            if r == 0:
                local.wait()
            else:
                remote(buf.at[src], buf.at[src], ss.at[r], rs.at[r], partner).wait_recv()
            pass_on(buf.at[src], fs.at[r], fr.at[r])

    forward(own[1], v_out, vs, vr, fvs, fvr)
    for k, (src, dst) in ways:
        whole = block_of(wo_out, src * 2 + core, shard // 2)
        remote(whole, whole, ws.at[k], wr.at[k], partner).wait_recv()
        half = block_of(wo_out, (src * 2 + core) * 2 + k, shard // 4)
        copy = remote(half, half, ws.at[2 + k], wr.at[2 + k], {"tp": dst})
        copy.start()
        sends.append(copy)
        pass_on(whole, wfs.at[k], wfr.at[k])
    forward(own[0], k_out, ks, kr, fks, fkr)
    for copy in own[2:] + [keep]:
        copy.wait()
    for k, _ in ways:
        half = block_of(wo_out, (t_far * 2 + core) * 2 + k, shard // 4)
        remote(half, half, ws.at[2 + k], wr.at[2 + k], partner).wait_recv()
        pass_on(half, wfs.at[2 + k], wfr.at[2 + k])
    for copy in sends:
        copy.wait_send()
    for r in range(1, cp_size):
        for s in range(2):
            place = q_out.at[lax.rem(me - r + cp_size, cp_size), s * sub : (s + 1) * sub, :]
            remote(place, place, qs.at[r, s], qr.at[r, s], partner).wait_recv()
    for copy in forwards:
        copy.wait()


def attend(sub, scale, q_ref, k_ref, v_ref, o_ref, lse_ref, k_scr, vt_scr, m_scr, l_scr, acc_scr, s_a, s_b, mx_a):
    blk = pl.program_id(0)
    core = lax.rem(lax.axis_index("cp"), 2)
    coef = scale * LOG2E
    half = k_ref.shape[1] // 2
    cols = q_ref.shape[1]
    chunk = half // 2
    k_scr[blk] = k_ref[0]
    vt_scr[blk] = v_ref[0].T
    m_scr[...] = jnp.full_like(m_scr, -jnp.inf)
    l_scr[...] = jnp.zeros_like(l_scr)
    acc_scr[...] = jnp.zeros_like(acc_scr)

    def fold(op, values):
        return op(values.reshape(values.shape[0] // 8, 8, cols), axis=0)

    def scores(b, h, c):
        kv = slice(h * half + c * chunk, h * half + (c + 1) * chunk)
        return lax.dot_general(k_scr[b, kv, :], q_ref[0], NT, preferred_element_type=jnp.float32)

    def mask(s, h, c):
        kv_pos = h * half + c * chunk + lax.broadcasted_iota(jnp.int32, s.shape, 0)
        col = lax.broadcasted_iota(jnp.int32, s.shape, 1)
        q_pos = jnp.where(col < sub, core * sub + col, (2 - core) * sub + col)
        return jnp.where(kv_pos <= q_pos, s, -jnp.inf)

    def step(buf, mx, b, h, nxt):
        m_old = m_scr[...]
        m_new = jnp.maximum(m_old, mx)
        mc = m_new * coef
        alpha = jnp.exp2((m_old - m_new) * coef)
        lsum = jnp.zeros((8, cols), jnp.float32)
        new_mx = None
        for c in range(2):
            rows = slice(c * chunk, (c + 1) * chunk)
            if nxt is not None:
                nbuf, nb, nh, masked = nxt
                s = scores(nb, nh, c)
                if masked:
                    s = mask(s, nh, c)
                nbuf[rows, :] = s
                part = fold(jnp.max, s)
                new_mx = part if new_mx is None else jnp.maximum(new_mx, part)
            p = jnp.exp2(buf[rows, :] * coef - mc)
            lsum = lsum + fold(jnp.sum, p)
            pv = jnp.dot(vt_scr[b, :, h * half + c * chunk : h * half + (c + 1) * chunk], p.astype(jnp.bfloat16), preferred_element_type=jnp.float32)
            acc_scr[...] = acc_scr[...] * alpha + pv if c == 0 else acc_scr[...] + pv
        l_scr[...] = l_scr[...] * alpha + jnp.sum(lsum, axis=0, keepdims=True)
        m_scr[...] = m_new
        return None if nxt is None else jnp.max(new_mx, axis=0, keepdims=True)

    for c in range(2):
        s_a[c * chunk : (c + 1) * chunk, :] = scores(0, 0, c)
    mx_a[...] = jnp.max(s_a[...], axis=0, keepdims=True)

    def body(b, carry):
        mx_b = step(s_a, mx_a[...], b, 0, (s_b, b, 1, False))
        mx_a[...] = step(s_b, mx_b, b, 1, (s_a, b + 1, 0, False))
        return carry

    lax.fori_loop(0, blk, body, 0)
    for c in range(2):
        rows = slice(c * chunk, (c + 1) * chunk)
        s_a[rows, :] = mask(s_a[rows, :], 0, c)
    mx_b = step(s_a, jnp.max(s_a[...], axis=0, keepdims=True), blk, 0, (s_b, blk, 1, True))
    step(s_b, mx_b, blk, 1, None)
    o_ref[0] = (acc_scr[...] / l_scr[...]).T.astype(o_ref.dtype)
    lse_ref[0] = m_scr[...] * coef + jnp.log2(l_scr[...])


def heads_to_rows(heads, tp_size, cp_size, o_in, o_out, ss, rs):
    me_tp = lax.axis_index("tp")
    me_cp = lax.axis_index("cp")
    core = lax.rem(me_cp, 2)
    head = me_tp * heads + me_cp // 2
    sub = o_out.shape[0]
    place = cols(o_out, head)
    group_barrier(me_tp, me_cp, tp_size, cp_size)
    for finish in range(2):
        if finish:
            for h in range(heads * tp_size):
                part = o_out.at[:, h * LANES : (h + 1) * LANES]
                pltpu.make_async_copy(part, part, rs.at[h]).wait()
        for s in range(2):
            dst_tp = core if s == 0 else 3 - core
            for r in range(cp_size):
                dst_cp = lax.rem(me_cp + r, cp_size)
                src = o_in.at[dst_cp, s * sub : (s + 1) * sub, :]
                copy = remote(src, place, ss.at[s, r], rs.at[head], {"tp": dst_tp, "cp": dst_cp})
                act = copy.wait_send if finish else copy.start
                if r:
                    act()
                    continue
                pl.when(dst_tp != me_tp)(act)
                if not finish:
                    pl.when(dst_tp == me_tp)(pltpu.make_async_copy(src, place, rs.at[head]).start)


def rows_to_heads(heads, tp_size, cp_size, g_in, g_out, ss, rs):
    me_tp = lax.axis_index("tp")
    me_cp = lax.axis_index("cp")
    core = lax.rem(me_cp, 2)
    sub = g_in.shape[0]
    row_core = jnp.where(me_tp < 2, me_tp, 3 - me_tp)
    slot = me_tp // 2
    place = g_out.at[me_cp, pl.ds(pl.multiple_of(slot * sub, sub), sub), :]
    group_barrier(me_tp, me_cp, tp_size, cp_size)
    for finish in range(2):
        if finish:
            for i in range(cp_size):
                for s in range(2):
                    part = g_out.at[i, s * sub : (s + 1) * sub, :]
                    pltpu.make_async_copy(part, part, rs.at[i, s]).wait()
        for rt in range(tp_size):
            dst_tp = lax.rem(me_tp + rt, tp_size)
            for r in range(heads):
                chip = lax.rem(me_cp // 2 + r, heads)
                src = cols(g_in, dst_tp * heads + chip)
                copy = remote(src, place, ss.at[rt, r], rs.at[me_cp, slot], {"tp": dst_tp, "cp": chip * 2 + row_core})
                act = copy.wait_send if finish else copy.start
                if rt or r:
                    act()
                    continue
                pl.when(row_core != core)(act)
                if not finish:
                    pl.when(row_core == core)(pltpu.make_async_copy(src, place, rs.at[me_cp, slot]).start)


def attend_back(heads, tp_size, cp_size, width, scale, q_ref, k_ref, v_ref, o_ref, do_ref, lse_ref, inv, q_gain, k_gain, cos_t, sin_t, gp_in, or_in, q_hbm, k_hbm,
                dq_out, dk_out, dv_out, gain_out, gp_out, oo_out,
                q_lin, k_lin, kt_scr, dqt_scr, dl_scr, dqs, acc_k, acc_v, dq, dk, pk, pv, sk, sv, part, got, loc, qs, qr, pks, pkr, pvs, pvr, ks, kr, vs, vr, ts, tr, gs, gr, os, orr):
    me_tp = lax.axis_index("tp")
    me = lax.axis_index("cp")
    core = lax.rem(me, 2)
    chip = me // 2
    rows = q_ref.shape[1]
    sub = rows // 2
    block_len = k_ref.shape[1]
    coef = scale * LOG2E
    f32 = jnp.float32
    partner = {"cp": me + 1 - 2 * core}
    cross_barrier(me_tp, me, tp_size, cp_size)
    sends = []
    loc_width = heads * LANES
    own = [
        pltpu.make_async_copy(gp_in, block_of(gp_out, me_tp, sub), loc.at[4]),
        pltpu.make_async_copy(or_in.at[:, pl.ds(pl.multiple_of(me_tp * loc_width, loc_width), loc_width)], block_of(oo_out, me_tp, sub), loc.at[5]),
        pltpu.make_async_copy(q_hbm, q_lin, loc.at[6]),
        pltpu.make_async_copy(k_hbm, k_lin, loc.at[7]),
    ]
    for r in range(1, tp_size):
        dst = lax.rem(me_tp + r, tp_size)
        sends.append(remote(or_in.at[:, pl.ds(pl.multiple_of(dst * loc_width, loc_width), loc_width)], block_of(oo_out, me_tp, sub), os.at[r], orr.at[r], {"tp": dst}))
    t_left, t_right, t_far = (lax.rem(me_tp + d, tp_size) for d in (tp_size - 1, 1, 2))
    ways = tuple(enumerate(((t_right, t_left), (t_left, t_right))))
    for k, (_, dst) in ways:
        sends.append(remote(gp_in, block_of(gp_out, me_tp, sub), gs.at[k], gr.at[k], {"tp": dst}))
    for copy in own + sends:
        copy.start()

    def relay(k, src, dst):
        half = block_of(gp_out, src * 2 + k, sub // 2)
        return remote(half, half, gs.at[2 + k], gr.at[2 + k], {"tp": dst})

    def prepare(i, carry):
        kt_scr[i] = k_ref[i].T
        prod = o_ref[i].astype(f32) * do_ref[i].astype(f32)
        dl_scr[i] = jnp.sum(prod.T, axis=0, keepdims=True)
        dqt_scr[i] = jnp.zeros((LANES, rows), f32)
        return carry

    lax.fori_loop(0, cp_size, prepare, 0)

    def tile(i, b, s, e, masked):
        q = q_ref[i]
        do = do_ref[i]
        lse = lse_ref[i]
        delta = dl_scr[i]
        for j in range(block_len // sub):
            kv = slice(j * sub, (j + 1) * sub)
            scores = lax.dot_general(k_ref[b, kv, :], q, NT, preferred_element_type=f32)
            p = jnp.exp2(scores * coef - lse)
            if masked:
                kv_pos = j * sub + lax.broadcasted_iota(jnp.int32, (sub, rows), 0)
                col = lax.broadcasted_iota(jnp.int32, (sub, rows), 1)
                q_pos = jnp.where(col < sub, core * sub + col, (2 - core) * sub + col)
                p = jnp.where(kv_pos <= q_pos, p, 0.0)
            dp = lax.dot_general(v_ref[b, kv, :], do, NT, preferred_element_type=f32)
            ds = (p * (dp - delta)).astype(jnp.bfloat16)
            for acc, left, right in ((acc_v, p.astype(jnp.bfloat16), do), (acc_k, ds, q)):
                new = jnp.dot(left, right, preferred_element_type=f32)
                acc[s, e, kv, :] = new if masked else acc[s, e, kv, :] + new
            dqt_scr[i] += jnp.dot(kt_scr[b, :, kv], ds, preferred_element_type=f32)

    def pair_copies(s):
        return [remote(acc.at[s, 1 - core], dst.at[s], ss.at[s], rs.at[s], partner) for acc, dst, ss, rs in ((acc_k, pk, pks, pkr), (acc_v, pv, pvs, pvr))]

    def home_copies(s):
        dst = {"cp": lax.rem(chip + 1 + s, heads) * 2 + core}
        return [remote(src.at[s], cols(out, chip), ss.at[s], rs.at[s], dst) for src, out, ss, rs in ((sk, dk, ks, kr), (sv, dv_out, vs, vr))]

    def add_pair(s):
        for copy in pair_copies(s):
            copy.wait()
        sk[s] = (acc_k[s, core] + pk[s]) * scale
        sv[s] = (acc_v[s, core] + pv[s]).astype(sv.dtype)

    def key_pair(s, carry):
        def key_block(e, inner):
            b = lax.rem(chip + 1 + s, heads) * 2 + e
            tile(b, b, s, e, True)

            def full(i, last):
                tile(i, b, s, e, False)
                return last

            return lax.fori_loop(b + 1, cp_size, full, inner)

        lax.fori_loop(0, 2, key_block, 0)
        for copy in pair_copies(s):
            copy.start()

        @pl.when(s == 1)
        def _():
            for k, (src, dst) in ways:
                whole = block_of(gp_out, src, sub)
                remote(whole, whole, gs.at[k], gr.at[k], partner).wait_recv()
                relay(k, src, dst).start()

        @pl.when(s > 0)
        def _():
            add_pair(s - 1)
            for copy in home_copies(s - 1):
                copy.start()

        return carry

    lax.fori_loop(0, heads, key_pair, 0)
    for r in range(cp_size):
        dst = lax.rem(me + r, cp_size)
        dqs[dst] = dqt_scr[dst].T * scale
        for s in range(2):
            src = dqs.at[dst, s * sub : (s + 1) * sub, :]
            place = cols(dq, chip, sub_rows(core, s, sub))
            if r == 0:
                copy = pltpu.make_async_copy(src, place, loc.at[s])
                own.append(copy)
            else:
                copy = remote(src, place, qs.at[r, s], qr.at[r, s], {"cp": dst})
                sends.append(copy)
            copy.start()
    last = heads - 1
    add_pair(last)
    for j, (src, out) in enumerate(((sk, dk), (sv, dv_out))):
        copy = pltpu.make_async_copy(src.at[last], cols(out, chip), loc.at[2 + j])
        copy.start()
        own.append(copy)
    for copy in own:
        copy.wait()
    inv_cols = inv[...].T
    n_chunk = inv.shape[0] // 2
    dots = []

    def first_pass(i, grad, lin, gain):
        gains = [jnp.zeros((1, LANES), f32)] * heads
        for r in range(n_chunk):
            part_rows = slice(r * LANES, (r + 1) * LANES)
            c = i * n_chunk + r
            norm = inv_cols[:, c : c + 1]
            total = jnp.zeros((LANES, LANES), f32)
            for h in range(heads):
                lanes = slice(h * LANES, (h + 1) * LANES)
                hat = lin[part_rows, lanes] * norm
                back = rolled(grad[part_rows, lanes], cos_t[part_rows, :], -sin_t[part_rows, :])
                both = back * hat
                gains[h] = gains[h] + jnp.sum(both, axis=0, keepdims=True)
                total = total + both * gain[:, lanes]
                grad[part_rows, lanes] = back * gain[:, lanes]
            dots.append(jnp.sum(total, axis=1, keepdims=True))
        for h in range(heads):
            gain_out[i * heads + h : i * heads + h + 1, :] = gains[h]

    for s in range(last):
        place = cols(dk, lax.rem(chip - 1 - s + heads, heads))
        remote(place, place, ks.at[s], kr.at[s], partner).wait_recv()
    first_pass(1, dk, k_lin, k_gain)
    for r in range(1, cp_size):
        src = lax.rem(me - r + cp_size, cp_size)
        for s in range(2):
            place = cols(dq, src // 2, sub_rows(lax.rem(src, 2), s, sub))
            remote(place, place, qs.at[r, s], qr.at[r, s], partner).wait_recv()
    first_pass(0, dq, q_lin, q_gain)
    part[...] = jnp.concatenate(dots[n_chunk:] + dots[:n_chunk], axis=1).T
    dot_cols = (share_over_tp(tp_size, me_tp, part, got, ts, tr)() / width).T
    for i, (grad, lin, out) in enumerate(((dq, q_lin, dq_out), (dk, k_lin, dk_out))):
        for r in range(n_chunk):
            part_rows = slice(r * LANES, (r + 1) * LANES)
            c = i * n_chunk + r
            norm = inv_cols[:, c : c + 1]
            out[part_rows, :] = (norm * (grad[part_rows, :] - lin[part_rows, :] * norm * dot_cols[:, c : c + 1])).astype(out.dtype)
    for s in range(last):
        sends.extend(home_copies(s))
        place = cols(dv_out, lax.rem(chip - 1 - s + heads, heads))
        remote(place, place, vs.at[s], vr.at[s], partner).wait_recv()
    for r in range(1, tp_size):
        place = block_of(oo_out, lax.rem(me_tp - r + tp_size, tp_size), sub)
        remote(place, place, os.at[r], orr.at[r], partner).wait_recv()
    for k, (src, dst) in ways:
        sends.append(relay(k, src, dst))
        half = block_of(gp_out, t_far * 2 + k, sub // 2)
        remote(half, half, gs.at[2 + k], gr.at[2 + k], partner).wait_recv()
    for copy in sends:
        copy.wait_send()


def reduce_tail(tp_size, cp_size, *refs):
    n_w = 4
    w_in, (dx_in, dy_in, small, y_in) = refs[:n_w], refs[n_w : 2 * n_w]
    refs = refs[2 * n_w :]
    w_out, (dx_out, y_out, small_out) = refs[:n_w], refs[n_w : n_w + 3]
    refs = refs[n_w + 3 :]
    acc, pair, far_a, far_b, fin_l, fin_r = (refs[i * n_w : (i + 1) * n_w] for i in range(6))
    refs = refs[6 * n_w :]
    dxa, dxb, dx_own, dx_fa, dx_fb, dx_fl, dx_fr, dx16, got_small, got_post, ss, rs, ps, pr, fs, fr, loc, sms, smr, gps, gpr = refs
    me_tp = lax.axis_index("tp")
    me_cp = lax.axis_index("cp")
    core = lax.rem(me_cp, 2)
    chip = me_cp // 2
    ring = cp_size // 2
    left, right, far = (lax.rem(chip + d, ring) for d in (ring - 1, 1, 2))
    t_left, t_right, t_far = (lax.rem(me_tp + d, tp_size) for d in (tp_size - 1, 1, 2))
    partner = {"cp": me_cp + 1 - 2 * core}
    to_l, to_r = {"cp": left * 2 + core}, {"cp": right * 2 + core}
    tp_l, tp_r = {"tp": t_left}, {"tp": t_right}
    dx_i, y_i = n_w, n_w + 1
    outs = []

    def ring_sems(t, kind):
        return ss.at[t, kind], rs.at[t, kind]

    def pair_sems(t, kind):
        return fs.at[t, kind], fr.at[t, kind]

    cross_barrier(me_tp, me_cp, tp_size, cp_size)
    sent = []

    def go(src, dst, s_sem, r_sem, device):
        copy = remote(src, dst, s_sem, r_sem, device)
        copy.start()
        sent.append(copy)

    def landed(dst, s_sem, r_sem):
        remote(dst, dst, s_sem, r_sem, partner).wait_recv()

    def piece(ref, t, x, c, part=None):
        size = w_in[t].shape[0] // cp_size
        first = (2 * x + c) * size
        if part is None:
            return ref.at[pl.ds(pl.multiple_of(first, size), size), :]
        return ref.at[pl.ds(pl.multiple_of(first + part * (size // 2), size // 2), size // 2), :]

    def rows_of(ref, y, part=None):
        size = dx_in.shape[0] // tp_size
        if part is None:
            return ref.at[pl.ds(pl.multiple_of(y * size, size), size), :]
        return ref.at[pl.ds(pl.multiple_of(y * size + part * (size // 2), size // 2), size // 2), :]

    def half_of(ref, part):
        size = ref.shape[0] // 2
        return ref.at[pl.ds(part * size, size), :]

    for r in range(1, cp_size):
        go(small, got_small.at[me_cp], sms.at[r], smr.at[r], {"cp": lax.rem(me_cp + r, cp_size)})
    go(rows_of(dx_in, t_far, 0), dx_fa, *ring_sems(dx_i, FAR_A), tp_l)
    go(rows_of(dx_in, t_far, 1), dx_fb, *ring_sems(dx_i, FAR_B), tp_r)
    go(rows_of(dx_in, t_left, 1), half_of(dx_fr, 1), *ring_sems(dx_i, NEAR_L), tp_l)
    go(rows_of(dx_in, t_right, 0), half_of(dx_fl, 0), *ring_sems(dx_i, NEAR_R), tp_r)
    def give(src, stream, out, dev_l, dev_r):
        copy = pltpu.make_async_copy(src, out, loc.at[stream, n_w])
        copy.start()
        outs.append(copy)
        go(src, out, *ring_sems(stream, OUT_L), dev_l)
        go(src, out, *ring_sems(stream, OUT_R), dev_r)

    give(y_in, y_i, rows_of(y_out, me_tp), tp_l, tp_r)
    order = (far, left, right, chip)
    loads = []
    for t in range(n_w):
        for i, x in enumerate(order):
            go(piece(w_in[t], t, x, 1 - core), pair[t].at[x], ps.at[t, i], pr.at[t, i], partner)
            copy = pltpu.make_async_copy(piece(w_in[t], t, x, core), acc[t].at[x], loc.at[t, i])
            copy.start()
            loads.append(copy)
    dx_loads = [
        pltpu.make_async_copy(rows_of(dx_in, t_left, 0), dxa, loc.at[n_w, 0]),
        pltpu.make_async_copy(rows_of(dx_in, t_right, 1), dxb, loc.at[n_w, 1]),
        pltpu.make_async_copy(rows_of(dx_in, me_tp), dx_own, loc.at[n_w, 2]),
    ]
    for copy in dx_loads:
        copy.start()

    for t in range(n_w):
        for i, x in enumerate(order):
            loads[t * 4 + i].wait()
            landed(pair[t].at[x], ps.at[t, i], pr.at[t, i])
            acc[t][x] += pair[t][x]
        go(half_of(acc[t].at[far], 0), far_a[t], *ring_sems(t, FAR_A), to_l)
        go(half_of(acc[t].at[far], 1), far_b[t], *ring_sems(t, FAR_B), to_r)
        go(half_of(acc[t].at[left], 1), half_of(fin_r[t], 1), *ring_sems(t, NEAR_L), to_l)
        go(half_of(acc[t].at[right], 0), half_of(fin_l[t], 0), *ring_sems(t, NEAR_R), to_r)

    got_small[me_cp] = small[...]
    for r in range(1, cp_size):
        landed(got_small.at[lax.rem(me_cp - r + cp_size, cp_size)], sms.at[r], smr.at[r])
    total = got_small[0]
    for i in range(1, cp_size):
        total = total + got_small[i]
    small_out[...] = total
    n_gain = small.shape[0] - got_post.shape[1]

    def second_half(t, acc_l, acc_r, fa, fb, fl, fr, dev_l, dev_r):
        half = fa.shape[0]
        landed(fa, *ring_sems(t, FAR_A))
        acc_l[...] += fa[...]
        landed(fb, *ring_sems(t, FAR_B))
        acc_r[...] += fb[...]
        go(acc_l, half_of(fr, 0), *ring_sems(t, SUM_L), dev_l)
        go(acc_r, half_of(fl, 1), *ring_sems(t, SUM_R), dev_r)

    def all_landed(t, fl, fr):
        landed(half_of(fr, 1), *ring_sems(t, NEAR_L))
        landed(half_of(fl, 0), *ring_sems(t, NEAR_R))
        landed(half_of(fr, 0), *ring_sems(t, SUM_L))
        landed(half_of(fl, 1), *ring_sems(t, SUM_R))

    for t in range(n_w):
        second_half(t, half_of(acc[t].at[left], 0), half_of(acc[t].at[right], 1), far_a[t], far_b[t], fin_l[t], fin_r[t], to_l, to_r)
    for copy in dx_loads:
        copy.wait()
    second_half(dx_i, dxa, dxb, dx_fa, dx_fb, dx_fl, dx_fr, tp_l, tp_r)
    post = small_out.at[pl.ds(n_gain, got_post.shape[1]), :]
    for r in range(1, tp_size):
        go(post, got_post.at[r], gps.at[r], gpr.at[r], {"tp": lax.rem(me_tp + r, tp_size)})

    for t in range(n_w):
        all_landed(t, fin_l[t], fin_r[t])
        acc[t][chip] = acc[t][chip] + (fin_l[t][...] + fin_r[t][...])
        src = acc[t].at[chip]
        dst = piece(w_out[t], t, chip, core)
        give(src, t, dst, to_l, to_r)
        go(src, dst, *pair_sems(t, 0), partner)
    all_landed(dx_i, dx_fl, dx_fr)
    dx16[...] = (dx_own[...] + (dx_fl[...] + dx_fr[...]) + dy_in[...].astype(jnp.float32)).astype(dx16.dtype)
    give(dx16, dx_i, rows_of(dx_out, me_tp), tp_l, tp_r)

    def relay(stream, part_of, x_l, x_r, dev_l, dev_r, pass_on):
        for arrived, x, kind, part, dev in ((OUT_L, x_r, RELAY_L, 0, dev_l), (OUT_R, x_l, RELAY_R, 1, dev_r)):
            whole = part_of(x)
            landed(whole, *ring_sems(stream, arrived))
            half = part_of(x, part)
            go(half, half, *ring_sems(stream, kind), dev)
            if pass_on:
                go(whole, whole, *pair_sems(stream, 1 + part), partner)

    for t in range(n_w):
        relay(t, functools.partial(lambda ref, t, x, part=None: piece(ref, t, x, core, part), w_out[t], t), left, right, to_l, to_r, True)
    for stream, out in ((y_i, y_out), (dx_i, dx_out)):
        relay(stream, functools.partial(rows_of, out), t_left, t_right, tp_l, tp_r, False)

    sums = small_out[n_gain:, :]
    for r in range(1, tp_size):
        landed(got_post.at[r], gps.at[r], gpr.at[r])
    sums = (sums + got_post[2]) + (got_post[1] + got_post[3])

    for t in range(n_w):
        for kind, part in PARTS:
            half = piece(w_out[t], t, far, core, part)
            landed(half, *ring_sems(t, kind))
            go(half, half, *pair_sems(t, 3 + part), partner)
    for stream, out in ((y_i, y_out), (dx_i, dx_out)):
        for kind, part in PARTS:
            landed(rows_of(out, t_far, part), *ring_sems(stream, kind))
    for t in range(n_w):
        for i, x in enumerate((chip, right, left)):
            landed(piece(w_out[t], t, x, 1 - core), *pair_sems(t, i))
        for part in range(2):
            landed(piece(w_out[t], t, far, 1 - core, part), *pair_sems(t, 3 + part))
    for copy in outs:
        copy.wait()
    for copy in sent:
        copy.wait_send()
    small_out[n_gain:, :] = sums


def solution(mesh):
    tp_size = mesh.shape["tp"]
    cp_size = mesh.shape["cp"]
    act_spec = P("dp", "cp", None)
    col_spec = P(None, "tp", None)
    part_col = P("dp", "tp", None)
    in_specs = (act_spec, col_spec, col_spec, col_spec, P("tp", None, None), P("tp", None), P("tp", None), P(None), act_spec)
    out_specs = (act_spec, act_spec, part_col, part_col, part_col, P(("dp", "tp"), None, None), P(("dp", "tp"), None), P(("dp", "tp"), None), P("dp"))
    dma = pltpu.SemaphoreType.DMA

    def local_run(x_in, w_q, w_k, w_v, w_o, q_norm_w, k_norm_w, post_norm_w, grad_y):
        n_batch, block_len, d_model = x_in.shape
        heads, head_dim = w_q.shape[1:]
        assert n_batch == 1 and w_k.shape[1] == heads and cp_size == 2 * heads and tp_size == 4
        sub = block_len // tp_size
        rows = 2 * sub
        width = heads * head_dim * tp_size
        scale = head_dim ** -0.5
        f32 = jnp.float32
        b16 = jnp.bfloat16
        tp_index = lax.axis_index("tp")
        cp_index = lax.axis_index("cp")
        cos_tab, sin_tab = rope_tables(cp_index * block_len, block_len, head_dim)
        x_loc = x_in[0]
        dy_loc = grad_y[0]
        w_q2, w_k2, w_v2 = (w.reshape(d_model, -1) for w in (w_q, w_k, w_v))
        gains = [g.reshape(1, -1) for g in (q_norm_w, k_norm_w)]
        loc_width = heads * head_dim

        q_lin = jnp.dot(x_loc, w_q2, preferred_element_type=f32)
        k_lin = jnp.dot(x_loc, w_k2, preferred_element_type=f32)
        v_val = jnp.dot(x_loc, w_v2, preferred_element_type=f32).astype(b16)
        vec = jnp.stack([jnp.sum(t * t, axis=1) for t in (q_lin, k_lin)]).reshape(-1, LANES)
        vec_shape = jax.ShapeDtypeStruct(vec.shape, f32)
        kv_shape = jax.ShapeDtypeStruct((cp_size, block_len, head_dim), b16)
        lin16 = VMEM((block_len, loc_width), b16)
        tp_scratch = VMEM((tp_size,) + vec.shape, f32)
        q_all, k_all, v_all, inv, w_o_full = vmem_call(
            functools.partial(scatter_qkv, heads, tp_size, cp_size, width),
            [jax.ShapeDtypeStruct((cp_size, rows, head_dim), b16), kv_shape, kv_shape, vec_shape, jax.ShapeDtypeStruct((width, d_model), b16)],
            9,
            [lin16, lin16, tp_scratch, dma((5,))] + [dma((cp_size, 2))] * 2 + [dma((heads,))] * 8 + [dma((tp_size,))] * 6,
            0,
            1,
            1,
        )(q_lin, k_lin, vec, *gains, cos_tab, sin_tab, w_o.reshape(-1, d_model), v_val)

        qspec = pl.BlockSpec((1, rows, head_dim), lambda i: (i, 0, 0))
        lspec = pl.BlockSpec((1, 1, rows), lambda i: (i, 0, 0))
        kvspec = pl.BlockSpec((1, block_len, head_dim), lambda i: (i, 0, 0))
        pair_flops = cp_size * (cp_size + 1) // 2 * rows * block_len * head_dim * 2
        o_all, lse = pl.pallas_call(
            functools.partial(attend, sub, scale),
            grid=(cp_size,),
            in_specs=[qspec, kvspec, kvspec],
            out_specs=[qspec, lspec],
            out_shape=[jax.ShapeDtypeStruct((cp_size, rows, head_dim), b16), jax.ShapeDtypeStruct((cp_size, 1, rows), f32)],
            scratch_shapes=[VMEM((cp_size, block_len, head_dim), b16), VMEM((cp_size, head_dim, block_len), b16), VMEM((1, rows), f32), VMEM((1, rows), f32), VMEM((head_dim, rows), f32)]
            + [VMEM((block_len // 2, rows), f32)] * 2 + [VMEM((1, rows), f32)],
            compiler_params=pltpu.CompilerParams(vmem_limit_bytes=LIMIT),
            cost_estimate=pl.CostEstimate(flops=2 * pair_flops, bytes_accessed=6 << 20, transcendentals=0),
        )(q_all, k_all, v_all)

        n_heads = heads * tp_size
        o_rows = vmem_call(
            functools.partial(heads_to_rows, heads, tp_size, cp_size),
            [jax.ShapeDtypeStruct((sub, width), b16)],
            1,
            [dma((2, cp_size)), dma((n_heads,))],
            1,
        )(o_all)[0]

        x_rows = lax.dynamic_slice_in_dim(x_loc, tp_index * sub, sub, 0)
        dy_rows = lax.dynamic_slice_in_dim(dy_loc, tp_index * sub, sub, 0)
        dy_f = dy_rows.astype(f32)
        proj = jnp.dot(o_rows, w_o_full, preferred_element_type=f32)
        post_inv = lax.rsqrt(jnp.mean(proj * proj, axis=-1, keepdims=True) + NORM_EPS)
        post_hat = proj * post_inv
        y_rows = (x_rows + post_hat * post_norm_w).astype(b16)
        grad_post = jnp.sum(dy_f * post_hat, axis=0)
        grad_hat = dy_f * post_norm_w
        gp_rows = (post_inv * (grad_hat - post_hat * jnp.mean(grad_hat * post_hat, axis=-1, keepdims=True))).astype(b16)
        do_rows = lax.dot_general(gp_rows, w_o_full, NT, preferred_element_type=f32).astype(b16)

        do_all = vmem_call(
            functools.partial(rows_to_heads, heads, tp_size, cp_size),
            [jax.ShapeDtypeStruct((cp_size, rows, head_dim), b16)],
            1,
            [dma((tp_size, heads)), dma((cp_size, 2))],
            2,
        )(do_rows)[0]

        lin_h, f_lin = jax.ShapeDtypeStruct((block_len, loc_width), b16), VMEM((block_len, loc_width), f32)
        head_f = VMEM((heads, block_len, head_dim), f32)
        pair_f = VMEM((heads, 2, block_len, head_dim), f32)
        dq16, dk16, dv16, gain_grads, grad_proj, o_own = vmem_call(
            functools.partial(attend_back, heads, tp_size, cp_size, width, scale),
            [lin_h, lin_h, lin_h, jax.ShapeDtypeStruct((2 * heads, head_dim), f32), jax.ShapeDtypeStruct((block_len, d_model), b16), lin_h],
            15,
            [f_lin, f_lin, VMEM((cp_size, head_dim, block_len), b16), VMEM((cp_size, head_dim, rows), f32), VMEM((cp_size, 1, rows), f32), VMEM((cp_size, rows, head_dim), f32)]
            + [pair_f, pair_f, f_lin, f_lin, head_f, head_f, head_f, VMEM((heads, block_len, head_dim), b16), VMEM(vec.shape, f32), tp_scratch, dma((8,))]
            + [dma((cp_size, 2))] * 2 + [dma((heads,))] * 8 + [dma((tp_size,))] * 6,
            3,
            2,
            2,
        )(q_all, k_all, v_all, o_all, do_all, lse, inv, *gains, cos_tab, sin_tab, gp_rows, o_rows, q_lin, k_lin)

        def wgrad(left, right):
            return lax.dot_general(left, right, (((0,), (0,)), ((), ())), preferred_element_type=f32)

        grad_w_o, grad_w_v, grad_w_q, grad_w_k = wgrad(o_own, grad_proj), wgrad(x_loc, dv16), wgrad(x_loc, dq16), wgrad(x_loc, dk16)
        dx_part = sum(lax.dot_general(g, w, NT, preferred_element_type=f32) for g, w in ((dq16, w_q2), (dk16, w_k2), (dv16, w_v2)))
        w_parts = [grad_w_o, grad_w_v, grad_w_q, grad_w_k]
        small = jnp.concatenate([gain_grads, grad_post.reshape(-1, head_dim)], axis=0)
        any_spec = pl.BlockSpec(memory_space=pl.ANY)
        vmem_spec = pl.BlockSpec(memory_space=VMEM)

        def bufs(lead, div):
            return [VMEM(lead + (w.shape[0] // div, w.shape[1]), f32) for w in w_parts]

        ring = cp_size // 2
        rows_dx, half_dx = VMEM((sub, d_model), f32), VMEM((sub // 2, d_model), f32)
        res = pl.pallas_call(
            functools.partial(reduce_tail, tp_size, cp_size),
            out_shape=[jax.ShapeDtypeStruct(w.shape, f32) for w in w_parts] + [jax.ShapeDtypeStruct((block_len, d_model), b16)] * 2 + [jax.ShapeDtypeStruct(small.shape, f32)],
            in_specs=[any_spec] * 5 + [vmem_spec] * 3,
            out_specs=[any_spec] * 6 + [vmem_spec],
            scratch_shapes=bufs((ring,), cp_size) * 2 + bufs((), 2 * cp_size) * 2 + bufs((), cp_size) * 2
            + [half_dx, half_dx, rows_dx, half_dx, half_dx, rows_dx, rows_dx, VMEM((sub, d_model), b16)]
            + [VMEM((cp_size,) + small.shape, f32), VMEM((tp_size, d_model // head_dim, head_dim), f32)]
            + [dma((6, 10))] * 2 + [dma((4, 4))] * 2 + [dma((4, 5))] * 2 + [dma((6, 5))] + [dma((cp_size,))] * 2 + [dma((tp_size,))] * 2,
            compiler_params=pltpu.CompilerParams(vmem_limit_bytes=LIMIT, collective_id=6, has_side_effects=True),
        )(*w_parts, dx_part, dy_rows, small, y_rows)
        grad_w_v, grad_w_q, grad_w_k = (g.reshape(w_q.shape) for g in res[1:4])
        grad_x, y_out, small_sum = res[4:]
        return (y_out[None], grad_x[None], grad_w_q, grad_w_k, grad_w_v, res[0].reshape(w_o.shape), small_sum[:heads], small_sum[heads : 2 * heads], small_sum[2 * heads :].reshape(-1))

    return jax.shard_map(local_run, mesh=mesh, in_specs=in_specs, out_specs=out_specs, check_vma=False)
```

```python
import functools
import math

import jax
import jax.numpy as jnp
from jax import lax
from jax.experimental import pallas as pl
from jax.experimental.pallas import tpu as pltpu
from jax.sharding import PartitionSpec as P

ROPE_THETA = 500000.0
NORM_EPS = 1e-6
LOG2E = 1.4426950408889634
LIMIT = 61 << 20
LANES = 128
FAR_A, FAR_B, NEAR_L, NEAR_R, SUM_L, SUM_R, OUT_L, OUT_R, RELAY_L, RELAY_R = range(10)
BOTH = range(2)
PARTS = tuple(zip((RELAY_L, RELAY_R), BOTH))
VMEM = pltpu.VMEM
MESH = pl.DeviceIdType.MESH
NT = (((1,), (1,)), ((), ()))


def rope_tables(start_pos, seq_rows, head_dim):
    half_dim = head_dim // 2
    lane = jnp.arange(head_dim)
    inv_freq = ROPE_THETA ** (-2.0 * (lane % half_dim).astype(jnp.float32) / head_dim)
    positions = (start_pos + jnp.arange(seq_rows)).astype(jnp.float32)
    angles = positions[:, None] * inv_freq[None, :]
    return jnp.cos(angles), jnp.where(lane < half_dim, -1.0, 1.0) * jnp.sin(angles)


def vmem_call(kernel, out_shape, n_in, scratch, collective_id, n_any=0, n_any_in=0):
    n_out = len(out_shape) - n_any
    return pl.pallas_call(
        kernel,
        out_shape=out_shape,
        in_specs=[pl.BlockSpec(memory_space=VMEM)] * (n_in - n_any_in) + [pl.BlockSpec(memory_space=pl.ANY)] * n_any_in,
        out_specs=[pl.BlockSpec(memory_space=VMEM)] * n_out + [pl.BlockSpec(memory_space=pl.ANY)] * n_any,
        scratch_shapes=scratch,
        compiler_params=pltpu.CompilerParams(vmem_limit_bytes=LIMIT, collective_id=collective_id, has_side_effects=True),
    )


def block_of(ref, index, size):
    return ref.at[pl.ds(pl.multiple_of(index * size, size), size), :]


def remote(src, dst, send_sem, recv_sem, device_id):
    return pltpu.make_async_remote_copy(src_ref=src, dst_ref=dst, send_sem=send_sem, recv_sem=recv_sem, device_id=device_id, device_id_type=MESH)


def cross_barrier(me_tp, me_cp, tp_size, cp_size):
    barrier = pltpu.get_barrier_semaphore()
    for axis, me, size in (("cp", me_cp, cp_size), ("tp", me_tp, tp_size)):
        for step in range(1, size):
            pl.semaphore_signal(barrier, inc=1, device_id={axis: lax.rem(me + step, size)}, device_id_type=MESH)
    pl.semaphore_wait(barrier, cp_size + tp_size - 2)


def cols(ref, head, rows=None):
    lanes = pl.ds(pl.multiple_of(head * LANES, LANES), LANES)
    return ref.at[:, lanes] if rows is None else ref.at[rows, lanes]


def sub_rows(core, slot, sub):
    first = core if slot == 0 else 3 - core
    return pl.ds(pl.multiple_of(first * sub, sub), sub)


def share_over_tp(tp_size, me, vec, got, ss, rs):
    copies = []
    for r in range(1, tp_size):
        copy = remote(vec, got.at[r], ss.at[r], rs.at[r], {"tp": lax.rem(me + r, tp_size)})
        copy.start()
        copies.append(copy)

    def finish():
        for copy in copies:
            copy.wait()
        return (vec[...] + got[2]) + (got[1] + got[3])

    return finish


def rolled(t, c, s):
    return t * c + pltpu.roll(t, LANES // 2, 1) * s


def group_barrier(me_tp, me_cp, tp_size, cp_size):
    barrier = pltpu.get_barrier_semaphore()
    for st in range(tp_size):
        for sc in range(cp_size):
            if st or sc:
                pl.semaphore_signal(barrier, inc=1, device_id={"tp": lax.rem(me_tp + st, tp_size), "cp": lax.rem(me_cp + sc, cp_size)}, device_id_type=MESH)
    pl.semaphore_wait(barrier, tp_size * cp_size - 1)


def scatter_qkv(heads, tp_size, cp_size, width, q_lin, k_lin, vec, q_gain, k_gain, cos_t, sin_t, wo_in, v_in, q_out, k_out, v_out, inv_out, wo_out, q16, k16, got, loc, qs, qr, ks, kr, vs, vr, fks, fkr, fvs, fvr, ts, tr, ws, wr, wfs, wfr):
    me_tp = lax.axis_index("tp")
    me = lax.axis_index("cp")
    core = lax.rem(me, 2)
    chip = me // 2
    sub = q_out.shape[1] // 2
    cross_barrier(me_tp, me, tp_size, cp_size)
    finish = share_over_tp(tp_size, me_tp, vec, got, ts, tr)
    far_chips = (1, heads - 1, 2)
    sends = []

    def spread(src, out, ss, rs):
        for r in far_chips:
            dst = lax.rem(chip + r, heads)
            copy = remote(cols(src, dst), out.at[me], ss.at[r], rs.at[r], {"cp": dst * 2 + core})
            copy.start()
            sends.append(copy)

    spread(v_in, v_out, vs, vr)
    shard = wo_in.shape[0]
    keep = pltpu.make_async_copy(wo_in, block_of(wo_out, me_tp, shard), loc.at[4])
    keep.start()
    t_left, t_right, t_far = (lax.rem(me_tp + d, tp_size) for d in (tp_size - 1, 1, 2))
    ways = tuple(enumerate(((t_right, t_left), (t_left, t_right))))
    for k, (_, dst) in ways:
        copy = remote(block_of(wo_in, core, shard // 2), block_of(wo_out, me_tp * 2 + core, shard // 2), ws.at[k], wr.at[k], {"tp": dst})
        copy.start()
        sends.append(copy)
    inv_out[...] = lax.rsqrt(finish() / width + NORM_EPS)
    n_chunk = inv_out.shape[0] // 2
    inv_cols = inv_out[...].T

    def rotate(lin, gain, out16, first):
        for r in range(n_chunk):
            rows = slice(r * LANES, (r + 1) * LANES)
            scale = inv_cols[:, first + r : first + r + 1]
            for h in range(heads):
                lanes = slice(h * LANES, (h + 1) * LANES)
                out16[rows, lanes] = rolled(lin[rows, lanes] * scale * gain[:, lanes], cos_t[rows, :], sin_t[rows, :]).astype(out16.dtype)

    rotate(k_lin, k_gain, k16, n_chunk)
    spread(k16, k_out, ks, kr)
    rotate(q_lin, q_gain, q16, 0)
    own = [pltpu.make_async_copy(cols(k16, chip), k_out.at[me], loc.at[0]), pltpu.make_async_copy(cols(v_in, chip), v_out.at[me], loc.at[1])]
    for r in range(cp_size):
        dst = lax.rem(me + r, cp_size)
        for s in BOTH:
            src = cols(q16, dst // 2, sub_rows(lax.rem(dst, 2), s, sub))
            place = q_out.at[me, s * sub : (s + 1) * sub, :]
            if r == 0:
                own.append(pltpu.make_async_copy(src, place, loc.at[2 + s]))
            else:
                copy = remote(src, place, qs.at[r, s], qr.at[r, s], {"cp": dst})
                copy.start()
                sends.append(copy)
    for copy in own:
        copy.start()
    partner = {"cp": me + 1 - 2 * core}
    forwards = []

    def pass_on(part, ss, rs):
        copy = remote(part, part, ss, rs, partner)
        copy.start()
        forwards.append(copy)

    def forward(local, buf, ss, rs, fs, fr):
        for r in (0,) + far_chips:
            src = lax.rem(chip - r + heads, heads) * 2 + core
            if r == 0:
                local.wait()
            else:
                remote(buf.at[src], buf.at[src], ss.at[r], rs.at[r], partner).wait_recv()
            pass_on(buf.at[src], fs.at[r], fr.at[r])

    forward(own[1], v_out, vs, vr, fvs, fvr)
    for k, (src, dst) in ways:
        whole = block_of(wo_out, src * 2 + core, shard // 2)
        remote(whole, whole, ws.at[k], wr.at[k], partner).wait_recv()
        half = block_of(wo_out, (src * 2 + core) * 2 + k, shard // 4)
        copy = remote(half, half, ws.at[2 + k], wr.at[2 + k], {"tp": dst})
        copy.start()
        sends.append(copy)
        pass_on(whole, wfs.at[k], wfr.at[k])
    forward(own[0], k_out, ks, kr, fks, fkr)
    for copy in own[2:] + [keep]:
        copy.wait()
    for k, _ in ways:
        half = block_of(wo_out, (t_far * 2 + core) * 2 + k, shard // 4)
        remote(half, half, ws.at[2 + k], wr.at[2 + k], partner).wait_recv()
        pass_on(half, wfs.at[2 + k], wfr.at[2 + k])
    for copy in sends:
        copy.wait_send()
    for r in range(1, cp_size):
        for s in BOTH:
            place = q_out.at[lax.rem(me - r + cp_size, cp_size), s * sub : (s + 1) * sub, :]
            remote(place, place, qs.at[r, s], qr.at[r, s], partner).wait_recv()
    for copy in forwards:
        copy.wait()


def attend(sub, scale, q_ref, k_ref, v_ref, o_ref, lse_ref, k_scr, vt_scr, m_scr, l_scr, acc_scr, s_a, s_b, mx_a):
    blk = pl.program_id(0)
    core = lax.rem(lax.axis_index("cp"), 2)
    coef = scale * LOG2E
    half = k_ref.shape[1] // 2
    cols = q_ref.shape[1]
    chunk = half // 2
    k_scr[blk] = k_ref[0]
    vt_scr[blk] = v_ref[0].T
    m_scr[...] = jnp.full_like(m_scr, -jnp.inf)
    l_scr[...] = jnp.zeros_like(l_scr)
    acc_scr[...] = jnp.zeros_like(acc_scr)

    def fold(op, values):
        return op(values.reshape(values.shape[0] // 8, 8, cols), axis=0)

    def scores(b, h, c):
        kv = slice(h * half + c * chunk, h * half + (c + 1) * chunk)
        return lax.dot_general(k_scr[b, kv, :], q_ref[0], NT, preferred_element_type=jnp.float32)

    def mask(s, h, c):
        kv_pos = h * half + c * chunk + lax.broadcasted_iota(jnp.int32, s.shape, 0)
        col = lax.broadcasted_iota(jnp.int32, s.shape, 1)
        q_pos = jnp.where(col < sub, core * sub + col, (2 - core) * sub + col)
        return jnp.where(kv_pos <= q_pos, s, -jnp.inf)

    def step(buf, mx, b, h, nxt):
        m_old = m_scr[...]
        m_new = jnp.maximum(m_old, mx)
        mc = m_new * coef
        alpha = jnp.exp2((m_old - m_new) * coef)
        lsum = jnp.zeros((8, cols), jnp.float32)
        new_mx = None
        for c in BOTH:
            rows = slice(c * chunk, (c + 1) * chunk)
            if nxt is not None:
                nbuf, nb, nh, masked = nxt
                s = scores(nb, nh, c)
                if masked:
                    s = mask(s, nh, c)
                nbuf[rows, :] = s
                part = fold(jnp.max, s)
                new_mx = part if new_mx is None else jnp.maximum(new_mx, part)
            p = jnp.exp2(buf[rows, :] * coef - mc)
            lsum = lsum + fold(jnp.sum, p)
            pv = jnp.dot(vt_scr[b, :, h * half + c * chunk : h * half + (c + 1) * chunk], p.astype(jnp.bfloat16), preferred_element_type=jnp.float32)
            acc_scr[...] = acc_scr[...] * alpha + pv if c == 0 else acc_scr[...] + pv
        l_scr[...] = l_scr[...] * alpha + jnp.sum(lsum, axis=0, keepdims=True)
        m_scr[...] = m_new
        return None if nxt is None else jnp.max(new_mx, axis=0, keepdims=True)

    for c in BOTH:
        s_a[c * chunk : (c + 1) * chunk, :] = scores(0, 0, c)
    mx_a[...] = jnp.max(s_a[...], axis=0, keepdims=True)

    def body(b, carry):
        mx_b = step(s_a, mx_a[...], b, 0, (s_b, b, 1, False))
        mx_a[...] = step(s_b, mx_b, b, 1, (s_a, b + 1, 0, False))
        return carry

    lax.fori_loop(0, blk, body, 0)
    for c in BOTH:
        rows = slice(c * chunk, (c + 1) * chunk)
        s_a[rows, :] = mask(s_a[rows, :], 0, c)
    mx_b = step(s_a, jnp.max(s_a[...], axis=0, keepdims=True), blk, 0, (s_b, blk, 1, True))
    step(s_b, mx_b, blk, 1, None)
    o_ref[0] = (acc_scr[...] / l_scr[...]).T.astype(o_ref.dtype)
    lse_ref[0] = m_scr[...] * coef + jnp.log2(l_scr[...])


def heads_to_rows(heads, tp_size, cp_size, o_in, o_out, ss, rs):
    me_tp = lax.axis_index("tp")
    me_cp = lax.axis_index("cp")
    core = lax.rem(me_cp, 2)
    head = me_tp * heads + me_cp // 2
    sub = o_out.shape[0]
    place = cols(o_out, head)
    group_barrier(me_tp, me_cp, tp_size, cp_size)
    for finish in BOTH:
        if finish:
            for h in range(heads * tp_size):
                part = o_out.at[:, h * LANES : (h + 1) * LANES]
                pltpu.make_async_copy(part, part, rs.at[h]).wait()
        for s in BOTH:
            dst_tp = core if s == 0 else 3 - core
            for r in range(cp_size):
                dst_cp = lax.rem(me_cp + r, cp_size)
                src = o_in.at[dst_cp, s * sub : (s + 1) * sub, :]
                copy = remote(src, place, ss.at[s, r], rs.at[head], {"tp": dst_tp, "cp": dst_cp})
                act = copy.wait_send if finish else copy.start
                if r:
                    act()
                    continue
                pl.when(dst_tp != me_tp)(act)
                if not finish:
                    pl.when(dst_tp == me_tp)(pltpu.make_async_copy(src, place, rs.at[head]).start)


def rows_to_heads(heads, tp_size, cp_size, g_in, g_out, ss, rs):
    me_tp = lax.axis_index("tp")
    me_cp = lax.axis_index("cp")
    core = lax.rem(me_cp, 2)
    sub = g_in.shape[0]
    row_core = jnp.where(me_tp < 2, me_tp, 3 - me_tp)
    slot = me_tp // 2
    place = g_out.at[me_cp, pl.ds(pl.multiple_of(slot * sub, sub), sub), :]
    group_barrier(me_tp, me_cp, tp_size, cp_size)
    for finish in BOTH:
        if finish:
            for i in range(cp_size):
                for s in BOTH:
                    part = g_out.at[i, s * sub : (s + 1) * sub, :]
                    pltpu.make_async_copy(part, part, rs.at[i, s]).wait()
        for rt in range(tp_size):
            dst_tp = lax.rem(me_tp + rt, tp_size)
            for r in range(heads):
                chip = lax.rem(me_cp // 2 + r, heads)
                src = cols(g_in, dst_tp * heads + chip)
                copy = remote(src, place, ss.at[rt, r], rs.at[me_cp, slot], {"tp": dst_tp, "cp": chip * 2 + row_core})
                act = copy.wait_send if finish else copy.start
                if rt or r:
                    act()
                    continue
                pl.when(row_core != core)(act)
                if not finish:
                    pl.when(row_core == core)(pltpu.make_async_copy(src, place, rs.at[me_cp, slot]).start)


def attend_back(heads, tp_size, cp_size, width, scale, q_ref, k_ref, v_ref, o_ref, do_ref, lse_ref, inv, q_gain, k_gain, cos_t, sin_t, gp_in, or_in, q_hbm, k_hbm,
                dq_out, dk_out, dv_out, gain_out, gp_out, oo_out,
                q_lin, k_lin, kt_scr, dqt_scr, dl_scr, dqs, acc_k, acc_v, dq, dk, pk, pv, sk, sv, part, got, loc, qs, qr, pks, pkr, pvs, pvr, ks, kr, vs, vr, ts, tr, gs, gr, os, orr):
    me_tp = lax.axis_index("tp")
    me = lax.axis_index("cp")
    core = lax.rem(me, 2)
    chip = me // 2
    rows = q_ref.shape[1]
    sub = rows // 2
    block_len = k_ref.shape[1]
    coef = scale * LOG2E
    f32 = jnp.float32
    partner = {"cp": me + 1 - 2 * core}
    cross_barrier(me_tp, me, tp_size, cp_size)
    sends = []
    loc_width = heads * LANES
    own = [
        pltpu.make_async_copy(gp_in, block_of(gp_out, me_tp, sub), loc.at[4]),
        pltpu.make_async_copy(or_in.at[:, pl.ds(pl.multiple_of(me_tp * loc_width, loc_width), loc_width)], block_of(oo_out, me_tp, sub), loc.at[5]),
        pltpu.make_async_copy(q_hbm, q_lin, loc.at[6]),
        pltpu.make_async_copy(k_hbm, k_lin, loc.at[7]),
    ]
    for r in range(1, tp_size):
        dst = lax.rem(me_tp + r, tp_size)
        sends.append(remote(or_in.at[:, pl.ds(pl.multiple_of(dst * loc_width, loc_width), loc_width)], block_of(oo_out, me_tp, sub), os.at[r], orr.at[r], {"tp": dst}))
    t_left, t_right, t_far = (lax.rem(me_tp + d, tp_size) for d in (tp_size - 1, 1, 2))
    ways = tuple(enumerate(((t_right, t_left), (t_left, t_right))))
    for k, (_, dst) in ways:
        sends.append(remote(gp_in, block_of(gp_out, me_tp, sub), gs.at[k], gr.at[k], {"tp": dst}))
    for copy in own + sends:
        copy.start()

    def relay(k, src, dst):
        half = block_of(gp_out, src * 2 + k, sub // 2)
        return remote(half, half, gs.at[2 + k], gr.at[2 + k], {"tp": dst})

    def prepare(i, carry):
        kt_scr[i] = k_ref[i].T
        prod = o_ref[i].astype(f32) * do_ref[i].astype(f32)
        dl_scr[i] = jnp.sum(prod.T, axis=0, keepdims=True)
        dqt_scr[i] = jnp.zeros((LANES, rows), f32)
        return carry

    lax.fori_loop(0, cp_size, prepare, 0)

    def tile(i, b, s, e, masked):
        q = q_ref[i]
        do = do_ref[i]
        lse = lse_ref[i]
        delta = dl_scr[i]
        for j in range(block_len // sub):
            kv = slice(j * sub, (j + 1) * sub)
            scores = lax.dot_general(k_ref[b, kv, :], q, NT, preferred_element_type=f32)
            p = jnp.exp2(scores * coef - lse)
            if masked:
                kv_pos = j * sub + lax.broadcasted_iota(jnp.int32, (sub, rows), 0)
                col = lax.broadcasted_iota(jnp.int32, (sub, rows), 1)
                q_pos = jnp.where(col < sub, core * sub + col, (2 - core) * sub + col)
                p = jnp.where(kv_pos <= q_pos, p, 0.0)
            dp = lax.dot_general(v_ref[b, kv, :], do, NT, preferred_element_type=f32)
            ds = (p * (dp - delta)).astype(jnp.bfloat16)
            for acc, left, right in ((acc_v, p.astype(jnp.bfloat16), do), (acc_k, ds, q)):
                new = jnp.dot(left, right, preferred_element_type=f32)
                acc[s, e, kv, :] = new if masked else acc[s, e, kv, :] + new
            dqt_scr[i] += jnp.dot(kt_scr[b, :, kv], ds, preferred_element_type=f32)

    def pair_copies(s):
        return [remote(acc.at[s, 1 - core], dst.at[s], ss.at[s], rs.at[s], partner) for acc, dst, ss, rs in ((acc_k, pk, pks, pkr), (acc_v, pv, pvs, pvr))]

    def home_copies(s):
        dst = {"cp": lax.rem(chip + 1 + s, heads) * 2 + core}
        return [remote(src.at[s], cols(out, chip), ss.at[s], rs.at[s], dst) for src, out, ss, rs in ((sk, dk, ks, kr), (sv, dv_out, vs, vr))]

    def add_pair(s):
        for copy in pair_copies(s):
            copy.wait()
        sk[s] = (acc_k[s, core] + pk[s]) * scale
        sv[s] = (acc_v[s, core] + pv[s]).astype(sv.dtype)

    last = heads - 1

    def dq_copies(r):
        dst = lax.rem(me + r, cp_size)
        copies = []
        for s in BOTH:
            src = dqs.at[dst, s * sub : (s + 1) * sub, :]
            place = cols(dq, chip, sub_rows(core, s, sub))
            copies.append(remote(src, place, qs.at[r, s], qr.at[r, s], {"cp": dst}) if r else pltpu.make_async_copy(src, place, loc.at[s]))
        return copies

    def send_dq(early):
        for r in range(cp_size):
            dst = lax.rem(me + r, cp_size)
            ready = dst // 2 < chip

            @pl.when(ready if early else jnp.logical_not(ready))
            def _():
                dqs[dst] = dqt_scr[dst].T * scale
                for copy in dq_copies(r):
                    copy.start()

    def key_pair(s, carry):
        def key_block(e, inner):
            b = lax.rem(chip + 1 + s, heads) * 2 + e
            tile(b, b, s, e, True)

            def full(i, last):
                tile(i, b, s, e, False)
                return last

            lax.fori_loop(b + 1, cp_size, full, inner)

            @pl.when(jnp.logical_and(e < 1, s > 0))
            def _():
                add_pair(s - 1)
                for copy in home_copies(s - 1):
                    copy.start()

            return inner

        @pl.when(s == last)
        def _():
            send_dq(True)

        lax.fori_loop(0, 2, key_block, 0)
        for copy in pair_copies(s):
            copy.start()

        @pl.when(s == 1)
        def _():
            for k, (src, dst) in ways:
                whole = block_of(gp_out, src, sub)
                remote(whole, whole, gs.at[k], gr.at[k], partner).wait_recv()
                relay(k, src, dst).start()

        return carry

    lax.fori_loop(0, heads, key_pair, 0)
    send_dq(False)
    own.extend(dq_copies(0))
    for r in range(1, cp_size):
        sends.extend(dq_copies(r))
    add_pair(last)
    for j, (src, out) in enumerate(((sk, dk), (sv, dv_out))):
        copy = pltpu.make_async_copy(src.at[last], cols(out, chip), loc.at[2 + j])
        copy.start()
        own.append(copy)
    for copy in own:
        copy.wait()
    inv_cols = inv[...].T
    n_chunk = inv.shape[0] // 2
    dots = []

    def first_pass(i, grad, lin, gain):
        gains = [jnp.zeros((1, LANES), f32)] * heads
        for r in range(n_chunk):
            part_rows = slice(r * LANES, (r + 1) * LANES)
            c = i * n_chunk + r
            norm = inv_cols[:, c : c + 1]
            total = jnp.zeros((LANES, LANES), f32)
            for h in range(heads):
                lanes = slice(h * LANES, (h + 1) * LANES)
                hat = lin[part_rows, lanes] * norm
                back = rolled(grad[part_rows, lanes], cos_t[part_rows, :], -sin_t[part_rows, :])
                both = back * hat
                gains[h] = gains[h] + jnp.sum(both, axis=0, keepdims=True)
                total = total + both * gain[:, lanes]
                grad[part_rows, lanes] = back * gain[:, lanes]
            dots.append(jnp.sum(total, axis=1, keepdims=True))
        for h in range(heads):
            gain_out[i * heads + h : i * heads + h + 1, :] = gains[h]

    for s in range(last):
        place = cols(dk, lax.rem(chip - 1 - s + heads, heads))
        remote(place, place, ks.at[s], kr.at[s], partner).wait_recv()
    first_pass(1, dk, k_lin, k_gain)
    for r in range(1, cp_size):
        src = lax.rem(me - r + cp_size, cp_size)
        for s in BOTH:
            place = cols(dq, src // 2, sub_rows(lax.rem(src, 2), s, sub))
            remote(place, place, qs.at[r, s], qr.at[r, s], partner).wait_recv()
    first_pass(0, dq, q_lin, q_gain)
    part[...] = jnp.concatenate(dots[n_chunk:] + dots[:n_chunk], axis=1).T
    dot_cols = (share_over_tp(tp_size, me_tp, part, got, ts, tr)() / width).T
    for i, (grad, lin, out) in enumerate(((dq, q_lin, dq_out), (dk, k_lin, dk_out))):
        for r in range(n_chunk):
            part_rows = slice(r * LANES, (r + 1) * LANES)
            c = i * n_chunk + r
            norm = inv_cols[:, c : c + 1]
            out[part_rows, :] = (norm * (grad[part_rows, :] - lin[part_rows, :] * norm * dot_cols[:, c : c + 1])).astype(out.dtype)
    for s in range(last):
        sends.extend(home_copies(s))
        place = cols(dv_out, lax.rem(chip - 1 - s + heads, heads))
        remote(place, place, vs.at[s], vr.at[s], partner).wait_recv()
    for r in range(1, tp_size):
        place = block_of(oo_out, lax.rem(me_tp - r + tp_size, tp_size), sub)
        remote(place, place, os.at[r], orr.at[r], partner).wait_recv()
    for k, (src, dst) in ways:
        sends.append(relay(k, src, dst))
        half = block_of(gp_out, t_far * 2 + k, sub // 2)
        remote(half, half, gs.at[2 + k], gr.at[2 + k], partner).wait_recv()
    for copy in sends:
        copy.wait_send()


def reduce_tail(tp_size, cp_size, *refs):
    n_w = 4
    (w_o_in, w_v_in), (dx_in, dy_in, small, y_in, x_in, dq_in, dk_in) = refs[:2], refs[2:9]
    refs = refs[9:]
    w_out, (dx_out, y_out, small_out) = refs[:n_w], refs[n_w : n_w + 3]
    refs = refs[n_w + 3 :]
    acc, pair, far_a, far_b, fin_l, fin_r = (refs[i * n_w : (i + 1) * n_w] for i in range(6))
    refs = refs[6 * n_w :]
    w_q_in, w_k_in, dxa, dxb, dx_own, dx_fa, dx_fb, dx_fl, dx_fr, dx16, got_small, got_post, ss, rs, ps, pr, fs, fr, loc, sms, smr, gps, gpr = refs
    w_in = (w_o_in, w_v_in, w_q_in, w_k_in)
    me_tp = lax.axis_index("tp")
    me_cp = lax.axis_index("cp")
    core = lax.rem(me_cp, 2)
    chip = me_cp // 2
    ring = cp_size // 2
    left, right, far = (lax.rem(chip + d, ring) for d in (ring - 1, 1, 2))
    t_left, t_right, t_far = (lax.rem(me_tp + d, tp_size) for d in (tp_size - 1, 1, 2))
    partner = {"cp": me_cp + 1 - 2 * core}
    to_l, to_r = {"cp": left * 2 + core}, {"cp": right * 2 + core}
    tp_l, tp_r = {"tp": t_left}, {"tp": t_right}
    dx_i, y_i = n_w, n_w + 1
    outs = []

    def ring_sems(t, kind):
        return ss.at[t, kind], rs.at[t, kind]

    def pair_sems(t, kind):
        return fs.at[t, kind], fr.at[t, kind]

    cross_barrier(me_tp, me_cp, tp_size, cp_size)
    sent = []

    def go(src, dst, s_sem, r_sem, device):
        copy = remote(src, dst, s_sem, r_sem, device)
        copy.start()
        sent.append(copy)

    def landed(dst, s_sem, r_sem):
        remote(dst, dst, s_sem, r_sem, partner).wait_recv()

    def piece(ref, t, x, c, part=None):
        size = w_in[t].shape[0] // cp_size
        first = (2 * x + c) * size
        if part is None:
            return ref.at[pl.ds(pl.multiple_of(first, size), size), :]
        return ref.at[pl.ds(pl.multiple_of(first + part * (size // 2), size // 2), size // 2), :]

    def rows_of(ref, y, part=None):
        size = dx_in.shape[0] // tp_size
        if part is None:
            return ref.at[pl.ds(pl.multiple_of(y * size, size), size), :]
        return ref.at[pl.ds(pl.multiple_of(y * size + part * (size // 2), size // 2), size // 2), :]

    def half_of(ref, part):
        size = ref.shape[0] // 2
        return ref.at[pl.ds(part * size, size), :]

    for r in range(1, cp_size):
        go(small, got_small.at[me_cp], sms.at[r], smr.at[r], {"cp": lax.rem(me_cp + r, cp_size)})
    go(rows_of(dx_in, t_far, 0), dx_fa, *ring_sems(dx_i, FAR_A), tp_l)
    go(rows_of(dx_in, t_far, 1), dx_fb, *ring_sems(dx_i, FAR_B), tp_r)
    go(rows_of(dx_in, t_left, 1), half_of(dx_fr, 1), *ring_sems(dx_i, NEAR_L), tp_l)
    go(rows_of(dx_in, t_right, 0), half_of(dx_fl, 0), *ring_sems(dx_i, NEAR_R), tp_r)
    def give(src, stream, out, dev_l, dev_r):
        copy = pltpu.make_async_copy(src, out, loc.at[stream, n_w])
        copy.start()
        outs.append(copy)
        go(src, out, *ring_sems(stream, OUT_L), dev_l)
        go(src, out, *ring_sems(stream, OUT_R), dev_r)

    give(y_in, y_i, rows_of(y_out, me_tp), tp_l, tp_r)
    order = (far, left, right, chip)
    loads = {}

    def start_pair(t):
        for i, x in enumerate(order):
            go(piece(w_in[t], t, x, 1 - core), pair[t].at[x], ps.at[t, i], pr.at[t, i], partner)
            copy = pltpu.make_async_copy(piece(w_in[t], t, x, core), acc[t].at[x], loc.at[t, i])
            copy.start()
            loads[t, i] = copy

    start_pair(0)
    start_pair(1)
    dx_loads = [
        pltpu.make_async_copy(rows_of(dx_in, t_left, 0), dxa, loc.at[n_w, 0]),
        pltpu.make_async_copy(rows_of(dx_in, t_right, 1), dxb, loc.at[n_w, 1]),
        pltpu.make_async_copy(rows_of(dx_in, me_tp), dx_own, loc.at[n_w, 2]),
    ]
    for copy in dx_loads:
        copy.start()

    for t in range(n_w):
        for i, x in enumerate(order):
            loads[t, i].wait()
            landed(pair[t].at[x], ps.at[t, i], pr.at[t, i])
            acc[t][x] += pair[t][x]
        go(half_of(acc[t].at[far], 0), far_a[t], *ring_sems(t, FAR_A), to_l)
        go(half_of(acc[t].at[far], 1), far_b[t], *ring_sems(t, FAR_B), to_r)
        go(half_of(acc[t].at[left], 1), half_of(fin_r[t], 1), *ring_sems(t, NEAR_L), to_l)
        go(half_of(acc[t].at[right], 0), half_of(fin_l[t], 0), *ring_sems(t, NEAR_R), to_r)
        if t < 2:
            out, grad = ((w_q_in, dq_in), (w_k_in, dk_in))[t]
            size = out.shape[0] // cp_size
            for p in range(cp_size):
                rows = slice(p * size, (p + 1) * size)
                out[rows, :] = jnp.dot(x_in[:, rows].T, grad[...], preferred_element_type=jnp.float32)
            start_pair(2 + t)

    got_small[me_cp] = small[...]
    for r in range(1, cp_size):
        landed(got_small.at[lax.rem(me_cp - r + cp_size, cp_size)], sms.at[r], smr.at[r])
    total = got_small[0]
    for i in range(1, cp_size):
        total = total + got_small[i]
    small_out[...] = total
    n_gain = small.shape[0] - got_post.shape[1]

    def second_half(t, acc_l, acc_r, fa, fb, fl, fr, dev_l, dev_r):
        half = fa.shape[0]
        landed(fa, *ring_sems(t, FAR_A))
        acc_l[...] += fa[...]
        landed(fb, *ring_sems(t, FAR_B))
        acc_r[...] += fb[...]
        go(acc_l, half_of(fr, 0), *ring_sems(t, SUM_L), dev_l)
        go(acc_r, half_of(fl, 1), *ring_sems(t, SUM_R), dev_r)

    def all_landed(t, fl, fr):
        landed(half_of(fr, 1), *ring_sems(t, NEAR_L))
        landed(half_of(fl, 0), *ring_sems(t, NEAR_R))
        landed(half_of(fr, 0), *ring_sems(t, SUM_L))
        landed(half_of(fl, 1), *ring_sems(t, SUM_R))

    for t in range(n_w):
        second_half(t, half_of(acc[t].at[left], 0), half_of(acc[t].at[right], 1), far_a[t], far_b[t], fin_l[t], fin_r[t], to_l, to_r)
    for copy in dx_loads:
        copy.wait()
    second_half(dx_i, dxa, dxb, dx_fa, dx_fb, dx_fl, dx_fr, tp_l, tp_r)
    post = small_out.at[pl.ds(n_gain, got_post.shape[1]), :]
    for r in range(1, tp_size):
        go(post, got_post.at[r], gps.at[r], gpr.at[r], {"tp": lax.rem(me_tp + r, tp_size)})

    for t in range(n_w):
        all_landed(t, fin_l[t], fin_r[t])
        acc[t][chip] = acc[t][chip] + (fin_l[t][...] + fin_r[t][...])
        src = acc[t].at[chip]
        dst = piece(w_out[t], t, chip, core)
        give(src, t, dst, to_l, to_r)
        go(src, dst, *pair_sems(t, 0), partner)
    all_landed(dx_i, dx_fl, dx_fr)
    dx16[...] = (dx_own[...] + (dx_fl[...] + dx_fr[...]) + dy_in[...].astype(jnp.float32)).astype(dx16.dtype)
    give(dx16, dx_i, rows_of(dx_out, me_tp), tp_l, tp_r)

    def relay(stream, part_of, x_l, x_r, dev_l, dev_r, pass_on):
        for arrived, x, kind, part, dev in ((OUT_L, x_r, RELAY_L, 0, dev_l), (OUT_R, x_l, RELAY_R, 1, dev_r)):
            whole = part_of(x)
            landed(whole, *ring_sems(stream, arrived))
            half = part_of(x, part)
            go(half, half, *ring_sems(stream, kind), dev)
            if pass_on:
                go(whole, whole, *pair_sems(stream, 1 + part), partner)

    for t in range(n_w):
        relay(t, functools.partial(lambda ref, t, x, part=None: piece(ref, t, x, core, part), w_out[t], t), left, right, to_l, to_r, True)
    for stream, out in ((y_i, y_out), (dx_i, dx_out)):
        relay(stream, functools.partial(rows_of, out), t_left, t_right, tp_l, tp_r, False)

    sums = small_out[n_gain:, :]
    for r in range(1, tp_size):
        landed(got_post.at[r], gps.at[r], gpr.at[r])
    sums = (sums + got_post[2]) + (got_post[1] + got_post[3])

    for t in range(n_w):
        for kind, part in PARTS:
            half = piece(w_out[t], t, far, core, part)
            landed(half, *ring_sems(t, kind))
            go(half, half, *pair_sems(t, 3 + part), partner)
    for stream, out in ((y_i, y_out), (dx_i, dx_out)):
        for kind, part in PARTS:
            landed(rows_of(out, t_far, part), *ring_sems(stream, kind))
    for t in range(n_w):
        for i, x in enumerate((chip, right, left)):
            landed(piece(w_out[t], t, x, 1 - core), *pair_sems(t, i))
        for part in BOTH:
            landed(piece(w_out[t], t, far, 1 - core, part), *pair_sems(t, 3 + part))
    for copy in outs:
        copy.wait()
    for copy in sent:
        copy.wait_send()
    small_out[n_gain:, :] = sums


def solution(mesh):
    tp_size = mesh.shape["tp"]
    cp_size = mesh.shape["cp"]
    act_spec = P("dp", "cp", None)
    col_spec = P(None, "tp", None)
    part_col = P("dp", "tp", None)
    in_specs = (act_spec, col_spec, col_spec, col_spec, P("tp", None, None), P("tp", None), P("tp", None), P(None), act_spec)
    out_specs = (act_spec, act_spec, part_col, part_col, part_col, P(("dp", "tp"), None, None), P(("dp", "tp"), None), P(("dp", "tp"), None), P("dp"))
    dma = pltpu.SemaphoreType.DMA

    def local_run(x_in, w_q, w_k, w_v, w_o, q_norm_w, k_norm_w, post_norm_w, grad_y):
        n_batch, block_len, d_model = x_in.shape
        heads, head_dim = w_q.shape[1:]
        assert n_batch == 1 and w_k.shape[1] == heads and cp_size == 2 * heads and tp_size == 4
        sub = block_len // tp_size
        rows = 2 * sub
        width = heads * head_dim * tp_size
        scale = head_dim ** -0.5
        f32 = jnp.float32
        b16 = jnp.bfloat16
        tp_index = lax.axis_index("tp")
        cp_index = lax.axis_index("cp")
        cos_tab, sin_tab = rope_tables(cp_index * block_len, block_len, head_dim)
        x_loc = x_in[0]
        dy_loc = grad_y[0]
        w_q2, w_k2, w_v2 = (w.reshape(d_model, -1) for w in (w_q, w_k, w_v))
        gains = [g.reshape(1, -1) for g in (q_norm_w, k_norm_w)]
        loc_width = heads * head_dim

        q_lin = jnp.dot(x_loc, w_q2, preferred_element_type=f32)
        k_lin = jnp.dot(x_loc, w_k2, preferred_element_type=f32)
        v_val = jnp.dot(x_loc, w_v2, preferred_element_type=f32).astype(b16)
        vec = jnp.stack([jnp.sum(t * t, axis=1) for t in (q_lin, k_lin)]).reshape(-1, LANES)
        vec_shape = jax.ShapeDtypeStruct(vec.shape, f32)
        kv_shape = jax.ShapeDtypeStruct((cp_size, block_len, head_dim), b16)
        lin16 = VMEM((block_len, loc_width), b16)
        tp_scratch = VMEM((tp_size,) + vec.shape, f32)
        q_all, k_all, v_all, inv, w_o_full = vmem_call(
            functools.partial(scatter_qkv, heads, tp_size, cp_size, width),
            [jax.ShapeDtypeStruct((cp_size, rows, head_dim), b16), kv_shape, kv_shape, vec_shape, jax.ShapeDtypeStruct((width, d_model), b16)],
            9,
            [lin16, lin16, tp_scratch, dma((5,))] + [dma((cp_size, 2))] * 2 + [dma((heads,))] * 8 + [dma((tp_size,))] * 6,
            0,
            1,
            1,
        )(q_lin, k_lin, vec, *gains, cos_tab, sin_tab, w_o.reshape(-1, d_model), v_val)

        qspec = pl.BlockSpec((1, rows, head_dim), lambda i: (i, 0, 0))
        lspec = pl.BlockSpec((1, 1, rows), lambda i: (i, 0, 0))
        kvspec = pl.BlockSpec((1, block_len, head_dim), lambda i: (i, 0, 0))
        pair_flops = cp_size * (cp_size + 1) // 2 * rows * block_len * head_dim * 2
        o_all, lse = pl.pallas_call(
            functools.partial(attend, sub, scale),
            grid=(cp_size,),
            in_specs=[qspec, kvspec, kvspec],
            out_specs=[qspec, lspec],
            out_shape=[jax.ShapeDtypeStruct((cp_size, rows, head_dim), b16), jax.ShapeDtypeStruct((cp_size, 1, rows), f32)],
            scratch_shapes=[VMEM((cp_size, block_len, head_dim), b16), VMEM((cp_size, head_dim, block_len), b16), VMEM((1, rows), f32), VMEM((1, rows), f32), VMEM((head_dim, rows), f32)]
            + [VMEM((block_len // 2, rows), f32)] * 2 + [VMEM((1, rows), f32)],
            compiler_params=pltpu.CompilerParams(vmem_limit_bytes=LIMIT),
            cost_estimate=pl.CostEstimate(flops=2 * pair_flops, bytes_accessed=6 << 20, transcendentals=0),
        )(q_all, k_all, v_all)

        n_heads = heads * tp_size
        o_rows = vmem_call(
            functools.partial(heads_to_rows, heads, tp_size, cp_size),
            [jax.ShapeDtypeStruct((sub, width), b16)],
            1,
            [dma((2, cp_size)), dma((n_heads,))],
            1,
        )(o_all)[0]

        x_rows = lax.dynamic_slice_in_dim(x_loc, tp_index * sub, sub, 0)
        dy_rows = lax.dynamic_slice_in_dim(dy_loc, tp_index * sub, sub, 0)
        dy_f = dy_rows.astype(f32)
        proj = jnp.dot(o_rows, w_o_full, preferred_element_type=f32)
        post_inv = lax.rsqrt(jnp.mean(proj * proj, axis=-1, keepdims=True) + NORM_EPS)
        post_hat = proj * post_inv
        y_rows = (x_rows + post_hat * post_norm_w).astype(b16)
        grad_post = jnp.sum(dy_f * post_hat, axis=0)
        grad_hat = dy_f * post_norm_w
        gp_rows = (post_inv * (grad_hat - post_hat * jnp.mean(grad_hat * post_hat, axis=-1, keepdims=True))).astype(b16)
        do_rows = lax.dot_general(gp_rows, w_o_full, NT, preferred_element_type=f32).astype(b16)

        do_all = vmem_call(
            functools.partial(rows_to_heads, heads, tp_size, cp_size),
            [jax.ShapeDtypeStruct((cp_size, rows, head_dim), b16)],
            1,
            [dma((tp_size, heads)), dma((cp_size, 2))],
            2,
        )(do_rows)[0]

        lin_h, f_lin = jax.ShapeDtypeStruct((block_len, loc_width), b16), VMEM((block_len, loc_width), f32)
        head_f = VMEM((heads, block_len, head_dim), f32)
        pair_f = VMEM((heads, 2, block_len, head_dim), f32)
        dq16, dk16, dv16, gain_grads, grad_proj, o_own = vmem_call(
            functools.partial(attend_back, heads, tp_size, cp_size, width, scale),
            [lin_h, lin_h, lin_h, jax.ShapeDtypeStruct((2 * heads, head_dim), f32), jax.ShapeDtypeStruct((block_len, d_model), b16), lin_h],
            15,
            [f_lin, f_lin, VMEM((cp_size, head_dim, block_len), b16), VMEM((cp_size, head_dim, rows), f32), VMEM((cp_size, 1, rows), f32), VMEM((cp_size, rows, head_dim), f32)]
            + [pair_f, pair_f, f_lin, f_lin, head_f, head_f, head_f, VMEM((heads, block_len, head_dim), b16), VMEM(vec.shape, f32), tp_scratch, dma((8,))]
            + [dma((cp_size, 2))] * 2 + [dma((heads,))] * 8 + [dma((tp_size,))] * 6,
            3,
            2,
            2,
        )(q_all, k_all, v_all, o_all, do_all, lse, inv, *gains, cos_tab, sin_tab, gp_rows, o_rows, q_lin, k_lin)

        def wgrad(left, right):
            return lax.dot_general(left, right, (((0,), (0,)), ((), ())), preferred_element_type=f32)

        grad_w_o, grad_w_v = wgrad(o_own, grad_proj), wgrad(x_loc, dv16)
        dx_part = sum(lax.dot_general(g, w, NT, preferred_element_type=f32) for g, w in ((dq16, w_q2), (dk16, w_k2), (dv16, w_v2)))
        w_parts = [grad_w_o, grad_w_v, grad_w_v, grad_w_v]
        small = jnp.concatenate([gain_grads, grad_post.reshape(-1, head_dim)], axis=0)
        any_spec = pl.BlockSpec(memory_space=pl.ANY)
        vmem_spec = pl.BlockSpec(memory_space=VMEM)

        def bufs(lead, div):
            return [VMEM(lead + (w.shape[0] // div, w.shape[1]), f32) for w in w_parts]

        ring = cp_size // 2
        rows_dx, half_dx = VMEM((sub, d_model), f32), VMEM((sub // 2, d_model), f32)
        res = pl.pallas_call(
            functools.partial(reduce_tail, tp_size, cp_size),
            out_shape=[jax.ShapeDtypeStruct(w.shape, f32) for w in w_parts] + [jax.ShapeDtypeStruct((block_len, d_model), b16)] * 2 + [jax.ShapeDtypeStruct(small.shape, f32)],
            in_specs=[any_spec] * 3 + [vmem_spec] * 6,
            out_specs=[any_spec] * 6 + [vmem_spec],
            scratch_shapes=bufs((ring,), cp_size) * 2 + bufs((), 2 * cp_size) * 2 + bufs((), cp_size) * 2
            + [VMEM(grad_w_v.shape, f32)] * 2 + [half_dx, half_dx, rows_dx, half_dx, half_dx, rows_dx, rows_dx, VMEM((sub, d_model), b16)]
            + [VMEM((cp_size,) + small.shape, f32), VMEM((tp_size, d_model // head_dim, head_dim), f32)]
            + [dma((6, 10))] * 2 + [dma((4, 4))] * 2 + [dma((4, 5))] * 2 + [dma((6, 5))] + [dma((cp_size,))] * 2 + [dma((tp_size,))] * 2,
            compiler_params=pltpu.CompilerParams(vmem_limit_bytes=LIMIT, collective_id=6, has_side_effects=True),
        )(grad_w_o, grad_w_v, dx_part, dy_rows, small, y_rows, x_loc, dq16, dk16)
        grad_w_v, grad_w_q, grad_w_k = (g.reshape(w_q.shape) for g in res[1:4])
        grad_x, y_out, small_sum = res[4:]
        return (y_out[None], grad_x[None], grad_w_q, grad_w_k, grad_w_v, res[0].reshape(w_o.shape), small_sum[:heads], small_sum[heads : 2 * heads], small_sum[2 * heads :].reshape(-1))

    return jax.shard_map(local_run, mesh=mesh, in_specs=in_specs, out_specs=out_specs, check_vma=False)
```

```python
import functools
import math

import jax
import jax.numpy as jnp
from jax import lax
from jax.experimental import pallas as pl
from jax.experimental.pallas import tpu as pltpu
from jax.sharding import PartitionSpec as P

ROPE_THETA = 500000.0
NORM_EPS = 1e-6
LOG2E = 1.4426950408889634
LIMIT = 61 << 20
SMALL = 28 << 20
LANES = 128
FAR_A, FAR_B, NEAR_L, NEAR_R, SUM_L, SUM_R, OUT_L, OUT_R, RELAY_L, RELAY_R = range(10)
BOTH = range(2)
PARTS = tuple(zip((RELAY_L, RELAY_R), BOTH))
VMEM = pltpu.VMEM
MESH = pl.DeviceIdType.MESH
NT = (((1,), (1,)), ((), ()))


def rope_tables(start_pos, seq_rows, head_dim):
    half_dim = head_dim // 2
    lane = jnp.arange(head_dim)
    inv_freq = ROPE_THETA ** (-2.0 * (lane % half_dim).astype(jnp.float32) / head_dim)
    positions = (start_pos + jnp.arange(seq_rows)).astype(jnp.float32)
    angles = positions[:, None] * inv_freq[None, :]
    return jnp.cos(angles), jnp.where(lane < half_dim, -1.0, 1.0) * jnp.sin(angles)


def vmem_call(kernel, out_shape, n_in, scratch, collective_id, n_any=0, n_any_in=0):
    n_out = len(out_shape) - n_any
    return pl.pallas_call(
        kernel,
        out_shape=out_shape,
        in_specs=[pl.BlockSpec(memory_space=VMEM)] * (n_in - n_any_in) + [pl.BlockSpec(memory_space=pl.ANY)] * n_any_in,
        out_specs=[pl.BlockSpec(memory_space=VMEM)] * n_out + [pl.BlockSpec(memory_space=pl.ANY)] * n_any,
        scratch_shapes=scratch,
        compiler_params=pltpu.CompilerParams(vmem_limit_bytes=LIMIT if collective_id == 3 else SMALL, collective_id=collective_id, has_side_effects=True),
    )


def block_of(ref, index, size):
    return ref.at[pl.ds(pl.multiple_of(index * size, size), size), :]


def remote(src, dst, send_sem, recv_sem, device_id):
    return pltpu.make_async_remote_copy(src_ref=src, dst_ref=dst, send_sem=send_sem, recv_sem=recv_sem, device_id=device_id, device_id_type=MESH)


def cross_barrier(me_tp, me_cp, tp_size, cp_size):
    barrier = pltpu.get_barrier_semaphore()
    for axis, me, size in (("cp", me_cp, cp_size), ("tp", me_tp, tp_size)):
        for step in range(1, size):
            pl.semaphore_signal(barrier, inc=1, device_id={axis: lax.rem(me + step, size)}, device_id_type=MESH)
    pl.semaphore_wait(barrier, cp_size + tp_size - 2)


def cols(ref, head, rows=None):
    lanes = pl.ds(pl.multiple_of(head * LANES, LANES), LANES)
    return ref.at[:, lanes] if rows is None else ref.at[rows, lanes]


def sub_rows(core, slot, sub):
    first = core if slot == 0 else 3 - core
    return pl.ds(pl.multiple_of(first * sub, sub), sub)


def share_over_tp(tp_size, me, vec, got, ss, rs):
    copies = []
    for r in range(1, tp_size):
        copy = remote(vec, got.at[r], ss.at[r], rs.at[r], {"tp": lax.rem(me + r, tp_size)})
        copy.start()
        copies.append(copy)

    def finish():
        for copy in copies:
            copy.wait()
        return (vec[...] + got[2]) + (got[1] + got[3])

    return finish


def rolled(t, c, s):
    return t * c + pltpu.roll(t, LANES // 2, 1) * s


def group_barrier(me_tp, me_cp, tp_size, cp_size):
    barrier = pltpu.get_barrier_semaphore()
    for st in range(tp_size):
        for sc in range(cp_size):
            if st or sc:
                pl.semaphore_signal(barrier, inc=1, device_id={"tp": lax.rem(me_tp + st, tp_size), "cp": lax.rem(me_cp + sc, cp_size)}, device_id_type=MESH)
    pl.semaphore_wait(barrier, tp_size * cp_size - 1)


def scatter_qkv(heads, tp_size, cp_size, width, q_lin, k_lin, vec, q_gain, k_gain, cos_t, sin_t, wo_in, v_in, q_out, k_out, v_out, inv_out, wo_out, q16, k16, got, loc, qs, qr, ks, kr, vs, vr, fks, fkr, fvs, fvr, ts, tr, ws, wr, wfs, wfr):
    me_tp = lax.axis_index("tp")
    me = lax.axis_index("cp")
    core = lax.rem(me, 2)
    chip = me // 2
    sub = q_out.shape[1] // 2
    cross_barrier(me_tp, me, tp_size, cp_size)
    finish = share_over_tp(tp_size, me_tp, vec, got, ts, tr)
    far_chips = (1, heads - 1, 2)
    sends = []

    def spread(src, out, ss, rs):
        for r in far_chips:
            dst = lax.rem(chip + r, heads)
            copy = remote(cols(src, dst), out.at[me], ss.at[r], rs.at[r], {"cp": dst * 2 + core})
            copy.start()
            sends.append(copy)

    spread(v_in, v_out, vs, vr)
    shard = wo_in.shape[0]
    keep = pltpu.make_async_copy(wo_in, block_of(wo_out, me_tp, shard), loc.at[4])
    keep.start()
    t_left, t_right, t_far = (lax.rem(me_tp + d, tp_size) for d in (tp_size - 1, 1, 2))
    ways = tuple(enumerate(((t_right, t_left), (t_left, t_right))))
    for k, (_, dst) in ways:
        copy = remote(block_of(wo_in, core, shard // 2), block_of(wo_out, me_tp * 2 + core, shard // 2), ws.at[k], wr.at[k], {"tp": dst})
        copy.start()
        sends.append(copy)
    inv_out[...] = lax.rsqrt(finish() / width + NORM_EPS)
    n_chunk = inv_out.shape[0] // 2
    inv_cols = inv_out[...].T

    def rotate(lin, gain, out16, first):
        for r in range(n_chunk):
            rows = slice(r * LANES, (r + 1) * LANES)
            scale = inv_cols[:, first + r : first + r + 1]
            for h in range(heads):
                lanes = slice(h * LANES, (h + 1) * LANES)
                out16[rows, lanes] = rolled(lin[rows, lanes] * scale * gain[:, lanes], cos_t[rows, :], sin_t[rows, :]).astype(out16.dtype)

    rotate(k_lin, k_gain, k16, n_chunk)
    spread(k16, k_out, ks, kr)
    rotate(q_lin, q_gain, q16, 0)
    own = [pltpu.make_async_copy(cols(k16, chip), k_out.at[me], loc.at[0]), pltpu.make_async_copy(cols(v_in, chip), v_out.at[me], loc.at[1])]
    for r in range(cp_size):
        dst = lax.rem(me + r, cp_size)
        for s in BOTH:
            src = cols(q16, dst // 2, sub_rows(lax.rem(dst, 2), s, sub))
            place = q_out.at[me, s * sub : (s + 1) * sub, :]
            if r == 0:
                own.append(pltpu.make_async_copy(src, place, loc.at[2 + s]))
            else:
                copy = remote(src, place, qs.at[r, s], qr.at[r, s], {"cp": dst})
                copy.start()
                sends.append(copy)
    for copy in own:
        copy.start()
    partner = {"cp": me + 1 - 2 * core}
    forwards = []

    def pass_on(part, ss, rs):
        copy = remote(part, part, ss, rs, partner)
        copy.start()
        forwards.append(copy)

    def forward(local, buf, ss, rs, fs, fr):
        for r in (0,) + far_chips:
            src = lax.rem(chip - r + heads, heads) * 2 + core
            if r == 0:
                local.wait()
            else:
                remote(buf.at[src], buf.at[src], ss.at[r], rs.at[r], partner).wait_recv()
            pass_on(buf.at[src], fs.at[r], fr.at[r])

    forward(own[1], v_out, vs, vr, fvs, fvr)
    for k, (src, dst) in ways:
        whole = block_of(wo_out, src * 2 + core, shard // 2)
        remote(whole, whole, ws.at[k], wr.at[k], partner).wait_recv()
        half = block_of(wo_out, (src * 2 + core) * 2 + k, shard // 4)
        copy = remote(half, half, ws.at[2 + k], wr.at[2 + k], {"tp": dst})
        copy.start()
        sends.append(copy)
        pass_on(whole, wfs.at[k], wfr.at[k])
    forward(own[0], k_out, ks, kr, fks, fkr)
    for copy in own[2:] + [keep]:
        copy.wait()
    for k, _ in ways:
        half = block_of(wo_out, (t_far * 2 + core) * 2 + k, shard // 4)
        remote(half, half, ws.at[2 + k], wr.at[2 + k], partner).wait_recv()
        pass_on(half, wfs.at[2 + k], wfr.at[2 + k])
    for copy in sends:
        copy.wait_send()
    for r in range(1, cp_size):
        for s in BOTH:
            place = q_out.at[lax.rem(me - r + cp_size, cp_size), s * sub : (s + 1) * sub, :]
            remote(place, place, qs.at[r, s], qr.at[r, s], partner).wait_recv()
    for copy in forwards:
        copy.wait()


def attend(sub, scale, q_ref, k_ref, v_ref, o_ref, lse_ref, k_scr, vt_scr, m_scr, l_scr, acc_scr, s_a, s_b, mx_a):
    blk = pl.program_id(0)
    core = lax.rem(lax.axis_index("cp"), 2)
    coef = scale * LOG2E
    half = k_ref.shape[1] // 2
    cols = q_ref.shape[1]
    chunk = half // 2
    k_scr[blk] = k_ref[0]
    vt_scr[blk] = v_ref[0].T
    m_scr[...] = jnp.full_like(m_scr, -jnp.inf)
    l_scr[...] = jnp.zeros_like(l_scr)
    acc_scr[...] = jnp.zeros_like(acc_scr)

    def fold(op, values):
        return op(values.reshape(values.shape[0] // 8, 8, cols), axis=0)

    def scores(b, h, c):
        kv = slice(h * half + c * chunk, h * half + (c + 1) * chunk)
        return lax.dot_general(k_scr[b, kv, :], q_ref[0], NT, preferred_element_type=jnp.float32)

    def mask(s, h, c):
        kv_pos = h * half + c * chunk + lax.broadcasted_iota(jnp.int32, s.shape, 0)
        col = lax.broadcasted_iota(jnp.int32, s.shape, 1)
        q_pos = jnp.where(col < sub, core * sub + col, (2 - core) * sub + col)
        return jnp.where(kv_pos <= q_pos, s, -jnp.inf)

    def step(buf, mx, b, h, nxt):
        m_old = m_scr[...]
        m_new = jnp.maximum(m_old, mx)
        mc = m_new * coef
        alpha = jnp.exp2((m_old - m_new) * coef)
        lsum = jnp.zeros((8, cols), jnp.float32)
        new_mx = None
        for c in BOTH:
            rows = slice(c * chunk, (c + 1) * chunk)
            if nxt is not None:
                nbuf, nb, nh, masked = nxt
                s = scores(nb, nh, c)
                if masked:
                    s = mask(s, nh, c)
                nbuf[rows, :] = s
                part = fold(jnp.max, s)
                new_mx = part if new_mx is None else jnp.maximum(new_mx, part)
            p = jnp.exp2(buf[rows, :] * coef - mc)
            lsum = lsum + fold(jnp.sum, p)
            pv = jnp.dot(vt_scr[b, :, h * half + c * chunk : h * half + (c + 1) * chunk], p.astype(jnp.bfloat16), preferred_element_type=jnp.float32)
            acc_scr[...] = acc_scr[...] * alpha + pv if c == 0 else acc_scr[...] + pv
        l_scr[...] = l_scr[...] * alpha + jnp.sum(lsum, axis=0, keepdims=True)
        m_scr[...] = m_new
        return None if nxt is None else jnp.max(new_mx, axis=0, keepdims=True)

    for c in BOTH:
        s_a[c * chunk : (c + 1) * chunk, :] = scores(0, 0, c)
    mx_a[...] = jnp.max(s_a[...], axis=0, keepdims=True)

    def body(b, carry):
        mx_b = step(s_a, mx_a[...], b, 0, (s_b, b, 1, False))
        mx_a[...] = step(s_b, mx_b, b, 1, (s_a, b + 1, 0, False))
        return carry

    lax.fori_loop(0, blk, body, 0)
    for c in BOTH:
        rows = slice(c * chunk, (c + 1) * chunk)
        s_a[rows, :] = mask(s_a[rows, :], 0, c)
    mx_b = step(s_a, jnp.max(s_a[...], axis=0, keepdims=True), blk, 0, (s_b, blk, 1, True))
    step(s_b, mx_b, blk, 1, None)
    o_ref[0] = (acc_scr[...] / l_scr[...]).T.astype(o_ref.dtype)
    lse_ref[0] = m_scr[...] * coef + jnp.log2(l_scr[...])


def heads_to_rows(heads, tp_size, cp_size, o_in, o_out, ss, rs):
    me_tp = lax.axis_index("tp")
    me_cp = lax.axis_index("cp")
    core = lax.rem(me_cp, 2)
    head = me_tp * heads + me_cp // 2
    sub = o_out.shape[0]
    place = cols(o_out, head)
    group_barrier(me_tp, me_cp, tp_size, cp_size)
    for finish in BOTH:
        if finish:
            for h in range(heads * tp_size):
                part = o_out.at[:, h * LANES : (h + 1) * LANES]
                pltpu.make_async_copy(part, part, rs.at[h]).wait()
        for s in BOTH:
            dst_tp = core if s == 0 else 3 - core
            for r in range(cp_size):
                dst_cp = lax.rem(me_cp + r, cp_size)
                src = o_in.at[dst_cp, s * sub : (s + 1) * sub, :]
                copy = remote(src, place, ss.at[s, r], rs.at[head], {"tp": dst_tp, "cp": dst_cp})
                act = copy.wait_send if finish else copy.start
                if r:
                    act()
                    continue
                pl.when(dst_tp != me_tp)(act)
                if not finish:
                    pl.when(dst_tp == me_tp)(pltpu.make_async_copy(src, place, rs.at[head]).start)


def rows_to_heads(heads, tp_size, cp_size, g_in, g_out, ss, rs):
    me_tp = lax.axis_index("tp")
    me_cp = lax.axis_index("cp")
    core = lax.rem(me_cp, 2)
    sub = g_in.shape[0]
    row_core = jnp.where(me_tp < 2, me_tp, 3 - me_tp)
    slot = me_tp // 2
    place = g_out.at[me_cp, pl.ds(pl.multiple_of(slot * sub, sub), sub), :]
    group_barrier(me_tp, me_cp, tp_size, cp_size)
    for finish in BOTH:
        if finish:
            for i in range(cp_size):
                for s in BOTH:
                    part = g_out.at[i, s * sub : (s + 1) * sub, :]
                    pltpu.make_async_copy(part, part, rs.at[i, s]).wait()
        for rt in range(tp_size):
            dst_tp = lax.rem(me_tp + rt, tp_size)
            for r in range(heads):
                chip = lax.rem(me_cp // 2 + r, heads)
                src = cols(g_in, dst_tp * heads + chip)
                copy = remote(src, place, ss.at[rt, r], rs.at[me_cp, slot], {"tp": dst_tp, "cp": chip * 2 + row_core})
                act = copy.wait_send if finish else copy.start
                if rt or r:
                    act()
                    continue
                pl.when(row_core != core)(act)
                if not finish:
                    pl.when(row_core == core)(pltpu.make_async_copy(src, place, rs.at[me_cp, slot]).start)


def attend_back(heads, tp_size, cp_size, width, scale, q_ref, k_ref, v_ref, o_ref, do_ref, lse_ref, inv, q_gain, k_gain, cos_t, sin_t, gp_in, or_in, q_hbm, k_hbm,
                dq_out, dk_out, dv_out, gain_out, gp_out, oo_out,
                q_lin, k_lin, kt_scr, dqt_scr, dl_scr, dqs, acc_k, acc_v, dq, dk, pk, pv, sk, sv, part, got, loc, qs, qr, pks, pkr, pvs, pvr, ks, kr, vs, vr, ts, tr, gs, gr, os, orr):
    me_tp = lax.axis_index("tp")
    me = lax.axis_index("cp")
    core = lax.rem(me, 2)
    chip = me // 2
    rows = q_ref.shape[1]
    sub = rows // 2
    block_len = k_ref.shape[1]
    coef = scale * LOG2E
    f32 = jnp.float32
    partner = {"cp": me + 1 - 2 * core}
    cross_barrier(me_tp, me, tp_size, cp_size)
    sends = []
    loc_width = heads * LANES
    own = [
        pltpu.make_async_copy(gp_in, block_of(gp_out, me_tp, sub), loc.at[4]),
        pltpu.make_async_copy(or_in.at[:, pl.ds(pl.multiple_of(me_tp * loc_width, loc_width), loc_width)], block_of(oo_out, me_tp, sub), loc.at[5]),
        pltpu.make_async_copy(q_hbm, q_lin, loc.at[6]),
        pltpu.make_async_copy(k_hbm, k_lin, loc.at[7]),
    ]
    for r in range(1, tp_size):
        dst = lax.rem(me_tp + r, tp_size)
        sends.append(remote(or_in.at[:, pl.ds(pl.multiple_of(dst * loc_width, loc_width), loc_width)], block_of(oo_out, me_tp, sub), os.at[r], orr.at[r], {"tp": dst}))
    t_left, t_right, t_far = (lax.rem(me_tp + d, tp_size) for d in (tp_size - 1, 1, 2))
    ways = tuple(enumerate(((t_right, t_left), (t_left, t_right))))
    for k, (_, dst) in ways:
        sends.append(remote(gp_in, block_of(gp_out, me_tp, sub), gs.at[k], gr.at[k], {"tp": dst}))
    for copy in own + sends:
        copy.start()

    def relay(k, src, dst):
        half = block_of(gp_out, src * 2 + k, sub // 2)
        return remote(half, half, gs.at[2 + k], gr.at[2 + k], {"tp": dst})

    def prepare(i, carry):
        kt_scr[i] = k_ref[i].T
        prod = o_ref[i].astype(f32) * do_ref[i].astype(f32)
        dl_scr[i] = jnp.sum(prod.T, axis=0, keepdims=True)
        dqt_scr[i] = jnp.zeros((LANES, rows), f32)
        return carry

    lax.fori_loop(0, cp_size, prepare, 0)

    def tile(i, b, s, e, masked):
        q = q_ref[i]
        do = do_ref[i]
        lse = lse_ref[i]
        delta = dl_scr[i]
        for j in range(block_len // sub):
            kv = slice(j * sub, (j + 1) * sub)
            scores = lax.dot_general(k_ref[b, kv, :], q, NT, preferred_element_type=f32)
            p = jnp.exp2(scores * coef - lse)
            if masked:
                kv_pos = j * sub + lax.broadcasted_iota(jnp.int32, (sub, rows), 0)
                col = lax.broadcasted_iota(jnp.int32, (sub, rows), 1)
                q_pos = jnp.where(col < sub, core * sub + col, (2 - core) * sub + col)
                p = jnp.where(kv_pos <= q_pos, p, 0.0)
            dp = lax.dot_general(v_ref[b, kv, :], do, NT, preferred_element_type=f32)
            ds = (p * (dp - delta)).astype(jnp.bfloat16)
            for acc, left, right in ((acc_v, p.astype(jnp.bfloat16), do), (acc_k, ds, q)):
                new = jnp.dot(left, right, preferred_element_type=f32)
                acc[s, e, kv, :] = new if masked else acc[s, e, kv, :] + new
            dqt_scr[i] += jnp.dot(kt_scr[b, :, kv], ds, preferred_element_type=f32)

    def pair_copies(s):
        return [remote(acc.at[s, 1 - core], dst.at[s], ss.at[s], rs.at[s], partner) for acc, dst, ss, rs in ((acc_k, pk, pks, pkr), (acc_v, pv, pvs, pvr))]

    def home_copies(s):
        dst = {"cp": lax.rem(chip + 1 + s, heads) * 2 + core}
        return [remote(src.at[s], cols(out, chip), ss.at[s], rs.at[s], dst) for src, out, ss, rs in ((sk, dk, ks, kr), (sv, dv_out, vs, vr))]

    def add_pair(s):
        for copy in pair_copies(s):
            copy.wait()
        sk[s] = (acc_k[s, core] + pk[s]) * scale
        sv[s] = (acc_v[s, core] + pv[s]).astype(sv.dtype)

    last = heads - 1

    def dq_copies(r):
        dst = lax.rem(me + r, cp_size)
        copies = []
        for s in BOTH:
            src = dqs.at[dst, s * sub : (s + 1) * sub, :]
            place = cols(dq, chip, sub_rows(core, s, sub))
            copies.append(remote(src, place, qs.at[r, s], qr.at[r, s], {"cp": dst}) if r else pltpu.make_async_copy(src, place, loc.at[s]))
        return copies

    def send_dq(early):
        for r in range(cp_size):
            dst = lax.rem(me + r, cp_size)
            ready = dst // 2 < chip

            @pl.when(ready if early else jnp.logical_not(ready))
            def _():
                dqs[dst] = dqt_scr[dst].T * scale
                for copy in dq_copies(r):
                    copy.start()

    def key_pair(s, carry):
        def key_block(e, inner):
            b = lax.rem(chip + 1 + s, heads) * 2 + e
            tile(b, b, s, e, True)

            def full(i, last):
                tile(i, b, s, e, False)
                return last

            lax.fori_loop(b + 1, cp_size, full, inner)

            @pl.when(jnp.logical_and(e < 1, s > 0))
            def _():
                add_pair(s - 1)
                for copy in home_copies(s - 1):
                    copy.start()

            return inner

        @pl.when(s == last)
        def _():
            send_dq(True)

        lax.fori_loop(0, 2, key_block, 0)
        for copy in pair_copies(s):
            copy.start()

        @pl.when(s == 1)
        def _():
            for k, (src, dst) in ways:
                whole = block_of(gp_out, src, sub)
                remote(whole, whole, gs.at[k], gr.at[k], partner).wait_recv()
                relay(k, src, dst).start()

        return carry

    lax.fori_loop(0, heads, key_pair, 0)
    send_dq(False)
    own.extend(dq_copies(0))
    for r in range(1, cp_size):
        sends.extend(dq_copies(r))
    add_pair(last)
    for j, (src, out) in enumerate(((sk, dk), (sv, dv_out))):
        copy = pltpu.make_async_copy(src.at[last], cols(out, chip), loc.at[2 + j])
        copy.start()
        own.append(copy)
    for copy in own:
        copy.wait()
    inv_cols = inv[...].T
    n_chunk = inv.shape[0] // 2
    dots = []

    def first_pass(i, grad, lin, gain):
        gains = [jnp.zeros((1, LANES), f32)] * heads
        for r in range(n_chunk):
            part_rows = slice(r * LANES, (r + 1) * LANES)
            c = i * n_chunk + r
            norm = inv_cols[:, c : c + 1]
            total = jnp.zeros((LANES, LANES), f32)
            for h in range(heads):
                lanes = slice(h * LANES, (h + 1) * LANES)
                hat = lin[part_rows, lanes] * norm
                back = rolled(grad[part_rows, lanes], cos_t[part_rows, :], -sin_t[part_rows, :])
                both = back * hat
                gains[h] = gains[h] + jnp.sum(both, axis=0, keepdims=True)
                total = total + both * gain[:, lanes]
                grad[part_rows, lanes] = back * gain[:, lanes]
            dots.append(jnp.sum(total, axis=1, keepdims=True))
        for h in range(heads):
            gain_out[i * heads + h : i * heads + h + 1, :] = gains[h]

    for s in range(last):
        place = cols(dk, lax.rem(chip - 1 - s + heads, heads))
        remote(place, place, ks.at[s], kr.at[s], partner).wait_recv()
    first_pass(1, dk, k_lin, k_gain)
    for r in range(1, cp_size):
        src = lax.rem(me - r + cp_size, cp_size)
        for s in BOTH:
            place = cols(dq, src // 2, sub_rows(lax.rem(src, 2), s, sub))
            remote(place, place, qs.at[r, s], qr.at[r, s], partner).wait_recv()
    first_pass(0, dq, q_lin, q_gain)
    part[...] = jnp.concatenate(dots[n_chunk:] + dots[:n_chunk], axis=1).T
    dot_cols = (share_over_tp(tp_size, me_tp, part, got, ts, tr)() / width).T
    for i, (grad, lin, out) in enumerate(((dq, q_lin, dq_out), (dk, k_lin, dk_out))):
        for r in range(n_chunk):
            part_rows = slice(r * LANES, (r + 1) * LANES)
            c = i * n_chunk + r
            norm = inv_cols[:, c : c + 1]
            out[part_rows, :] = (norm * (grad[part_rows, :] - lin[part_rows, :] * norm * dot_cols[:, c : c + 1])).astype(out.dtype)
    for s in range(last):
        sends.extend(home_copies(s))
        place = cols(dv_out, lax.rem(chip - 1 - s + heads, heads))
        remote(place, place, vs.at[s], vr.at[s], partner).wait_recv()
    for r in range(1, tp_size):
        place = block_of(oo_out, lax.rem(me_tp - r + tp_size, tp_size), sub)
        remote(place, place, os.at[r], orr.at[r], partner).wait_recv()
    for k, (src, dst) in ways:
        sends.append(relay(k, src, dst))
        half = block_of(gp_out, t_far * 2 + k, sub // 2)
        remote(half, half, gs.at[2 + k], gr.at[2 + k], partner).wait_recv()
    for copy in sends:
        copy.wait_send()


def reduce_tail(tp_size, cp_size, *refs):
    n_w = 4
    (w_o_in, w_v_in), (dx_in, dy_in, small, y_in, x_in, dq_in, dk_in) = refs[:2], refs[2:9]
    refs = refs[9:]
    w_out, (dx_out, y_out, small_out) = refs[:n_w], refs[n_w : n_w + 3]
    refs = refs[n_w + 3 :]
    acc, pair, far_a, far_b, fin_l, fin_r = (refs[i * n_w : (i + 1) * n_w] for i in range(6))
    refs = refs[6 * n_w :]
    w_q_in, w_k_in, dxa, dxb, dx_own, dx_fa, dx_fb, dx_fl, dx_fr, dx16, got_small, got_post, ss, rs, ps, pr, fs, fr, loc, sms, smr, gps, gpr = refs
    w_in = (w_o_in, w_v_in, w_q_in, w_k_in)
    me_tp = lax.axis_index("tp")
    me_cp = lax.axis_index("cp")
    core = lax.rem(me_cp, 2)
    chip = me_cp // 2
    ring = cp_size // 2
    left, right, far = (lax.rem(chip + d, ring) for d in (ring - 1, 1, 2))
    t_left, t_right, t_far = (lax.rem(me_tp + d, tp_size) for d in (tp_size - 1, 1, 2))
    partner = {"cp": me_cp + 1 - 2 * core}
    to_l, to_r = {"cp": left * 2 + core}, {"cp": right * 2 + core}
    tp_l, tp_r = {"tp": t_left}, {"tp": t_right}
    dx_i, y_i = n_w, n_w + 1
    outs = []

    def ring_sems(t, kind):
        return ss.at[t, kind], rs.at[t, kind]

    def pair_sems(t, kind):
        return fs.at[t, kind], fr.at[t, kind]

    cross_barrier(me_tp, me_cp, tp_size, cp_size)
    sent = []

    def go(src, dst, s_sem, r_sem, device):
        copy = remote(src, dst, s_sem, r_sem, device)
        copy.start()
        sent.append(copy)

    def landed(dst, s_sem, r_sem):
        remote(dst, dst, s_sem, r_sem, partner).wait_recv()

    def piece(ref, t, x, c, part=None):
        size = w_in[t].shape[0] // cp_size
        first = (2 * x + c) * size
        if part is None:
            return ref.at[pl.ds(pl.multiple_of(first, size), size), :]
        return ref.at[pl.ds(pl.multiple_of(first + part * (size // 2), size // 2), size // 2), :]

    def rows_of(ref, y, part=None):
        size = dx_in.shape[0] // tp_size
        if part is None:
            return ref.at[pl.ds(pl.multiple_of(y * size, size), size), :]
        return ref.at[pl.ds(pl.multiple_of(y * size + part * (size // 2), size // 2), size // 2), :]

    def half_of(ref, part):
        size = ref.shape[0] // 2
        return ref.at[pl.ds(part * size, size), :]

    for r in range(1, cp_size):
        go(small, got_small.at[me_cp], sms.at[r], smr.at[r], {"cp": lax.rem(me_cp + r, cp_size)})
    go(rows_of(dx_in, t_far, 0), dx_fa, *ring_sems(dx_i, FAR_A), tp_l)
    go(rows_of(dx_in, t_far, 1), dx_fb, *ring_sems(dx_i, FAR_B), tp_r)
    go(rows_of(dx_in, t_left, 1), half_of(dx_fr, 1), *ring_sems(dx_i, NEAR_L), tp_l)
    go(rows_of(dx_in, t_right, 0), half_of(dx_fl, 0), *ring_sems(dx_i, NEAR_R), tp_r)
    def give(src, stream, out, dev_l, dev_r):
        copy = pltpu.make_async_copy(src, out, loc.at[stream, n_w])
        copy.start()
        outs.append(copy)
        go(src, out, *ring_sems(stream, OUT_L), dev_l)
        go(src, out, *ring_sems(stream, OUT_R), dev_r)

    give(y_in, y_i, rows_of(y_out, me_tp), tp_l, tp_r)
    order = (far, left, right, chip)
    loads = {}

    def start_pair(t):
        for i, x in enumerate(order):
            go(piece(w_in[t], t, x, 1 - core), pair[t].at[x], ps.at[t, i], pr.at[t, i], partner)
            copy = pltpu.make_async_copy(piece(w_in[t], t, x, core), acc[t].at[x], loc.at[t, i])
            copy.start()
            loads[t, i] = copy

    start_pair(0)
    start_pair(1)
    dx_loads = [
        pltpu.make_async_copy(rows_of(dx_in, t_left, 0), dxa, loc.at[n_w, 0]),
        pltpu.make_async_copy(rows_of(dx_in, t_right, 1), dxb, loc.at[n_w, 1]),
        pltpu.make_async_copy(rows_of(dx_in, me_tp), dx_own, loc.at[n_w, 2]),
    ]
    for copy in dx_loads:
        copy.start()

    for t in range(n_w):
        for i, x in enumerate(order):
            loads[t, i].wait()
            landed(pair[t].at[x], ps.at[t, i], pr.at[t, i])
            acc[t][x] += pair[t][x]
        go(half_of(acc[t].at[far], 0), far_a[t], *ring_sems(t, FAR_A), to_l)
        go(half_of(acc[t].at[far], 1), far_b[t], *ring_sems(t, FAR_B), to_r)
        go(half_of(acc[t].at[left], 1), half_of(fin_r[t], 1), *ring_sems(t, NEAR_L), to_l)
        go(half_of(acc[t].at[right], 0), half_of(fin_l[t], 0), *ring_sems(t, NEAR_R), to_r)
        if t < 2:
            out, grad = ((w_q_in, dq_in), (w_k_in, dk_in))[t]
            size = out.shape[0] // cp_size
            for p in range(cp_size):
                rows = slice(p * size, (p + 1) * size)
                out[rows, :] = jnp.dot(x_in[:, rows].T, grad[...], preferred_element_type=jnp.float32)
            start_pair(2 + t)

    got_small[me_cp] = small[...]
    for r in range(1, cp_size):
        landed(got_small.at[lax.rem(me_cp - r + cp_size, cp_size)], sms.at[r], smr.at[r])
    total = got_small[0]
    for i in range(1, cp_size):
        total = total + got_small[i]
    small_out[...] = total
    n_gain = small.shape[0] - got_post.shape[1]

    def second_half(t, acc_l, acc_r, fa, fb, fl, fr, dev_l, dev_r):
        half = fa.shape[0]
        landed(fa, *ring_sems(t, FAR_A))
        acc_l[...] += fa[...]
        landed(fb, *ring_sems(t, FAR_B))
        acc_r[...] += fb[...]
        go(acc_l, half_of(fr, 0), *ring_sems(t, SUM_L), dev_l)
        go(acc_r, half_of(fl, 1), *ring_sems(t, SUM_R), dev_r)

    def all_landed(t, fl, fr):
        landed(half_of(fr, 1), *ring_sems(t, NEAR_L))
        landed(half_of(fl, 0), *ring_sems(t, NEAR_R))
        landed(half_of(fr, 0), *ring_sems(t, SUM_L))
        landed(half_of(fl, 1), *ring_sems(t, SUM_R))

    for t in range(n_w):
        second_half(t, half_of(acc[t].at[left], 0), half_of(acc[t].at[right], 1), far_a[t], far_b[t], fin_l[t], fin_r[t], to_l, to_r)
    for copy in dx_loads:
        copy.wait()
    second_half(dx_i, dxa, dxb, dx_fa, dx_fb, dx_fl, dx_fr, tp_l, tp_r)
    post = small_out.at[pl.ds(n_gain, got_post.shape[1]), :]
    for r in range(1, tp_size):
        go(post, got_post.at[r], gps.at[r], gpr.at[r], {"tp": lax.rem(me_tp + r, tp_size)})

    for t in range(n_w):
        all_landed(t, fin_l[t], fin_r[t])
        acc[t][chip] = acc[t][chip] + (fin_l[t][...] + fin_r[t][...])
        src = acc[t].at[chip]
        dst = piece(w_out[t], t, chip, core)
        give(src, t, dst, to_l, to_r)
        go(src, dst, *pair_sems(t, 0), partner)
    all_landed(dx_i, dx_fl, dx_fr)
    dx16[...] = (dx_own[...] + (dx_fl[...] + dx_fr[...]) + dy_in[...].astype(jnp.float32)).astype(dx16.dtype)
    give(dx16, dx_i, rows_of(dx_out, me_tp), tp_l, tp_r)

    def relay(stream, part_of, x_l, x_r, dev_l, dev_r, pass_on):
        for arrived, x, kind, part, dev in ((OUT_L, x_r, RELAY_L, 0, dev_l), (OUT_R, x_l, RELAY_R, 1, dev_r)):
            whole = part_of(x)
            landed(whole, *ring_sems(stream, arrived))
            half = part_of(x, part)
            go(half, half, *ring_sems(stream, kind), dev)
            if pass_on:
                go(whole, whole, *pair_sems(stream, 1 + part), partner)

    for t in range(n_w):
        relay(t, functools.partial(lambda ref, t, x, part=None: piece(ref, t, x, core, part), w_out[t], t), left, right, to_l, to_r, True)
    for stream, out in ((y_i, y_out), (dx_i, dx_out)):
        relay(stream, functools.partial(rows_of, out), t_left, t_right, tp_l, tp_r, False)

    sums = small_out[n_gain:, :]
    for r in range(1, tp_size):
        landed(got_post.at[r], gps.at[r], gpr.at[r])
    sums = (sums + got_post[2]) + (got_post[1] + got_post[3])

    for t in range(n_w):
        for kind, part in PARTS:
            half = piece(w_out[t], t, far, core, part)
            landed(half, *ring_sems(t, kind))
            go(half, half, *pair_sems(t, 3 + part), partner)
    for stream, out in ((y_i, y_out), (dx_i, dx_out)):
        for kind, part in PARTS:
            landed(rows_of(out, t_far, part), *ring_sems(stream, kind))
    for t in range(n_w):
        for i, x in enumerate((chip, right, left)):
            landed(piece(w_out[t], t, x, 1 - core), *pair_sems(t, i))
        for part in BOTH:
            landed(piece(w_out[t], t, far, 1 - core, part), *pair_sems(t, 3 + part))
    for copy in outs:
        copy.wait()
    for copy in sent:
        copy.wait_send()
    small_out[n_gain:, :] = sums


def solution(mesh):
    tp_size = mesh.shape["tp"]
    cp_size = mesh.shape["cp"]
    act_spec = P("dp", "cp", None)
    col_spec = P(None, "tp", None)
    part_col = P("dp", "tp", None)
    in_specs = (act_spec, col_spec, col_spec, col_spec, P("tp", None, None), P("tp", None), P("tp", None), P(None), act_spec)
    out_specs = (act_spec, act_spec, part_col, part_col, part_col, P(("dp", "tp"), None, None), P(("dp", "tp"), None), P(("dp", "tp"), None), P("dp"))
    dma = pltpu.SemaphoreType.DMA

    def local_run(x_in, w_q, w_k, w_v, w_o, q_norm_w, k_norm_w, post_norm_w, grad_y):
        n_batch, block_len, d_model = x_in.shape
        heads, head_dim = w_q.shape[1:]
        assert n_batch == 1 and w_k.shape[1] == heads and cp_size == 2 * heads and tp_size == 4
        sub = block_len // tp_size
        rows = 2 * sub
        width = heads * head_dim * tp_size
        scale = head_dim ** -0.5
        f32 = jnp.float32
        b16 = jnp.bfloat16
        tp_index = lax.axis_index("tp")
        cp_index = lax.axis_index("cp")
        cos_tab, sin_tab = rope_tables(cp_index * block_len, block_len, head_dim)
        x_loc = x_in[0]
        dy_loc = grad_y[0]
        w_q2, w_k2, w_v2 = (w.reshape(d_model, -1) for w in (w_q, w_k, w_v))
        gains = [g.reshape(1, -1) for g in (q_norm_w, k_norm_w)]
        loc_width = heads * head_dim

        q_lin = jnp.dot(x_loc, w_q2, preferred_element_type=f32)
        k_lin = jnp.dot(x_loc, w_k2, preferred_element_type=f32)
        v_val = jnp.dot(x_loc, w_v2, preferred_element_type=f32).astype(b16)
        vec = jnp.stack([jnp.sum(t * t, axis=1) for t in (q_lin, k_lin)]).reshape(-1, LANES)
        vec_shape = jax.ShapeDtypeStruct(vec.shape, f32)
        kv_shape = jax.ShapeDtypeStruct((cp_size, block_len, head_dim), b16)
        lin16 = VMEM((block_len, loc_width), b16)
        tp_scratch = VMEM((tp_size,) + vec.shape, f32)
        q_all, k_all, v_all, inv, w_o_full = vmem_call(
            functools.partial(scatter_qkv, heads, tp_size, cp_size, width),
            [jax.ShapeDtypeStruct((cp_size, rows, head_dim), b16), kv_shape, kv_shape, vec_shape, jax.ShapeDtypeStruct((width, d_model), b16)],
            9,
            [lin16, lin16, tp_scratch, dma((5,))] + [dma((cp_size, 2))] * 2 + [dma((heads,))] * 8 + [dma((tp_size,))] * 6,
            0,
            1,
            1,
        )(q_lin, k_lin, vec, *gains, cos_tab, sin_tab, w_o.reshape(-1, d_model), v_val)

        qspec = pl.BlockSpec((1, rows, head_dim), lambda i: (i, 0, 0))
        lspec = pl.BlockSpec((1, 1, rows), lambda i: (i, 0, 0))
        kvspec = pl.BlockSpec((1, block_len, head_dim), lambda i: (i, 0, 0))
        pair_flops = cp_size * (cp_size + 1) // 2 * rows * block_len * head_dim * 2
        o_all, lse = pl.pallas_call(
            functools.partial(attend, sub, scale),
            grid=(cp_size,),
            in_specs=[qspec, kvspec, kvspec],
            out_specs=[qspec, lspec],
            out_shape=[jax.ShapeDtypeStruct((cp_size, rows, head_dim), b16), jax.ShapeDtypeStruct((cp_size, 1, rows), f32)],
            scratch_shapes=[VMEM((cp_size, block_len, head_dim), b16), VMEM((cp_size, head_dim, block_len), b16), VMEM((1, rows), f32), VMEM((1, rows), f32), VMEM((head_dim, rows), f32)]
            + [VMEM((block_len // 2, rows), f32)] * 2 + [VMEM((1, rows), f32)],
            compiler_params=pltpu.CompilerParams(vmem_limit_bytes=SMALL),
            cost_estimate=pl.CostEstimate(flops=2 * pair_flops, bytes_accessed=6 << 20, transcendentals=0),
        )(q_all, k_all, v_all)

        n_heads = heads * tp_size
        o_rows = vmem_call(
            functools.partial(heads_to_rows, heads, tp_size, cp_size),
            [jax.ShapeDtypeStruct((sub, width), b16)],
            1,
            [dma((2, cp_size)), dma((n_heads,))],
            1,
        )(o_all)[0]

        x_rows = lax.dynamic_slice_in_dim(x_loc, tp_index * sub, sub, 0)
        dy_rows = lax.dynamic_slice_in_dim(dy_loc, tp_index * sub, sub, 0)
        dy_f = dy_rows.astype(f32)
        proj = jnp.dot(o_rows, w_o_full, preferred_element_type=f32)
        post_inv = lax.rsqrt(jnp.mean(proj * proj, axis=-1, keepdims=True) + NORM_EPS)
        post_hat = proj * post_inv
        y_rows = (x_rows + post_hat * post_norm_w).astype(b16)
        grad_post = jnp.sum(dy_f * post_hat, axis=0)
        grad_hat = dy_f * post_norm_w
        gp_rows = (post_inv * (grad_hat - post_hat * jnp.mean(grad_hat * post_hat, axis=-1, keepdims=True))).astype(b16)
        do_rows = lax.dot_general(gp_rows, w_o_full, NT, preferred_element_type=f32).astype(b16)

        do_all = vmem_call(
            functools.partial(rows_to_heads, heads, tp_size, cp_size),
            [jax.ShapeDtypeStruct((cp_size, rows, head_dim), b16)],
            1,
            [dma((tp_size, heads)), dma((cp_size, 2))],
            2,
        )(do_rows)[0]

        lin_h, f_lin = jax.ShapeDtypeStruct((block_len, loc_width), b16), VMEM((block_len, loc_width), f32)
        head_f = VMEM((heads, block_len, head_dim), f32)
        pair_f = VMEM((heads, 2, block_len, head_dim), f32)
        dq16, dk16, dv16, gain_grads, grad_proj, o_own = vmem_call(
            functools.partial(attend_back, heads, tp_size, cp_size, width, scale),
            [lin_h, lin_h, lin_h, jax.ShapeDtypeStruct((2 * heads, head_dim), f32), jax.ShapeDtypeStruct((block_len, d_model), b16), lin_h],
            15,
            [f_lin, f_lin, VMEM((cp_size, head_dim, block_len), b16), VMEM((cp_size, head_dim, rows), f32), VMEM((cp_size, 1, rows), f32), VMEM((cp_size, rows, head_dim), f32)]
            + [pair_f, pair_f, f_lin, f_lin, head_f, head_f, head_f, VMEM((heads, block_len, head_dim), b16), VMEM(vec.shape, f32), tp_scratch, dma((8,))]
            + [dma((cp_size, 2))] * 2 + [dma((heads,))] * 8 + [dma((tp_size,))] * 6,
            3,
            2,
            2,
        )(q_all, k_all, v_all, o_all, do_all, lse, inv, *gains, cos_tab, sin_tab, gp_rows, o_rows, q_lin, k_lin)

        def wgrad(left, right):
            return lax.dot_general(left, right, (((0,), (0,)), ((), ())), preferred_element_type=f32)

        grad_w_o, grad_w_v = wgrad(o_own, grad_proj), wgrad(x_loc, dv16)
        dx_part = sum(lax.dot_general(g, w, NT, preferred_element_type=f32) for g, w in ((dq16, w_q2), (dk16, w_k2), (dv16, w_v2)))
        w_parts = [grad_w_o, grad_w_v, grad_w_v, grad_w_v]
        small = jnp.concatenate([gain_grads, grad_post.reshape(-1, head_dim)], axis=0)
        any_spec = pl.BlockSpec(memory_space=pl.ANY)
        vmem_spec = pl.BlockSpec(memory_space=VMEM)

        def bufs(lead, div):
            return [VMEM(lead + (w.shape[0] // div, w.shape[1]), f32) for w in w_parts]

        ring = cp_size // 2
        rows_dx, half_dx = VMEM((sub, d_model), f32), VMEM((sub // 2, d_model), f32)
        res = pl.pallas_call(
            functools.partial(reduce_tail, tp_size, cp_size),
            out_shape=[jax.ShapeDtypeStruct(w.shape, f32) for w in w_parts] + [jax.ShapeDtypeStruct((block_len, d_model), b16)] * 2 + [jax.ShapeDtypeStruct(small.shape, f32)],
            in_specs=[any_spec] * 3 + [vmem_spec] * 6,
            out_specs=[any_spec] * 6 + [vmem_spec],
            scratch_shapes=bufs((ring,), cp_size) * 2 + bufs((), 2 * cp_size) * 2 + bufs((), cp_size) * 2
            + [VMEM(grad_w_v.shape, f32)] * 2 + [half_dx, half_dx, rows_dx, half_dx, half_dx, rows_dx, rows_dx, VMEM((sub, d_model), b16)]
            + [VMEM((cp_size,) + small.shape, f32), VMEM((tp_size, d_model // head_dim, head_dim), f32)]
            + [dma((6, 10))] * 2 + [dma((4, 4))] * 2 + [dma((4, 5))] * 2 + [dma((6, 5))] + [dma((cp_size,))] * 2 + [dma((tp_size,))] * 2,
            compiler_params=pltpu.CompilerParams(vmem_limit_bytes=LIMIT, collective_id=6, has_side_effects=True),
        )(grad_w_o, grad_w_v, dx_part, dy_rows, small, y_rows, x_loc, dq16, dk16)
        grad_w_v, grad_w_q, grad_w_k = (g.reshape(w_q.shape) for g in res[1:4])
        grad_x, y_out, small_sum = res[4:]
        return (y_out[None], grad_x[None], grad_w_q, grad_w_k, grad_w_v, res[0].reshape(w_o.shape), small_sum[:heads], small_sum[heads : 2 * heads], small_sum[2 * heads :].reshape(-1))

    return jax.shard_map(local_run, mesh=mesh, in_specs=in_specs, out_specs=out_specs, check_vma=False)
```
